32 devices in a mesh: dp: 4 (over y, z), stage: 8 (over x, core).
Axes of the slice: x: 4, y: 2, z: 2, core: 2. Of those that a mesh axis runs over, the one named last changes fastest.
The devices are a block of a 4x4x8 slice.
Arguments:
- tokens: int32 [64, 64], P('dp'), parts along dimension 0
- labels: int32 [64, 64], P('dp'), parts along dimension 0
- emb_table: bfloat16 [30592, 128], replicated
- w_up: bfloat16 [8, 128, 512], P('stage')
- w_down: bfloat16 [8, 512, 128], P('stage')
Outputs:
- output 1: float32 [4], P('dp'), parts along dimension 0
- output 2: float32 [32, 128, 512], P(('dp', 'stage')), parts along dimension 0
- output 3: float32 [32, 512, 128], P(('dp', 'stage')), parts along dimension 0
- output 4: float32 [122368, 128], P('dp'), parts along dimension 0
There are 4 independent parts. The reference program is written for one: setup_inputs(seed, part) draws one part's arguments, and reference() takes and returns one part's arrays. A program takes and returns all parts, laid end to end along the dimension named above; an argument that names none is the same for every part.
All inputs are finite; a program needn't handle non-finite values.
Results may differ from the reference program's by a relative error of at most 0.02.
Values are sent between devices in bfloat16 or wider.
A program may use at most 768 MiB of HBM per device.

```python
import jax
import jax.numpy as jnp
from jax import lax

VOCAB_SIZE = 30592
MODEL_DIM = 128
FFN_DIM = 512
NUM_STAGES = 8
NUM_MICRO = 16
SEQ_TOKENS = 64

LOGIT_SCALE = MODEL_DIM ** -0.5
INV_COUNT = 1.0 / (NUM_MICRO * SEQ_TOKENS)


def setup_inputs(seed: int = 0, part: int = 0) -> dict:
    key_part = jax.random.fold_in(jax.random.key(seed), part)
    key_ids, key_shift = jax.random.split(key_part)
    key_emb, key_up, key_down = jax.random.split(jax.random.key(seed + 1), 3)
    raw_ids = jax.random.randint(key_ids, (NUM_MICRO, SEQ_TOKENS + 1), 0, VOCAB_SIZE)
    shifts = jax.random.randint(key_shift, (NUM_MICRO, SEQ_TOKENS + 1), 0, 9)
    sequence = jnp.right_shift(raw_ids, shifts)
    sequence = sequence.at[0, 0].set(VOCAB_SIZE - 1).at[0, 1].set(0)
    emb_table = jax.random.normal(key_emb, (VOCAB_SIZE, MODEL_DIM), jnp.float32)
    w_up = jax.random.normal(key_up, (NUM_STAGES, MODEL_DIM, FFN_DIM), jnp.float32) * MODEL_DIM ** -0.5
    w_down = jax.random.normal(key_down, (NUM_STAGES, FFN_DIM, MODEL_DIM), jnp.float32) * (2.0 / (FFN_DIM * NUM_STAGES)) ** 0.5
    return {"tokens": sequence[:, :-1], "labels": sequence[:, 1:], "emb_table": emb_table.astype(jnp.bfloat16), "w_up": w_up.astype(jnp.bfloat16), "w_down": w_down.astype(jnp.bfloat16)}


def rms_normalize(x_act):
    x_wide = x_act.astype(jnp.float32)
    inv_rms = lax.rsqrt(jnp.mean(x_wide * x_wide, axis=-1, keepdims=True) + 1e-6)
    return (x_wide * inv_rms).astype(jnp.bfloat16)


def micro_loss(table_f32, up_f32, down_f32, tok_row, lab_row):
    x_act = table_f32[tok_row].astype(jnp.bfloat16)

    def layer_step(x_cur, weights):
        x_wide = x_cur.astype(jnp.float32)
        pre_act = jnp.dot(x_wide, weights[0], preferred_element_type=jnp.float32).astype(jnp.bfloat16)
        hidden = jax.nn.gelu(pre_act.astype(jnp.float32)).astype(jnp.bfloat16)
        branch = jnp.dot(hidden.astype(jnp.float32), weights[1], preferred_element_type=jnp.float32)
        return (x_wide + branch).astype(jnp.bfloat16), None

    x_act, _ = lax.scan(layer_step, x_act, (up_f32, down_f32))
    normed = rms_normalize(x_act)
    logits = (jnp.dot(normed.astype(jnp.float32), table_f32.T, preferred_element_type=jnp.float32) * LOGIT_SCALE).astype(jnp.bfloat16)
    logit_f = logits.astype(jnp.float32)
    log_norm = jax.nn.logsumexp(logit_f, axis=-1)
    picked = jnp.take_along_axis(logit_f, lab_row[:, None], axis=-1)[:, 0]
    return jnp.sum(log_norm - picked) * INV_COUNT


def reference(tokens, labels, emb_table, w_up, w_down):
    table_f32 = emb_table.astype(jnp.float32)
    up_f32 = w_up.astype(jnp.float32)
    down_f32 = w_down.astype(jnp.float32)
    grad_fn = jax.value_and_grad(micro_loss, argnums=(0, 1, 2))

    def micro_step(loop_state, micro_rows):
        loss_sum, grad_emb, grad_up, grad_down = loop_state
        loss_val, grad_all = grad_fn(table_f32, up_f32, down_f32, micro_rows[0], micro_rows[1])
        return (loss_sum + loss_val, grad_emb + grad_all[0], grad_up + grad_all[1], grad_down + grad_all[2]), None

    init_carry = (jnp.zeros((), jnp.float32), jnp.zeros_like(table_f32), jnp.zeros_like(up_f32), jnp.zeros_like(down_f32))
    (loss_sum, grad_emb, grad_up, grad_down), _ = lax.scan(micro_step, init_carry, (tokens, labels))
    return loss_sum.reshape(1), grad_up, grad_down, grad_emb
```

```python
import functools
import math

import jax
import jax.numpy as jnp
from jax import lax
from jax.experimental import pallas as pl
from jax.experimental.pallas import tpu as pltpu
from jax.sharding import PartitionSpec as P

MESH = pl.DeviceIdType.MESH
F32 = jnp.float32
BF16 = jnp.bfloat16
LOG2E = math.log2(math.e)
LN2 = math.log(2.0)
GELU_C = math.sqrt(2.0 / math.pi)
HEAD_BLOCK = 2048
EMB_BLOCK = 512
VMEM_BYTES = 60 * 1024 * 1024


def dot_nn(a, b):
    return lax.dot_general(a, b, (((1,), (0,)), ((), ())), preferred_element_type=F32)


def dot_nt(a, b):
    return lax.dot_general(a, b, (((1,), (1,)), ((), ())), preferred_element_type=F32)


def dot_tn(a, b):
    return lax.dot_general(a, b, (((0,), (0,)), ((), ())), preferred_element_type=F32)


def gelu_value(a):
    return a * (0.5 * (1.0 + jnp.tanh(GELU_C * (a + 0.044715 * (a * a * a)))))


def gelu_slope(a):
    sq = a * a
    t = jnp.tanh(GELU_C * (a + 0.044715 * (sq * a)))
    return 0.5 * (1.0 + t) + (0.5 * a) * (1.0 - t * t) * (GELU_C * (1.0 + (3.0 * 0.044715) * sq))


def column_of(row, size):
    return jnp.transpose(jnp.broadcast_to(row, (size, size)))


def row_of(col, size):
    eye = lax.broadcasted_iota(jnp.int32, (size, size), 0) == lax.broadcasted_iota(jnp.int32, (size, size), 1)
    return jnp.sum(jnp.where(eye, jnp.broadcast_to(col, (size, size)), 0.0), axis=0, keepdims=True)


def token_kernel(
    n_stage, tok_ref, lab_ref, emb_hbm, wup_hbm, wdn_hbm,
    n_out, st_out, xs_out, gs_out, dx_out, ids_out, starts_out,
    wup, wdn, emb, z_buf, xs, gs, pre, n_loc, st_loc, gat,
    loc_sem, wsend, upr, dnr, xsend, xrecv, gsend, grecv, nsend, nrecv, ssend, srecv, dsend, drecv,
):
    me = lax.axis_index("stage")
    n_chip = n_stage // 2
    chip, core = me // 2, lax.rem(me, 2)
    sib = chip * 2 + (1 - core)
    right = lax.rem(chip + 1, n_chip) * 2 + core
    left = lax.rem(chip + n_chip - 1, n_chip) * 2 + core
    far = lax.rem(chip + 2, n_chip) * 2 + core
    peers = [lax.rem(me + d, n_stage) for d in range(1, n_stage)]
    tok_n, dim = n_loc.shape
    vocab = emb.shape[0]
    total = n_stage * tok_n
    scale = dim ** -0.5

    load_up = pltpu.make_async_copy(wup_hbm, wup.at[me], loc_sem.at[0])
    load_dn = pltpu.make_async_copy(wdn_hbm, wdn.at[me], loc_sem.at[1])
    load_emb = pltpu.make_async_copy(emb_hbm, emb, loc_sem.at[2])
    load_up.start()
    load_dn.start()
    load_emb.start()

    barrier = pltpu.get_barrier_semaphore()
    for peer in peers:
        pl.semaphore_signal(barrier, inc=1, device_id={"stage": peer}, device_id_type=MESH)
    pl.semaphore_wait(barrier, n_stage - 1)
    load_up.wait()
    load_dn.wait()

    def up_copy(i, slot, dst):
        return pltpu.make_async_remote_copy(
            wup.at[slot], wup.at[slot], wsend.at[i], upr.at[slot], device_id={"stage": dst}, device_id_type=MESH)

    def dn_copy(i, slot, dst):
        return pltpu.make_async_remote_copy(
            wdn.at[slot], wdn.at[slot], wsend.at[i], dnr.at[slot], device_id={"stage": dst}, device_id_type=MESH)

    first = [up_copy(0, me, right), dn_copy(1, me, left), dn_copy(2, me, right), up_copy(3, me, left),
             up_copy(4, me, sib), dn_copy(5, me, sib)]
    for copy in first:
        copy.start()

    tok_row = tok_ref[...]
    pos = lax.broadcasted_iota(jnp.int32, (n_stage, tok_n), 0) * tok_n + lax.broadcasted_iota(jnp.int32, (n_stage, tok_n), 1)
    key_row = tok_row * total + pos
    lane = lax.broadcasted_iota(jnp.int32, (tok_n, tok_n), 1)
    key_cols = [column_of(key_row[j:j + 1, :], tok_n) for j in range(n_stage)]
    tok_cols = [column_of(tok_row[j:j + 1, :], tok_n) for j in range(n_stage)]
    rank_rows = []
    for i in range(n_stage):
        acc = jnp.zeros((tok_n, tok_n), jnp.int32)
        for j in range(n_stage):
            acc = acc + jnp.where(key_cols[j] < key_row[i:i + 1, :], 1, 0)
        rank_rows.append(jnp.sum(acc, axis=0, keepdims=True))
    rank_cols = [column_of(r, tok_n) for r in rank_rows]
    for c in range(n_stage):
        acc = jnp.zeros((tok_n, tok_n), jnp.int32)
        for j in range(n_stage):
            acc = acc + jnp.where(rank_cols[j] == lane + c * tok_n, tok_cols[j], 0)
        ids_out[c] = jnp.broadcast_to(jnp.sum(acc, axis=0, keepdims=True), (8, tok_n))
    acc = jnp.zeros((tok_n, tok_n), jnp.int32)
    for j in range(n_stage):
        acc = acc + jnp.where(tok_cols[j] < lane * EMB_BLOCK, 1, 0)
    starts_out[0:8, :] = jnp.broadcast_to(jnp.sum(acc, axis=0, keepdims=True), (8, tok_n))
    for i in range(n_stage):
        starts_out[8 + i:9 + i, :] = rank_rows[i]

    load_emb.wait()
    pick = jnp.concatenate(
        [column_of(tok_ref[pl.ds(me, 1), :], tok_n), column_of(lab_ref[pl.ds(me, 1), :], tok_n)], axis=0)
    lane2 = lax.broadcasted_iota(jnp.int32, (2 * tok_n, tok_n), 1)

    def blocks(body):
        full = vocab // HEAD_BLOCK

        def step(i, carry):
            body(pl.multiple_of(i * HEAD_BLOCK, HEAD_BLOCK), HEAD_BLOCK)
            return carry

        lax.fori_loop(0, full, step, 0)
        if vocab % HEAD_BLOCK:
            body(full * HEAD_BLOCK, vocab % HEAD_BLOCK)

    gat[...] = jnp.zeros_like(gat)

    def gather_block(v0, size):
        hot = jnp.concatenate(
            [jnp.where(pick == lane2 + (v0 + j * tok_n), 1.0, 0.0).astype(BF16) for j in range(size // tok_n)], axis=1)
        gat[...] += dot_nn(hot, emb[pl.ds(v0, size), :])

    blocks(gather_block)
    x0 = gat[0:tok_n, :].astype(BF16)
    lab_rows = gat[tok_n:2 * tok_n, :]
    lab_bf = lab_rows.astype(BF16)

    up_copy(0, left, sib).wait_recv()
    second = [up_copy(6, left, right), up_copy(7, left, sib)]
    second[0].start()
    second[1].start()
    dn_copy(0, right, sib).wait_recv()
    second += [dn_copy(8, right, left), dn_copy(9, right, sib)]
    second[2].start()
    second[3].start()
    dn_copy(0, left, sib).wait_recv()
    second.append(dn_copy(10, left, sib))
    second[4].start()
    up_copy(0, right, sib).wait_recv()
    second.append(up_copy(11, right, sib))
    second[5].start()
    up_copy(0, far, sib).wait_recv()
    second.append(up_copy(12, far, sib))
    second[6].start()
    dn_copy(0, far, sib).wait_recv()
    second.append(dn_copy(13, far, sib))
    second[7].start()

    def x_copy(layer):
        return pltpu.make_async_remote_copy(
            xs.at[layer], xs_out.at[me], xsend.at[layer], xrecv.at[me], device_id={"stage": layer}, device_id_type=MESH)

    def g_copy(layer):
        return pltpu.make_async_remote_copy(
            gs.at[layer + 1], gs_out.at[me], gsend.at[layer], grecv.at[me], device_id={"stage": layer}, device_id_type=MESH)

    own_x = pltpu.make_async_copy(xs.at[me], xs_out.at[me], loc_sem.at[0])
    own_g = pltpu.make_async_copy(gs.at[me + 1], gs_out.at[me], loc_sem.at[1])

    xs[0] = x0

    def forward(layer, carry):
        @pl.when(lax.rem(layer, 2) != core)
        def _():
            up_copy(0, layer, sib).wait_recv()
            dn_copy(0, layer, sib).wait_recv()

        x = xs[layer]
        a = dot_nn(x, wup[layer]).astype(BF16)
        pre[layer] = a
        h = gelu_value(a.astype(F32)).astype(BF16)
        xs[layer + 1] = (x.astype(F32) + dot_nn(h, wdn[layer])).astype(BF16)

        @pl.when(layer != me)
        def _():
            x_copy(layer).start()

        @pl.when(layer == me)
        def _():
            own_x.start()

        return carry

    lax.fori_loop(0, n_stage, forward, 0)

    x_last = xs[n_stage].astype(F32)
    inv = lax.rsqrt(jnp.mean(x_last * x_last, axis=-1, keepdims=True) + 1e-6)
    n_val = (x_last * inv).astype(BF16)
    n_loc[...] = n_val

    def spread(src, dst, send, recv):
        return [pltpu.make_async_remote_copy(src, dst.at[me], send.at[d], recv.at[me], device_id={"stage": peer},
                                             device_id_type=MESH) for d, peer in enumerate(peers)]

    def stat_block(v0, size):
        z = (dot_nt(n_loc[...], emb[pl.ds(v0, size), :]) * scale).astype(BF16)
        z_buf[:, pl.ds(v0, size)] = z
        parts = [z[:, j * tok_n:(j + 1) * tok_n].astype(F32) for j in range(size // tok_n)]
        m_old = gat[0:tok_n, :]
        m_new = functools.reduce(jnp.maximum, parts, m_old)
        s_new = gat[tok_n:2 * tok_n, :] * jnp.exp2((m_old - m_new) * LOG2E)
        for part in parts:
            s_new = s_new + jnp.exp2((part - m_new) * LOG2E)
        gat[0:tok_n, :] = m_new
        gat[tok_n:2 * tok_n, :] = s_new

    gat[0:tok_n, :] = jnp.full((tok_n, dim), -1e30, F32)
    gat[tok_n:2 * tok_n, :] = jnp.zeros((tok_n, dim), F32)
    send_n = spread(n_loc, n_out, nsend, nrecv)
    for copy in send_n:
        copy.start()
    own_n = pltpu.make_async_copy(n_loc, n_out.at[me], loc_sem.at[2])
    own_n.start()
    blocks(stat_block)
    m_lane = gat[0:tok_n, :]
    m_tok = jnp.max(m_lane, axis=-1, keepdims=True)
    s_tok = jnp.sum(gat[tok_n:2 * tok_n, :] * jnp.exp2((m_lane - m_tok) * LOG2E), axis=-1, keepdims=True)
    lse = m_tok + jnp.log(s_tok)
    level = lse * LOG2E + math.log2(total)
    z_pair = (dot_nt(n_val, lab_bf) * scale).astype(BF16).astype(F32)
    eye = lax.broadcasted_iota(jnp.int32, (tok_n, tok_n), 0) == lane
    z_lab = jnp.sum(jnp.where(eye, z_pair, 0.0), axis=-1, keepdims=True)
    p_lab = jnp.exp2(z_lab * LOG2E - level)
    d_lab = (p_lab - 1.0 / total).astype(BF16).astype(F32)
    p_lab = p_lab.astype(BF16).astype(F32)
    st_loc[...] = jnp.concatenate(
        [row_of(level, tok_n), row_of(d_lab, tok_n), row_of(lse - z_lab, tok_n), jnp.zeros((5, tok_n), F32)], axis=0)
    level_full = jnp.broadcast_to(level, (tok_n, tok_n))

    gat[0:tok_n, :] = (d_lab - p_lab) * lab_rows
    send_s = spread(st_loc, st_out, ssend, srecv)
    for copy in send_s:
        copy.start()
    own_s = pltpu.make_async_copy(st_loc, st_out.at[me], loc_sem.at[3])
    own_s.start()

    def grad_block(v0, size):
        parts = []
        for j in range(size // tok_n):
            z = z_buf[:, pl.ds(v0 + j * tok_n, tok_n)].astype(F32)
            parts.append(jnp.exp2(z * LOG2E - level_full).astype(BF16))
        gat[0:tok_n, :] += dot_nn(jnp.concatenate(parts, axis=1), emb[pl.ds(v0, size), :])

    blocks(grad_block)
    dn = (gat[0:tok_n, :] * scale).astype(BF16).astype(F32)
    corr = jnp.mean(dn * x_last, axis=-1, keepdims=True)
    gs[n_stage] = (inv * dn - x_last * (inv * inv * inv * corr)).astype(BF16)

    def backward(i, carry):
        layer = n_stage - 1 - i
        g = gs[layer + 1]
        dh = dot_nt(g, wdn[layer]).astype(BF16).astype(F32)
        da = (dh * gelu_slope(pre[layer].astype(F32))).astype(BF16)
        gs[layer] = (g.astype(F32) + dot_nt(da, wup[layer])).astype(BF16)

        @pl.when(layer != me)
        def _():
            g_copy(layer).start()

        @pl.when(layer == me)
        def _():
            own_g.start()

        return carry

    lax.fori_loop(0, n_stage, backward, 0)
    send_d = spread(gs.at[0], dx_out, dsend, drecv)
    for copy in send_d:
        copy.start()
    own_d = pltpu.make_async_copy(gs.at[0], dx_out.at[me], loc_sem.at[4])
    own_d.start()

    for copy in first + second + send_n + send_s:
        copy.wait_send()
    for copy in (own_x, own_g, own_n, own_s, own_d):
        copy.wait()
    for d, peer in enumerate(peers):
        pltpu.make_async_remote_copy(xs.at[peer], xs_out.at[peer], xsend.at[peer], xrecv.at[peer],
                                     device_id={"stage": peer}, device_id_type=MESH).wait()
        pltpu.make_async_remote_copy(gs.at[peer + 1], gs_out.at[peer], gsend.at[peer], grecv.at[peer],
                                     device_id={"stage": peer}, device_id_type=MESH).wait()
        for src, dst, send, recv in ((n_loc, n_out, nsend, nrecv), (st_loc, st_out, ssend, srecv)):
            pltpu.make_async_remote_copy(src, dst.at[peer], send.at[d], recv.at[peer],
                                         device_id={"stage": peer}, device_id_type=MESH).wait_recv()
        pltpu.make_async_remote_copy(gs.at[0], dx_out.at[peer], dsend.at[d], drecv.at[peer],
                                     device_id={"stage": peer}, device_id_type=MESH).wait_recv()
    for copy in send_d:
        copy.wait_send()


def weight_kernel(x_ref, g_ref, wup_ref, wdn_ref, st_ref, gup_ref, gdn_ref, loss_ref):
    n_stage, tok_n, _ = x_ref.shape
    step = 2

    def body(i, carry):
        x = jnp.concatenate([x_ref[step * i + k] for k in range(step)], axis=0)
        g = jnp.concatenate([g_ref[step * i + k] for k in range(step)], axis=0)
        a = dot_nn(x, wup_ref[...]).astype(BF16).astype(F32)
        sq = a * a
        t = jnp.tanh(GELU_C * (a + 0.044715 * (sq * a)))
        cdf = 0.5 * (1.0 + t)
        h = (a * cdf).astype(BF16)
        slope = cdf + (0.5 * a) * (1.0 - t * t) * (GELU_C * (1.0 + (3.0 * 0.044715) * sq))
        dh = dot_nt(g, wdn_ref[...]).astype(BF16).astype(F32)
        da = (dh * slope).astype(BF16)
        gup_ref[...] += dot_tn(x, da)
        gdn_ref[...] += dot_tn(h, g)
        return carry

    gup_ref[...] = jnp.zeros_like(gup_ref)
    gdn_ref[...] = jnp.zeros_like(gdn_ref)
    lax.fori_loop(0, n_stage // step, body, 0)
    nll = jnp.sum(st_ref[:, 2, :], keepdims=True) * (1.0 / (n_stage * tok_n))
    loss_ref[...] = jnp.broadcast_to(nll, loss_ref.shape)


def table_kernel(starts_sm, emb_ref, n_ref, st_ref, lab_ref, dx_ref, ids_ref, rank_ref, out_ref, n_t, level, d_lab, lab16, dxs):
    n_chunk, tok_n, dim = n_ref.shape
    total = n_chunk * tok_n
    blk = pl.program_id(0)
    rows = out_ref.shape[0]
    scale = dim ** -0.5

    @pl.when(blk == 0)
    def _():
        row_id = lax.broadcasted_iota(jnp.int32, (tok_n, tok_n), 0)
        for i in range(n_chunk):
            cols = slice(i * tok_n, (i + 1) * tok_n)
            n_t[:, cols] = jnp.transpose(n_ref[i])
            level[:, cols] = jnp.broadcast_to(st_ref[i, 0:1, :], (8, tok_n))
            d_lab[:, cols] = jnp.broadcast_to(st_ref[i, 1:2, :], (16, tok_n)).astype(BF16)
        for c in range(n_chunk):
            acc = jnp.zeros((tok_n, dim), F32)
            for i in range(n_chunk):
                hot = jnp.where(rank_ref[i:i + 1, :] == row_id + c * tok_n, 1.0, 0.0).astype(BF16)
                acc = acc + dot_nn(hot, dx_ref[i])
            dxs[c] = acc.astype(BF16)

    wide = 2 * tok_n
    e = emb_ref[...]
    base = blk * rows
    acc = jnp.zeros((rows, dim), F32)
    row16 = lax.broadcasted_iota(jnp.int16, (rows, wide), 0)
    for t in range(total // wide):
        cols = slice(t * wide, (t + 1) * wide)
        z = (dot_nn(e, n_t[:, cols]) * scale).astype(BF16).astype(F32)
        p = jnp.exp2(z * LOG2E - level[0:1, cols]).astype(BF16)
        lab = jnp.concatenate([lab_ref[2 * t:2 * t + 1, :], lab_ref[2 * t + 1:2 * t + 2, :]], axis=1) - base
        lab = jnp.broadcast_to(lab, (16, wide)).astype(jnp.int16)
        dz = jnp.where(row16 == lab[0:1, :], d_lab[0:1, cols], p)
        nn = jnp.concatenate([n_ref[2 * t], n_ref[2 * t + 1]], axis=0)
        acc = acc + dot_nn(dz, nn)

    row32 = lax.broadcasted_iota(jnp.int32, (rows, tok_n), 0)

    def token_term(c):
        hot = jnp.where(row32 == ids_ref[c, 0:1, :] - base, 1.0, 0.0).astype(BF16)
        return dot_nn(hot, dxs[c])

    first = jnp.minimum(starts_sm[blk] // tok_n, n_chunk - 1)
    last = (starts_sm[blk + 1] + tok_n - 1) // tok_n
    out_ref[...] = acc * scale + token_term(first)

    def more(c, carry):
        out_ref[...] += token_term(c)
        return carry

    lax.fori_loop(first + 1, last, more, 0)


def solution(mesh):
    n_stage = mesh.shape["stage"]

    def device_fn(tokens, labels, emb_table, w_up, w_down):
        vocab, dim = emb_table.shape
        ffn = w_up.shape[2]
        total = tokens.shape[0] * tokens.shape[1]
        tok_n = total // n_stage
        tok8 = tokens.reshape(n_stage, tok_n)
        lab8 = labels.reshape(n_stage, tok_n)
        w_up, w_down = w_up[0], w_down[0]
        vmem = pl.BlockSpec(memory_space=pltpu.VMEM)
        hbm = pl.BlockSpec(memory_space=pl.ANY)
        dma = pltpu.SemaphoreType.DMA
        n_blk = pl.cdiv(vocab, EMB_BLOCK)
        act = jax.ShapeDtypeStruct((n_stage, tok_n, dim), BF16)
        n_all, st_all, xs_all, gs_all, dx_all, ids, starts = pl.pallas_call(
            functools.partial(token_kernel, n_stage),
            out_shape=[act, jax.ShapeDtypeStruct((n_stage, 8, tok_n), F32), act, act, act,
                       jax.ShapeDtypeStruct((n_stage, 8, tok_n), jnp.int32),
                       jax.ShapeDtypeStruct((8 + n_stage, tok_n), jnp.int32)],
            in_specs=[vmem, vmem, hbm, hbm, hbm],
            out_specs=[hbm, hbm, hbm, hbm, hbm, vmem, vmem],
            scratch_shapes=[
                pltpu.VMEM((n_stage, dim, ffn), BF16), pltpu.VMEM((n_stage, ffn, dim), BF16),
                pltpu.VMEM((vocab, dim), BF16), pltpu.VMEM((tok_n, vocab), BF16),
                pltpu.VMEM((n_stage + 1, tok_n, dim), BF16), pltpu.VMEM((n_stage + 1, tok_n, dim), BF16),
                pltpu.VMEM((n_stage, tok_n, ffn), BF16), pltpu.VMEM((tok_n, dim), BF16),
                pltpu.VMEM((8, tok_n), F32), pltpu.VMEM((2 * tok_n, dim), F32),
                dma((5,)), dma((14,))] + [dma((n_stage,))] * 12,
            compiler_params=pltpu.CompilerParams(collective_id=0, has_side_effects=True, vmem_limit_bytes=VMEM_BYTES),
            name="token_pass",
        )(tok8, lab8, emb_table, w_up, w_down)

        grad_up, grad_down, loss = pl.pallas_call(
            weight_kernel,
            out_shape=[jax.ShapeDtypeStruct((dim, ffn), F32), jax.ShapeDtypeStruct((ffn, dim), F32),
                       jax.ShapeDtypeStruct((8, 128), F32)],
            in_specs=[vmem] * 5, out_specs=[vmem] * 3,
            compiler_params=pltpu.CompilerParams(vmem_limit_bytes=VMEM_BYTES),
            name="weight_grads",
        )(xs_all, gs_all, w_up, w_down, st_all)

        whole3 = lambda i, s: (0, 0, 0)
        whole2 = lambda i, s: (0, 0)
        grad_emb = pl.pallas_call(
            table_kernel,
            grid_spec=pltpu.PrefetchScalarGridSpec(
                num_scalar_prefetch=1, grid=(n_blk,),
                in_specs=[pl.BlockSpec((EMB_BLOCK, dim), lambda i, s: (i, 0)),
                          pl.BlockSpec((n_stage, tok_n, dim), whole3), pl.BlockSpec((n_stage, 8, tok_n), whole3),
                          pl.BlockSpec((n_stage, tok_n), whole2), pl.BlockSpec((n_stage, tok_n, dim), whole3),
                          pl.BlockSpec((n_stage, 8, tok_n), whole3), pl.BlockSpec((n_stage, tok_n), whole2)],
                out_specs=pl.BlockSpec((EMB_BLOCK, dim), lambda i, s: (i, 0)),
                scratch_shapes=[pltpu.VMEM((dim, total), BF16), pltpu.VMEM((8, total), F32), pltpu.VMEM((16, total), BF16),
                                pltpu.VMEM((16, total), jnp.int16), pltpu.VMEM((n_stage, tok_n, dim), BF16)]),
            out_shape=jax.ShapeDtypeStruct((vocab, dim), F32),
            compiler_params=pltpu.CompilerParams(dimension_semantics=("arbitrary",), vmem_limit_bytes=VMEM_BYTES),
            name="table_grad",
        )(starts[0], emb_table, n_all, st_all, lab8, dx_all, ids, starts[8:])
        return loss[0, :1], grad_up[None], grad_down[None], grad_emb

    return jax.shard_map(
        device_fn, mesh=mesh,
        in_specs=(P("dp", None), P("dp", None), P(None, None), P("stage", None, None), P("stage", None, None)),
        out_specs=(P("dp"), P(("dp", "stage"), None, None), P(("dp", "stage"), None, None), P("dp", None)),
        check_vma=False)
```

```python
import functools
import math

import jax
import jax.numpy as jnp
from jax import lax
from jax.experimental import pallas as pl
from jax.experimental.pallas import tpu as pltpu
from jax.sharding import PartitionSpec as P

MESH = pl.DeviceIdType.MESH
F32 = jnp.float32
BF16 = jnp.bfloat16
LOG2E = math.log2(math.e)
LN2 = math.log(2.0)
GELU_C = math.sqrt(2.0 / math.pi)
HEAD_BLOCK = 2048
EMB_BLOCK = 1024
VMEM_BYTES = 60 * 1024 * 1024


def dot_nn(a, b):
    return lax.dot_general(a, b, (((1,), (0,)), ((), ())), preferred_element_type=F32)


def dot_nt(a, b):
    return lax.dot_general(a, b, (((1,), (1,)), ((), ())), preferred_element_type=F32)


def dot_tn(a, b):
    return lax.dot_general(a, b, (((0,), (0,)), ((), ())), preferred_element_type=F32)


def gelu_value(a):
    return a * (0.5 * (1.0 + jnp.tanh(GELU_C * (a + 0.044715 * (a * a * a)))))


def gelu_slope(a):
    sq = a * a
    t = jnp.tanh(GELU_C * (a + 0.044715 * (sq * a)))
    return 0.5 * (1.0 + t) + (0.5 * a) * (1.0 - t * t) * (GELU_C * (1.0 + (3.0 * 0.044715) * sq))


def column_of(row, size):
    return jnp.transpose(jnp.broadcast_to(row, (size, size)))


def joined_row(ref, i, size):
    per = size // ref.shape[1]
    return jnp.concatenate([ref[pl.ds(i * per + k, 1), :] for k in range(per)], axis=1)


def row_of(col, size):
    eye = lax.broadcasted_iota(jnp.int32, (size, size), 0) == lax.broadcasted_iota(jnp.int32, (size, size), 1)
    return jnp.sum(jnp.where(eye, jnp.broadcast_to(col, (size, size)), 0.0), axis=0, keepdims=True)


def token_kernel(
    n_stage, tok_ref, lab_ref, emb_hbm, wup_hbm, wdn_hbm,
    n_out, st_out, xs_out, gs_out, dx_out, ids_out, rank_out, lab_out, starts_out,
    wup, wdn, emb, z_buf, xs, gs, pre, n_loc, st_loc, gat,
    loc_sem, wsend, upr, dnr, xsend, xrecv, gsend, grecv, nsend, nrecv, ssend, srecv, dsend, drecv,
):
    me = lax.axis_index("stage")
    n_chip = n_stage // 2
    chip, core = me // 2, lax.rem(me, 2)
    sib = chip * 2 + (1 - core)
    right = lax.rem(chip + 1, n_chip) * 2 + core
    left = lax.rem(chip + n_chip - 1, n_chip) * 2 + core
    far = lax.rem(chip + 2, n_chip) * 2 + core
    peers = [lax.rem(me + d, n_stage) for d in range(1, n_stage)]
    tok_n, dim = n_loc.shape
    vocab = emb.shape[0]
    total = n_stage * tok_n
    scale = dim ** -0.5

    load_up = pltpu.make_async_copy(wup_hbm, wup.at[me], loc_sem.at[0])
    load_dn = pltpu.make_async_copy(wdn_hbm, wdn.at[me], loc_sem.at[1])
    load_emb = pltpu.make_async_copy(emb_hbm, emb, loc_sem.at[2])
    load_up.start()
    load_dn.start()
    load_emb.start()

    barrier = pltpu.get_barrier_semaphore()
    for peer in peers:
        pl.semaphore_signal(barrier, inc=1, device_id={"stage": peer}, device_id_type=MESH)
    pl.semaphore_wait(barrier, n_stage - 1)
    load_up.wait()
    load_dn.wait()

    def up_copy(i, slot, dst):
        return pltpu.make_async_remote_copy(
            wup.at[slot], wup.at[slot], wsend.at[i], upr.at[slot], device_id={"stage": dst}, device_id_type=MESH)

    def dn_copy(i, slot, dst):
        return pltpu.make_async_remote_copy(
            wdn.at[slot], wdn.at[slot], wsend.at[i], dnr.at[slot], device_id={"stage": dst}, device_id_type=MESH)

    first = [up_copy(0, me, right), dn_copy(1, me, left), dn_copy(2, me, right), up_copy(3, me, left),
             up_copy(4, me, sib), dn_copy(5, me, sib)]
    for copy in first:
        copy.start()

    tok_row = jnp.concatenate([joined_row(tok_ref, i, tok_n) for i in range(n_stage)], axis=0)
    pos = lax.broadcasted_iota(jnp.int32, (n_stage, tok_n), 0) * tok_n + lax.broadcasted_iota(jnp.int32, (n_stage, tok_n), 1)
    key_row = tok_row * total + pos
    lane = lax.broadcasted_iota(jnp.int32, (tok_n, tok_n), 1)
    key_cols = [column_of(key_row[j:j + 1, :], tok_n) for j in range(n_stage)]
    tok_cols = [column_of(tok_row[j:j + 1, :], tok_n) for j in range(n_stage)]
    rank_rows = []
    for i in range(n_stage):
        acc = jnp.zeros((tok_n, tok_n), jnp.int32)
        for j in range(n_stage):
            acc = acc + jnp.where(key_cols[j] < key_row[i:i + 1, :], 1, 0)
        rank_rows.append(jnp.sum(acc, axis=0, keepdims=True))
    rank_cols = [column_of(r, tok_n) for r in rank_rows]
    for c in range(n_stage):
        acc = jnp.zeros((tok_n, tok_n), jnp.int32)
        for j in range(n_stage):
            acc = acc + jnp.where(rank_cols[j] == lane + c * tok_n, tok_cols[j], 0)
        ids_out[c] = jnp.broadcast_to(jnp.sum(acc, axis=0, keepdims=True), (8, tok_n))
    acc = jnp.zeros((tok_n, tok_n), jnp.int32)
    for j in range(n_stage):
        acc = acc + jnp.where(tok_cols[j] < lane * EMB_BLOCK, 1, 0)
    starts_out[...] = jnp.sum(acc, axis=0, keepdims=True)
    for i in range(n_stage):
        rank_out[i:i + 1, :] = rank_rows[i]
        lab_out[i:i + 1, :] = joined_row(lab_ref, i, tok_n)

    load_emb.wait()
    pick = jnp.concatenate(
        [column_of(joined_row(tok_ref, me, tok_n), tok_n), column_of(joined_row(lab_ref, me, tok_n), tok_n)], axis=0)
    lane2 = lax.broadcasted_iota(jnp.int32, (2 * tok_n, tok_n), 1)

    def blocks(body):
        full = vocab // HEAD_BLOCK

        def step(i, carry):
            body(pl.multiple_of(i * HEAD_BLOCK, HEAD_BLOCK), HEAD_BLOCK)
            return carry

        lax.fori_loop(0, full, step, 0)
        if vocab % HEAD_BLOCK:
            body(full * HEAD_BLOCK, vocab % HEAD_BLOCK)

    gat[...] = jnp.zeros_like(gat)

    def gather_block(v0, size):
        hot = jnp.concatenate(
            [jnp.where(pick == lane2 + (v0 + j * tok_n), 1.0, 0.0).astype(BF16) for j in range(size // tok_n)], axis=1)
        gat[...] += dot_nn(hot, emb[pl.ds(v0, size), :])

    blocks(gather_block)
    x0 = gat[0:tok_n, :].astype(BF16)
    lab_rows = gat[tok_n:2 * tok_n, :]
    lab_bf = lab_rows.astype(BF16)

    up_copy(0, left, sib).wait_recv()
    second = [up_copy(6, left, right), up_copy(7, left, sib)]
    second[0].start()
    second[1].start()
    dn_copy(0, right, sib).wait_recv()
    second += [dn_copy(8, right, left), dn_copy(9, right, sib)]
    second[2].start()
    second[3].start()
    dn_copy(0, left, sib).wait_recv()
    second.append(dn_copy(10, left, sib))
    second[4].start()
    up_copy(0, right, sib).wait_recv()
    second.append(up_copy(11, right, sib))
    second[5].start()
    up_copy(0, far, sib).wait_recv()
    second.append(up_copy(12, far, sib))
    second[6].start()
    dn_copy(0, far, sib).wait_recv()
    second.append(dn_copy(13, far, sib))
    second[7].start()

    def x_copy(layer):
        return pltpu.make_async_remote_copy(
            xs.at[layer], xs_out.at[me], xsend.at[layer], xrecv.at[me], device_id={"stage": layer}, device_id_type=MESH)

    def g_copy(layer):
        return pltpu.make_async_remote_copy(
            gs.at[layer + 1], gs_out.at[me], gsend.at[layer], grecv.at[me], device_id={"stage": layer}, device_id_type=MESH)

    own_x = pltpu.make_async_copy(xs.at[me], xs_out.at[me], loc_sem.at[0])
    own_g = pltpu.make_async_copy(gs.at[me + 1], gs_out.at[me], loc_sem.at[1])

    xs[0] = x0

    def forward(layer, carry):
        @pl.when(lax.rem(layer, 2) != core)
        def _():
            up_copy(0, layer, sib).wait_recv()
            dn_copy(0, layer, sib).wait_recv()

        x = xs[layer]
        a = dot_nn(x, wup[layer]).astype(BF16)
        pre[layer] = a
        h = gelu_value(a.astype(F32)).astype(BF16)
        xs[layer + 1] = (x.astype(F32) + dot_nn(h, wdn[layer])).astype(BF16)

        @pl.when(layer != me)
        def _():
            x_copy(layer).start()

        @pl.when(layer == me)
        def _():
            own_x.start()

        return carry

    lax.fori_loop(0, n_stage, forward, 0)

    x_last = xs[n_stage].astype(F32)
    inv = lax.rsqrt(jnp.mean(x_last * x_last, axis=-1, keepdims=True) + 1e-6)
    n_val = (x_last * inv).astype(BF16)
    n_loc[...] = n_val

    def spread(src, dst, send, recv):
        return [pltpu.make_async_remote_copy(src, dst.at[me], send.at[d], recv.at[me], device_id={"stage": peer},
                                             device_id_type=MESH) for d, peer in enumerate(peers)]

    def stat_block(v0, size):
        z = (dot_nt(n_loc[...], emb[pl.ds(v0, size), :]) * scale).astype(BF16)
        z_buf[:, pl.ds(v0, size)] = z
        parts = [z[:, j * tok_n:(j + 1) * tok_n].astype(F32) for j in range(size // tok_n)]
        m_old = gat[0:tok_n, :]
        m_new = functools.reduce(jnp.maximum, parts, m_old)
        s_new = gat[tok_n:2 * tok_n, :] * jnp.exp2((m_old - m_new) * LOG2E)
        for part in parts:
            s_new = s_new + jnp.exp2((part - m_new) * LOG2E)
        gat[0:tok_n, :] = m_new
        gat[tok_n:2 * tok_n, :] = s_new

    gat[0:tok_n, :] = jnp.full((tok_n, dim), -1e30, F32)
    gat[tok_n:2 * tok_n, :] = jnp.zeros((tok_n, dim), F32)
    send_n = spread(n_loc, n_out, nsend, nrecv)
    for copy in send_n:
        copy.start()
    own_n = pltpu.make_async_copy(n_loc, n_out.at[me], loc_sem.at[2])
    own_n.start()
    blocks(stat_block)
    m_lane = gat[0:tok_n, :]
    m_tok = jnp.max(m_lane, axis=-1, keepdims=True)
    s_tok = jnp.sum(gat[tok_n:2 * tok_n, :] * jnp.exp2((m_lane - m_tok) * LOG2E), axis=-1, keepdims=True)
    lse = m_tok + jnp.log(s_tok)
    level = lse * LOG2E + math.log2(total)
    z_pair = (dot_nt(n_val, lab_bf) * scale).astype(BF16).astype(F32)
    eye = lax.broadcasted_iota(jnp.int32, (tok_n, tok_n), 0) == lane
    z_lab = jnp.sum(jnp.where(eye, z_pair, 0.0), axis=-1, keepdims=True)
    p_lab = jnp.exp2(z_lab * LOG2E - level)
    d_lab = (p_lab - 1.0 / total).astype(BF16).astype(F32)
    p_lab = p_lab.astype(BF16).astype(F32)
    st_loc[...] = jnp.concatenate(
        [row_of(level, tok_n), row_of(d_lab, tok_n), row_of(lse - z_lab, tok_n), jnp.zeros((5, tok_n), F32)], axis=0)
    level_full = jnp.broadcast_to(level, (tok_n, tok_n))

    gat[0:tok_n, :] = (d_lab - p_lab) * lab_rows
    send_s = spread(st_loc, st_out, ssend, srecv)
    for copy in send_s:
        copy.start()
    own_s = pltpu.make_async_copy(st_loc, st_out.at[me], loc_sem.at[3])
    own_s.start()

    def grad_block(v0, size):
        parts = []
        for j in range(size // tok_n):
            z = z_buf[:, pl.ds(v0 + j * tok_n, tok_n)].astype(F32)
            parts.append(jnp.exp2(z * LOG2E - level_full).astype(BF16))
        gat[0:tok_n, :] += dot_nn(jnp.concatenate(parts, axis=1), emb[pl.ds(v0, size), :])

    blocks(grad_block)
    dn = (gat[0:tok_n, :] * scale).astype(BF16).astype(F32)
    corr = jnp.mean(dn * x_last, axis=-1, keepdims=True)
    gs[n_stage] = (inv * dn - x_last * (inv * inv * inv * corr)).astype(BF16)

    def backward(i, carry):
        layer = n_stage - 1 - i
        g = gs[layer + 1]
        dh = dot_nt(g, wdn[layer]).astype(BF16).astype(F32)
        da = (dh * gelu_slope(pre[layer].astype(F32))).astype(BF16)
        gs[layer] = (g.astype(F32) + dot_nt(da, wup[layer])).astype(BF16)

        @pl.when(layer != me)
        def _():
            g_copy(layer).start()

        @pl.when(layer == me)
        def _():
            own_g.start()

        return carry

    lax.fori_loop(0, n_stage, backward, 0)
    send_d = spread(gs.at[0], dx_out, dsend, drecv)
    for copy in send_d:
        copy.start()
    own_d = pltpu.make_async_copy(gs.at[0], dx_out.at[me], loc_sem.at[4])
    own_d.start()

    for copy in first + second + send_n + send_s:
        copy.wait_send()
    for copy in (own_x, own_g, own_n, own_s, own_d):
        copy.wait()
    for d, peer in enumerate(peers):
        pltpu.make_async_remote_copy(xs.at[peer], xs_out.at[peer], xsend.at[peer], xrecv.at[peer],
                                     device_id={"stage": peer}, device_id_type=MESH).wait()
        pltpu.make_async_remote_copy(gs.at[peer + 1], gs_out.at[peer], gsend.at[peer], grecv.at[peer],
                                     device_id={"stage": peer}, device_id_type=MESH).wait()
        for src, dst, send, recv in ((n_loc, n_out, nsend, nrecv), (st_loc, st_out, ssend, srecv)):
            pltpu.make_async_remote_copy(src, dst.at[peer], send.at[d], recv.at[peer],
                                         device_id={"stage": peer}, device_id_type=MESH).wait_recv()
        pltpu.make_async_remote_copy(gs.at[0], dx_out.at[peer], dsend.at[d], drecv.at[peer],
                                     device_id={"stage": peer}, device_id_type=MESH).wait_recv()
    for copy in send_d:
        copy.wait_send()


def weight_kernel(x_ref, g_ref, wup_ref, wdn_ref, st_ref, gup_ref, gdn_ref, loss_ref):
    n_stage, tok_n, _ = x_ref.shape
    step = 2

    def body(i, carry):
        x = jnp.concatenate([x_ref[step * i + k] for k in range(step)], axis=0)
        g = jnp.concatenate([g_ref[step * i + k] for k in range(step)], axis=0)
        a = dot_nn(x, wup_ref[...]).astype(BF16).astype(F32)
        sq = a * a
        t = jnp.tanh(GELU_C * (a + 0.044715 * (sq * a)))
        cdf = 0.5 * (1.0 + t)
        h = (a * cdf).astype(BF16)
        slope = cdf + (0.5 * a) * (1.0 - t * t) * (GELU_C * (1.0 + (3.0 * 0.044715) * sq))
        dh = dot_nt(g, wdn_ref[...]).astype(BF16).astype(F32)
        da = (dh * slope).astype(BF16)
        gup_ref[...] += dot_tn(x, da)
        gdn_ref[...] += dot_tn(h, g)
        return carry

    gup_ref[...] = jnp.zeros_like(gup_ref)
    gdn_ref[...] = jnp.zeros_like(gdn_ref)
    lax.fori_loop(0, n_stage // step, body, 0)
    loss_ref[0] = jnp.sum(st_ref[:, 2, :]) * (1.0 / (n_stage * tok_n))


def table_kernel(starts_sm, emb_ref, n_ref, st_ref, lab_ref, dx_ref, ids_ref, rank_ref, out_ref, n_t, level, d_lab, lab16, dxs):
    n_chunk, tok_n, dim = n_ref.shape
    total = n_chunk * tok_n
    blk = pl.program_id(0)
    rows = out_ref.shape[0]
    scale = dim ** -0.5

    @pl.when(blk == 0)
    def _():
        row_id = lax.broadcasted_iota(jnp.int32, (tok_n, tok_n), 0)
        for i in range(n_chunk):
            cols = slice(i * tok_n, (i + 1) * tok_n)
            n_t[:, cols] = jnp.transpose(n_ref[i])
            level[:, cols] = jnp.broadcast_to(st_ref[i, 0:1, :], (8, tok_n))
            d_lab[:, cols] = jnp.broadcast_to(st_ref[i, 1:2, :], (16, tok_n)).astype(BF16)
        for c in range(n_chunk):
            acc = jnp.zeros((tok_n, dim), F32)
            for i in range(n_chunk):
                hot = jnp.where(rank_ref[i:i + 1, :] == row_id + c * tok_n, 1.0, 0.0).astype(BF16)
                acc = acc + dot_nn(hot, dx_ref[i])
            dxs[c] = acc.astype(BF16)

    wide = 2 * tok_n
    e = emb_ref[...]
    base = blk * rows
    acc = jnp.zeros((rows, dim), F32)
    row16 = lax.broadcasted_iota(jnp.int16, (rows, wide), 0)
    for t in range(total // wide):
        cols = slice(t * wide, (t + 1) * wide)
        z = (dot_nn(e, n_t[:, cols]) * scale).astype(BF16).astype(F32)
        p = jnp.exp2(z * LOG2E - level[0:1, cols]).astype(BF16)
        lab = jnp.concatenate([lab_ref[2 * t:2 * t + 1, :], lab_ref[2 * t + 1:2 * t + 2, :]], axis=1) - base
        lab = jnp.broadcast_to(lab, (16, wide)).astype(jnp.int16)
        dz = jnp.where(row16 == lab[0:1, :], d_lab[0:1, cols], p)
        nn = jnp.concatenate([n_ref[2 * t], n_ref[2 * t + 1]], axis=0)
        acc = acc + dot_nn(dz, nn)

    row32 = lax.broadcasted_iota(jnp.int32, (rows, tok_n), 0)

    def token_term(c):
        hot = jnp.where(row32 == ids_ref[c, 0:1, :] - base, 1.0, 0.0).astype(BF16)
        return dot_nn(hot, dxs[c])

    first = jnp.minimum(starts_sm[0, blk] // tok_n, n_chunk - 1)
    last = (starts_sm[0, blk + 1] + tok_n - 1) // tok_n
    out_ref[...] = acc * scale + token_term(first)

    def more(c, carry):
        out_ref[...] += token_term(c)
        return carry

    lax.fori_loop(first + 1, last, more, 0)


def solution(mesh):
    n_stage = mesh.shape["stage"]

    def device_fn(tokens, labels, emb_table, w_up, w_down):
        vocab, dim = emb_table.shape
        ffn = w_up.shape[2]
        total = tokens.shape[0] * tokens.shape[1]
        tok_n = total // n_stage
        w_up, w_down = w_up[0], w_down[0]
        vmem = pl.BlockSpec(memory_space=pltpu.VMEM)
        hbm = pl.BlockSpec(memory_space=pl.ANY)
        dma = pltpu.SemaphoreType.DMA
        n_blk = pl.cdiv(vocab, EMB_BLOCK)
        act = jax.ShapeDtypeStruct((n_stage, tok_n, dim), BF16)
        n_all, st_all, xs_all, gs_all, dx_all, ids, rank, lab8, starts = pl.pallas_call(
            functools.partial(token_kernel, n_stage),
            out_shape=[act, jax.ShapeDtypeStruct((n_stage, 8, tok_n), F32), act, act, act,
                       jax.ShapeDtypeStruct((n_stage, 8, tok_n), jnp.int32),
                       jax.ShapeDtypeStruct((n_stage, tok_n), jnp.int32), jax.ShapeDtypeStruct((n_stage, tok_n), jnp.int32),
                       jax.ShapeDtypeStruct((1, tok_n), jnp.int32)],
            in_specs=[vmem, vmem, hbm, hbm, hbm],
            out_specs=[hbm] * 5 + [vmem] * 4,
            scratch_shapes=[
                pltpu.VMEM((n_stage, dim, ffn), BF16), pltpu.VMEM((n_stage, ffn, dim), BF16),
                pltpu.VMEM((vocab, dim), BF16), pltpu.VMEM((tok_n, vocab), BF16),
                pltpu.VMEM((n_stage + 1, tok_n, dim), BF16), pltpu.VMEM((n_stage + 1, tok_n, dim), BF16),
                pltpu.VMEM((n_stage, tok_n, ffn), BF16), pltpu.VMEM((tok_n, dim), BF16),
                pltpu.VMEM((8, tok_n), F32), pltpu.VMEM((2 * tok_n, dim), F32),
                dma((5,)), dma((14,))] + [dma((n_stage,))] * 12,
            compiler_params=pltpu.CompilerParams(collective_id=0, has_side_effects=True, vmem_limit_bytes=VMEM_BYTES),
            name="token_pass",
        )(tokens, labels, emb_table, w_up, w_down)

        grad_up, grad_down, loss = pl.pallas_call(
            weight_kernel,
            out_shape=[jax.ShapeDtypeStruct((dim, ffn), F32), jax.ShapeDtypeStruct((ffn, dim), F32),
                       jax.ShapeDtypeStruct((1,), F32)],
            in_specs=[vmem] * 5, out_specs=[vmem, vmem, pl.BlockSpec(memory_space=pltpu.SMEM)],
            compiler_params=pltpu.CompilerParams(vmem_limit_bytes=VMEM_BYTES),
            name="weight_grads",
        )(xs_all, gs_all, w_up, w_down, st_all)

        whole3 = lambda i, s: (0, 0, 0)
        whole2 = lambda i, s: (0, 0)
        grad_emb = pl.pallas_call(
            table_kernel,
            grid_spec=pltpu.PrefetchScalarGridSpec(
                num_scalar_prefetch=1, grid=(n_blk,),
                in_specs=[pl.BlockSpec((EMB_BLOCK, dim), lambda i, s: (i, 0)),
                          pl.BlockSpec((n_stage, tok_n, dim), whole3), pl.BlockSpec((n_stage, 8, tok_n), whole3),
                          pl.BlockSpec((n_stage, tok_n), whole2), pl.BlockSpec((n_stage, tok_n, dim), whole3),
                          pl.BlockSpec((n_stage, 8, tok_n), whole3), pl.BlockSpec((n_stage, tok_n), whole2)],
                out_specs=pl.BlockSpec((EMB_BLOCK, dim), lambda i, s: (i, 0)),
                scratch_shapes=[pltpu.VMEM((dim, total), BF16), pltpu.VMEM((8, total), F32), pltpu.VMEM((16, total), BF16),
                                pltpu.VMEM((16, total), jnp.int16), pltpu.VMEM((n_stage, tok_n, dim), BF16)]),
            out_shape=jax.ShapeDtypeStruct((vocab, dim), F32),
            compiler_params=pltpu.CompilerParams(dimension_semantics=("arbitrary",), vmem_limit_bytes=VMEM_BYTES),
            name="table_grad",
        )(starts, emb_table, n_all, st_all, lab8, dx_all, ids, rank)
        return loss, grad_up[None], grad_down[None], grad_emb

    return jax.shard_map(
        device_fn, mesh=mesh,
        in_specs=(P("dp", None), P("dp", None), P(None, None), P("stage", None, None), P("stage", None, None)),
        out_specs=(P("dp"), P(("dp", "stage"), None, None), P(("dp", "stage"), None, None), P("dp", None)),
        check_vma=False)
```

```python
import functools
import math

import jax
import jax.numpy as jnp
from jax import lax
from jax.experimental import pallas as pl
from jax.experimental.pallas import tpu as pltpu
from jax.sharding import PartitionSpec as P

MESH = pl.DeviceIdType.MESH
F32 = jnp.float32
BF16 = jnp.bfloat16
LOG2E = math.log2(math.e)
LN2 = math.log(2.0)
GELU_C = math.sqrt(2.0 / math.pi)
HEAD_BLOCK = 2048
TABLE_BLOCK = 1024
EMB_BLOCK = 2048
VMEM_BYTES = 60 * 1024 * 1024


def dot_nn(a, b):
    return lax.dot_general(a, b, (((1,), (0,)), ((), ())), preferred_element_type=F32)


def dot_nt(a, b):
    return lax.dot_general(a, b, (((1,), (1,)), ((), ())), preferred_element_type=F32)


def dot_tn(a, b):
    return lax.dot_general(a, b, (((0,), (0,)), ((), ())), preferred_element_type=F32)


def gelu_value(a):
    return a * (0.5 * (1.0 + jnp.tanh(GELU_C * (a + 0.044715 * (a * a * a)))))


def gelu_slope(a):
    sq = a * a
    t = jnp.tanh(GELU_C * (a + 0.044715 * (sq * a)))
    return 0.5 * (1.0 + t) + (0.5 * a) * (1.0 - t * t) * (GELU_C * (1.0 + (3.0 * 0.044715) * sq))


def column_of(row, size):
    return jnp.transpose(jnp.broadcast_to(row, (size, size)))


def joined_row(ref, i, size):
    per = size // ref.shape[1]
    return jnp.concatenate([ref[pl.ds(i * per + k, 1), :] for k in range(per)], axis=1)


def row_of(col, size):
    eye = lax.broadcasted_iota(jnp.int32, (size, size), 0) == lax.broadcasted_iota(jnp.int32, (size, size), 1)
    return jnp.sum(jnp.where(eye, jnp.broadcast_to(col, (size, size)), 0.0), axis=0, keepdims=True)


def token_kernel(
    n_stage, tok_ref, lab_ref, emb_hbm, wup_hbm, wdn_hbm,
    st_out, xs_out, gs_out, dx_out, table_out, ids_out, rank_out, starts_out,
    wup, wdn, emb, z_buf, xs, gs, pre, n_all, st_all, gat, n_t, level_t, d_lab_t, table,
    loc_sem, wsend, upr, dnr, xsend, xrecv, gsend, grecv, nsend, nrecv, ssend, srecv, dsend, drecv, tsend, trecv, tloc,
):
    me = lax.axis_index("stage")
    n_chip = n_stage // 2
    chip, core = me // 2, lax.rem(me, 2)
    sib = chip * 2 + (1 - core)
    right = lax.rem(chip + 1, n_chip) * 2 + core
    left = lax.rem(chip + n_chip - 1, n_chip) * 2 + core
    far = lax.rem(chip + 2, n_chip) * 2 + core
    peers = [lax.rem(me + d, n_stage) for d in range(1, n_stage)]
    _, tok_n, dim = n_all.shape
    vocab = emb.shape[0]
    total = n_stage * tok_n
    scale = dim ** -0.5

    load_up = pltpu.make_async_copy(wup_hbm, wup.at[me], loc_sem.at[0])
    load_dn = pltpu.make_async_copy(wdn_hbm, wdn.at[me], loc_sem.at[1])
    load_emb = pltpu.make_async_copy(emb_hbm, emb, loc_sem.at[2])
    load_up.start()
    load_dn.start()
    load_emb.start()

    barrier = pltpu.get_barrier_semaphore()
    for peer in peers:
        pl.semaphore_signal(barrier, inc=1, device_id={"stage": peer}, device_id_type=MESH)
    pl.semaphore_wait(barrier, n_stage - 1)
    load_up.wait()
    load_dn.wait()

    def up_copy(i, slot, dst):
        return pltpu.make_async_remote_copy(
            wup.at[slot], wup.at[slot], wsend.at[i], upr.at[slot], device_id={"stage": dst}, device_id_type=MESH)

    def dn_copy(i, slot, dst):
        return pltpu.make_async_remote_copy(
            wdn.at[slot], wdn.at[slot], wsend.at[i], dnr.at[slot], device_id={"stage": dst}, device_id_type=MESH)

    first = [up_copy(0, me, right), dn_copy(1, me, left), dn_copy(2, me, right), up_copy(3, me, left),
             up_copy(4, me, sib), dn_copy(5, me, sib)]
    for copy in first:
        copy.start()

    tok_row = jnp.concatenate([joined_row(tok_ref, i, tok_n) for i in range(n_stage)], axis=0)
    pos = lax.broadcasted_iota(jnp.int32, (n_stage, tok_n), 0) * tok_n + lax.broadcasted_iota(jnp.int32, (n_stage, tok_n), 1)
    key_row = tok_row * total + pos
    lane = lax.broadcasted_iota(jnp.int32, (tok_n, tok_n), 1)
    key_cols = [column_of(key_row[j:j + 1, :], tok_n) for j in range(n_stage)]
    tok_cols = [column_of(tok_row[j:j + 1, :], tok_n) for j in range(n_stage)]
    rank_rows = []
    for i in range(n_stage):
        acc = jnp.zeros((tok_n, tok_n), jnp.int32)
        for j in range(n_stage):
            acc = acc + jnp.where(key_cols[j] < key_row[i:i + 1, :], 1, 0)
        rank_rows.append(jnp.sum(acc, axis=0, keepdims=True))
    rank_cols = [column_of(r, tok_n) for r in rank_rows]
    for c in range(n_stage):
        acc = jnp.zeros((tok_n, tok_n), jnp.int32)
        for j in range(n_stage):
            acc = acc + jnp.where(rank_cols[j] == lane + c * tok_n, tok_cols[j], 0)
        ids_out[c] = jnp.broadcast_to(jnp.sum(acc, axis=0, keepdims=True), (8, tok_n))
    ids_out[n_stage] = jnp.full((8, tok_n), -1, jnp.int32)
    acc = jnp.zeros((tok_n, tok_n), jnp.int32)
    for j in range(n_stage):
        acc = acc + jnp.where(tok_cols[j] < lane * EMB_BLOCK, 1, 0)
    starts_out[...] = jnp.sum(acc, axis=0, keepdims=True)
    for i in range(n_stage):
        rank_out[i:i + 1, :] = rank_rows[i]

    load_emb.wait()
    pick = jnp.concatenate(
        [column_of(joined_row(tok_ref, me, tok_n), tok_n), column_of(joined_row(lab_ref, me, tok_n), tok_n)], axis=0)
    lane2 = lax.broadcasted_iota(jnp.int32, (2 * tok_n, tok_n), 1)

    def blocks(body):
        full = vocab // HEAD_BLOCK

        def step(i, carry):
            body(pl.multiple_of(i * HEAD_BLOCK, HEAD_BLOCK), HEAD_BLOCK)
            return carry

        lax.fori_loop(0, full, step, 0)
        if vocab % HEAD_BLOCK:
            body(full * HEAD_BLOCK, vocab % HEAD_BLOCK)

    gat[...] = jnp.zeros_like(gat)

    def gather_block(v0, size):
        hot = jnp.concatenate(
            [jnp.where(pick == lane2 + (v0 + j * tok_n), 1.0, 0.0).astype(BF16) for j in range(size // tok_n)], axis=1)
        gat[...] += dot_nn(hot, emb[pl.ds(v0, size), :])

    blocks(gather_block)
    x0 = gat[0:tok_n, :].astype(BF16)
    lab_rows = gat[tok_n:2 * tok_n, :]
    lab_bf = lab_rows.astype(BF16)

    up_copy(0, left, sib).wait_recv()
    second = [up_copy(6, left, right), up_copy(7, left, sib)]
    second[0].start()
    second[1].start()
    dn_copy(0, right, sib).wait_recv()
    second += [dn_copy(8, right, left), dn_copy(9, right, sib)]
    second[2].start()
    second[3].start()
    dn_copy(0, left, sib).wait_recv()
    second.append(dn_copy(10, left, sib))
    second[4].start()
    up_copy(0, right, sib).wait_recv()
    second.append(up_copy(11, right, sib))
    second[5].start()
    up_copy(0, far, sib).wait_recv()
    second.append(up_copy(12, far, sib))
    second[6].start()
    dn_copy(0, far, sib).wait_recv()
    second.append(dn_copy(13, far, sib))
    second[7].start()

    def x_copy(layer):
        return pltpu.make_async_remote_copy(
            xs.at[layer], xs_out.at[me], xsend.at[layer], xrecv.at[me], device_id={"stage": layer}, device_id_type=MESH)

    def g_copy(layer):
        return pltpu.make_async_remote_copy(
            gs.at[layer + 1], gs_out.at[me], gsend.at[layer], grecv.at[me], device_id={"stage": layer}, device_id_type=MESH)

    own_x = pltpu.make_async_copy(xs.at[me], xs_out.at[me], loc_sem.at[0])
    own_g = pltpu.make_async_copy(gs.at[me + 1], gs_out.at[me], loc_sem.at[1])

    xs[0] = x0

    def forward(layer, carry):
        @pl.when(lax.rem(layer, 2) != core)
        def _():
            up_copy(0, layer, sib).wait_recv()
            dn_copy(0, layer, sib).wait_recv()

        x = xs[layer]
        a = dot_nn(x, wup[layer]).astype(BF16)
        pre[layer] = a
        h = gelu_value(a.astype(F32)).astype(BF16)
        xs[layer + 1] = (x.astype(F32) + dot_nn(h, wdn[layer])).astype(BF16)

        @pl.when(layer != me)
        def _():
            x_copy(layer).start()

        @pl.when(layer == me)
        def _():
            own_x.start()

        return carry

    lax.fori_loop(0, n_stage, forward, 0)

    x_last = xs[n_stage].astype(F32)
    inv = lax.rsqrt(jnp.mean(x_last * x_last, axis=-1, keepdims=True) + 1e-6)
    n_val = (x_last * inv).astype(BF16)
    n_all[me] = n_val

    def spread(src, dst, send, recv):
        return [pltpu.make_async_remote_copy(src, dst.at[me], send.at[d], recv.at[me], device_id={"stage": peer},
                                             device_id_type=MESH) for d, peer in enumerate(peers)]

    def stat_block(v0, size):
        z = (dot_nt(n_all[me], emb[pl.ds(v0, size), :]) * scale).astype(BF16)
        z_buf[:, pl.ds(v0, size)] = z
        parts = [z[:, j * tok_n:(j + 1) * tok_n].astype(F32) for j in range(size // tok_n)]
        m_old = gat[0:tok_n, :]
        m_new = functools.reduce(jnp.maximum, parts, m_old)
        s_new = gat[tok_n:2 * tok_n, :] * jnp.exp2((m_old - m_new) * LOG2E)
        for part in parts:
            s_new = s_new + jnp.exp2((part - m_new) * LOG2E)
        gat[0:tok_n, :] = m_new
        gat[tok_n:2 * tok_n, :] = s_new

    gat[0:tok_n, :] = jnp.full((tok_n, dim), -1e30, F32)
    gat[tok_n:2 * tok_n, :] = jnp.zeros((tok_n, dim), F32)
    send_n = spread(n_all.at[me], n_all, nsend, nrecv)
    for copy in send_n:
        copy.start()
    blocks(stat_block)
    m_lane = gat[0:tok_n, :]
    m_tok = jnp.max(m_lane, axis=-1, keepdims=True)
    s_tok = jnp.sum(gat[tok_n:2 * tok_n, :] * jnp.exp2((m_lane - m_tok) * LOG2E), axis=-1, keepdims=True)
    lse = m_tok + jnp.log(s_tok)
    level = lse * LOG2E + math.log2(total)
    z_pair = (dot_nt(n_val, lab_bf) * scale).astype(BF16).astype(F32)
    eye = lax.broadcasted_iota(jnp.int32, (tok_n, tok_n), 0) == lane
    z_lab = jnp.sum(jnp.where(eye, z_pair, 0.0), axis=-1, keepdims=True)
    p_lab = jnp.exp2(z_lab * LOG2E - level)
    d_lab = (p_lab - 1.0 / total).astype(BF16).astype(F32)
    p_lab = p_lab.astype(BF16).astype(F32)
    st_all[me] = jnp.concatenate(
        [row_of(level, tok_n), row_of(d_lab, tok_n), row_of(lse - z_lab, tok_n), jnp.zeros((5, tok_n), F32)], axis=0)
    level_full = jnp.broadcast_to(level, (tok_n, tok_n))

    gat[0:tok_n, :] = (d_lab - p_lab) * lab_rows
    send_s = spread(st_all.at[me], st_all, ssend, srecv)
    for copy in send_s:
        copy.start()

    def grad_block(v0, size):
        parts = []
        for j in range(size // tok_n):
            z = z_buf[:, pl.ds(v0 + j * tok_n, tok_n)].astype(F32)
            parts.append(jnp.exp2(z * LOG2E - level_full).astype(BF16))
        gat[0:tok_n, :] += dot_nn(jnp.concatenate(parts, axis=1), emb[pl.ds(v0, size), :])

    blocks(grad_block)
    dn = (gat[0:tok_n, :] * scale).astype(BF16).astype(F32)
    corr = jnp.mean(dn * x_last, axis=-1, keepdims=True)
    gs[n_stage] = (inv * dn - x_last * (inv * inv * inv * corr)).astype(BF16)

    def backward(i, carry):
        layer = n_stage - 1 - i
        g = gs[layer + 1]
        dh = dot_nt(g, wdn[layer]).astype(BF16).astype(F32)
        da = (dh * gelu_slope(pre[layer].astype(F32))).astype(BF16)
        gs[layer] = (g.astype(F32) + dot_nt(da, wup[layer])).astype(BF16)

        @pl.when(layer != me)
        def _():
            g_copy(layer).start()

        @pl.when(layer == me)
        def _():
            own_g.start()

        return carry

    lax.fori_loop(0, n_stage, backward, 0)
    send_d = spread(gs.at[0], dx_out, dsend, drecv)
    for copy in send_d:
        copy.start()
    own_d = pltpu.make_async_copy(gs.at[0], dx_out.at[me], loc_sem.at[4])
    own_d.start()

    for peer in peers:
        for buf, send, recv in ((n_all, nsend, nrecv), (st_all, ssend, srecv)):
            pltpu.make_async_remote_copy(buf.at[peer], buf.at[peer], send.at[0], recv.at[peer],
                                         device_id={"stage": peer}, device_id_type=MESH).wait_recv()
    own_s = pltpu.make_async_copy(st_all, st_out, loc_sem.at[3])
    own_s.start()
    for i in range(n_stage):
        cols = slice(i * tok_n, (i + 1) * tok_n)
        n_t[:, cols] = jnp.transpose(n_all[i])
        level_t[:, cols] = jnp.broadcast_to(st_all[i, 0:1, :], (8, tok_n))
        d_lab_t[:, cols] = jnp.broadcast_to(st_all[i, 1:2, :], (16, tok_n)).astype(BF16)
    half = vocab // 2
    wide = 2 * tok_n

    def table_copies(j, size):
        local = pl.ds(pl.multiple_of(j * TABLE_BLOCK, 16), size)
        rows = pl.ds(pl.multiple_of(core * half + j * TABLE_BLOCK, 16), size)
        return (pltpu.make_async_remote_copy(table.at[local], table_out.at[rows], tsend.at[j], trecv.at[j],
                                             device_id={"stage": sib}, device_id_type=MESH),
                pltpu.make_async_copy(table.at[local], table_out.at[rows], tloc.at[j]))

    def table_start(j, size):
        for copy in table_copies(j, size):
            copy.start()

    def table_block(j, size):
        base = pl.multiple_of(core * half + j * TABLE_BLOCK, 16)
        e = emb[pl.ds(base, size), :]
        row16 = lax.broadcasted_iota(jnp.int16, (size, wide), 0)
        acc = jnp.zeros((size, dim), F32)
        for t in range(total // wide):
            cols = slice(t * wide, (t + 1) * wide)
            z = (dot_nn(e, n_t[:, cols]) * scale).astype(BF16).astype(F32)
            p = jnp.exp2(z * LOG2E - level_t[0:1, cols]).astype(BF16)
            lab = jnp.concatenate([joined_row(lab_ref, 2 * t, tok_n), joined_row(lab_ref, 2 * t + 1, tok_n)], axis=1) - base
            lab = jnp.broadcast_to(lab, (16, wide)).astype(jnp.int16)
            dz = jnp.where(row16 == lab[0:1, :], d_lab_t[0:1, cols], p)
            acc = acc + dot_nn(dz, jnp.concatenate([n_all[2 * t], n_all[2 * t + 1]], axis=0))
        table[pl.ds(pl.multiple_of(j * TABLE_BLOCK, 16), size), :] = acc * scale

    full, tail = half // TABLE_BLOCK, half % TABLE_BLOCK

    def table_step(j, carry):
        @pl.when(j > 0)
        def _():
            table_start(j - 1, TABLE_BLOCK)

        table_block(j, TABLE_BLOCK)
        return carry

    lax.fori_loop(0, full, table_step, 0)
    table_start(full - 1, TABLE_BLOCK)
    if tail:
        table_block(full, tail)

    for copy in first + second + send_n + send_s:
        copy.wait_send()
    for copy in (own_x, own_g, own_s, own_d):
        copy.wait()
    for peer in peers:
        pltpu.make_async_remote_copy(xs.at[peer], xs_out.at[peer], xsend.at[peer], xrecv.at[peer],
                                     device_id={"stage": peer}, device_id_type=MESH).wait()
        pltpu.make_async_remote_copy(gs.at[peer + 1], gs_out.at[peer], gsend.at[peer], grecv.at[peer],
                                     device_id={"stage": peer}, device_id_type=MESH).wait()
        pltpu.make_async_remote_copy(gs.at[0], dx_out.at[peer], dsend.at[0], drecv.at[peer],
                                     device_id={"stage": peer}, device_id_type=MESH).wait_recv()
    for copy in send_d:
        copy.wait_send()
    if tail:
        table_start(full, tail)

    def table_wait(j, size):
        remote, local = table_copies(j, size)
        remote.wait_send()
        local.wait()
        rows = pl.ds(pl.multiple_of((1 - core) * half + j * TABLE_BLOCK, 16), size)
        pltpu.make_async_remote_copy(table.at[pl.ds(pl.multiple_of(j * TABLE_BLOCK, 16), size)], table_out.at[rows],
                                     tsend.at[j], trecv.at[j], device_id={"stage": sib}, device_id_type=MESH).wait_recv()

    def wait_step(j, carry):
        table_wait(j, TABLE_BLOCK)
        return carry

    lax.fori_loop(0, full, wait_step, 0)
    if tail:
        table_wait(full, tail)


def weight_kernel(x_ref, g_ref, wup_ref, wdn_ref, st_ref, gup_ref, gdn_ref, loss_ref):
    n_stage, tok_n, _ = x_ref.shape
    step = 2

    def body(i, carry):
        x = jnp.concatenate([x_ref[step * i + k] for k in range(step)], axis=0)
        g = jnp.concatenate([g_ref[step * i + k] for k in range(step)], axis=0)
        a = dot_nn(x, wup_ref[...]).astype(BF16).astype(F32)
        sq = a * a
        t = jnp.tanh(GELU_C * (a + 0.044715 * (sq * a)))
        cdf = 0.5 * (1.0 + t)
        h = (a * cdf).astype(BF16)
        slope = cdf + (0.5 * a) * (1.0 - t * t) * (GELU_C * (1.0 + (3.0 * 0.044715) * sq))
        dh = dot_nt(g, wdn_ref[...]).astype(BF16).astype(F32)
        da = (dh * slope).astype(BF16)
        gup_ref[...] += dot_tn(x, da)
        gdn_ref[...] += dot_tn(h, g)
        return carry

    gup_ref[...] = jnp.zeros_like(gup_ref)
    gdn_ref[...] = jnp.zeros_like(gdn_ref)
    lax.fori_loop(0, n_stage // step, body, 0)
    loss_ref[0] = jnp.sum(st_ref[:, 2, :]) * (1.0 / (n_stage * tok_n))


def table_kernel(starts_sm, part_ref, dx_ref, ids_ref, rank_ref, out_ref, dxs):
    n_chunk, tok_n, dim = dx_ref.shape
    blk = pl.program_id(0)
    rows = out_ref.shape[0]

    @pl.when(blk == 0)
    def _():
        row_id = lax.broadcasted_iota(jnp.int32, (tok_n, tok_n), 0)
        for c in range(n_chunk):
            acc = jnp.zeros((tok_n, dim), F32)
            for i in range(n_chunk):
                hot = jnp.where(rank_ref[i:i + 1, :] == row_id + c * tok_n, 1.0, 0.0).astype(BF16)
                acc = acc + dot_nn(hot, dx_ref[i])
            dxs[c] = acc.astype(BF16)
        dxs[n_chunk] = jnp.zeros((tok_n, dim), BF16)

    base = blk * rows
    row16 = lax.broadcasted_iota(jnp.int16, (rows, tok_n), 0)

    def hot_rows(c):
        ids = jnp.broadcast_to(ids_ref[c, 0:1, :] - base, (16, tok_n)).astype(jnp.int16)
        return jnp.where(row16 == ids[0:1, :], jnp.ones((), BF16), jnp.zeros((), BF16))

    first = jnp.minimum(starts_sm[0, blk] // tok_n, n_chunk - 1)
    last = (starts_sm[0, blk + 1] + tok_n - 1) // tok_n
    out_ref[...] = part_ref[...] + dot_nn(jnp.concatenate([hot_rows(first), hot_rows(first + 1)], axis=1),
                                          jnp.concatenate([dxs[first], dxs[first + 1]], axis=0))

    def more(c, carry):
        out_ref[...] += dot_nn(hot_rows(c), dxs[c])
        return carry

    lax.fori_loop(first + 2, last, more, 0)


def solution(mesh):
    n_stage = mesh.shape["stage"]

    def device_fn(tokens, labels, emb_table, w_up, w_down):
        vocab, dim = emb_table.shape
        ffn = w_up.shape[2]
        total = tokens.shape[0] * tokens.shape[1]
        tok_n = total // n_stage
        w_up, w_down = w_up[0], w_down[0]
        vmem = pl.BlockSpec(memory_space=pltpu.VMEM)
        hbm = pl.BlockSpec(memory_space=pl.ANY)
        dma = pltpu.SemaphoreType.DMA
        n_blk = pl.cdiv(vocab, EMB_BLOCK)
        act = jax.ShapeDtypeStruct((n_stage, tok_n, dim), BF16)
        st_all, xs_all, gs_all, dx_all, part, ids, rank, starts = pl.pallas_call(
            functools.partial(token_kernel, n_stage),
            out_shape=[jax.ShapeDtypeStruct((n_stage, 8, tok_n), F32), act, act, act,
                       jax.ShapeDtypeStruct((vocab, dim), F32),
                       jax.ShapeDtypeStruct((n_stage + 1, 8, tok_n), jnp.int32),
                       jax.ShapeDtypeStruct((n_stage, tok_n), jnp.int32), jax.ShapeDtypeStruct((1, tok_n), jnp.int32)],
            in_specs=[vmem, vmem, hbm, hbm, hbm],
            out_specs=[hbm] * 5 + [vmem] * 3,
            scratch_shapes=[
                pltpu.VMEM((n_stage, dim, ffn), BF16), pltpu.VMEM((n_stage, ffn, dim), BF16),
                pltpu.VMEM((vocab, dim), BF16), pltpu.VMEM((tok_n, vocab), BF16),
                pltpu.VMEM((n_stage + 1, tok_n, dim), BF16), pltpu.VMEM((n_stage + 1, tok_n, dim), BF16),
                pltpu.VMEM((n_stage, tok_n, ffn), BF16), pltpu.VMEM((n_stage, tok_n, dim), BF16),
                pltpu.VMEM((n_stage, 8, tok_n), F32), pltpu.VMEM((2 * tok_n, dim), F32),
                pltpu.VMEM((dim, total), BF16), pltpu.VMEM((8, total), F32), pltpu.VMEM((16, total), BF16),
                pltpu.VMEM((vocab // 2, dim), F32),
                dma((5,)), dma((14,))] + [dma((n_stage,))] * 12 + [dma((pl.cdiv(vocab // 2, TABLE_BLOCK),))] * 3,
            compiler_params=pltpu.CompilerParams(collective_id=0, has_side_effects=True, vmem_limit_bytes=VMEM_BYTES),
            name="token_pass",
        )(tokens, labels, emb_table, w_up, w_down)

        grad_up, grad_down, loss = pl.pallas_call(
            weight_kernel,
            out_shape=[jax.ShapeDtypeStruct((dim, ffn), F32), jax.ShapeDtypeStruct((ffn, dim), F32),
                       jax.ShapeDtypeStruct((1,), F32)],
            in_specs=[vmem] * 5, out_specs=[vmem, vmem, pl.BlockSpec(memory_space=pltpu.SMEM)],
            compiler_params=pltpu.CompilerParams(vmem_limit_bytes=VMEM_BYTES),
            name="weight_grads",
        )(xs_all, gs_all, w_up, w_down, st_all)

        whole3 = lambda i, s: (0, 0, 0)
        whole2 = lambda i, s: (0, 0)
        grad_emb = pl.pallas_call(
            table_kernel,
            grid_spec=pltpu.PrefetchScalarGridSpec(
                num_scalar_prefetch=1, grid=(n_blk,),
                in_specs=[pl.BlockSpec((EMB_BLOCK, dim), lambda i, s: (i, 0)), pl.BlockSpec((n_stage, tok_n, dim), whole3),
                          pl.BlockSpec((n_stage + 1, 8, tok_n), whole3), pl.BlockSpec((n_stage, tok_n), whole2)],
                out_specs=pl.BlockSpec((EMB_BLOCK, dim), lambda i, s: (i, 0)),
                scratch_shapes=[pltpu.VMEM((n_stage + 1, tok_n, dim), BF16)]),
            out_shape=jax.ShapeDtypeStruct((vocab, dim), F32),
            compiler_params=pltpu.CompilerParams(dimension_semantics=("arbitrary",), vmem_limit_bytes=VMEM_BYTES),
            name="table_grad",
        )(starts, part, dx_all, ids, rank)
        return loss, grad_up[None], grad_down[None], grad_emb

    return jax.shard_map(
        device_fn, mesh=mesh,
        in_specs=(P("dp", None), P("dp", None), P(None, None), P("stage", None, None), P("stage", None, None)),
        out_specs=(P("dp"), P(("dp", "stage"), None, None), P(("dp", "stage"), None, None), P("dp", None)),
        check_vma=False)
```

```python
import functools
import math

import jax
import jax.numpy as jnp
from jax import lax
from jax.experimental import pallas as pl
from jax.experimental.pallas import tpu as pltpu
from jax.sharding import PartitionSpec as P

MESH = pl.DeviceIdType.MESH
F32 = jnp.float32
BF16 = jnp.bfloat16
LOG2E = math.log2(math.e)
LN2 = math.log(2.0)
GELU_C = math.sqrt(2.0 / math.pi)
HEAD_BLOCK = 2048
TABLE_BLOCK = 1024
EMB_BLOCK = 1024
VMEM_BYTES = 60 * 1024 * 1024


def dot_nn(a, b):
    return lax.dot_general(a, b, (((1,), (0,)), ((), ())), preferred_element_type=F32)


def dot_nt(a, b):
    return lax.dot_general(a, b, (((1,), (1,)), ((), ())), preferred_element_type=F32)


def dot_tn(a, b):
    return lax.dot_general(a, b, (((0,), (0,)), ((), ())), preferred_element_type=F32)


def gelu_value(a):
    return a * (0.5 * (1.0 + jnp.tanh(GELU_C * (a + 0.044715 * (a * a * a)))))


def gelu_slope(a):
    sq = a * a
    t = jnp.tanh(GELU_C * (a + 0.044715 * (sq * a)))
    return 0.5 * (1.0 + t) + (0.5 * a) * (1.0 - t * t) * (GELU_C * (1.0 + (3.0 * 0.044715) * sq))


def column_of(row, size):
    return jnp.transpose(jnp.broadcast_to(row, (size, size)))


def joined_row(ref, i, size):
    per = size // ref.shape[1]
    return jnp.concatenate([ref[pl.ds(i * per + k, 1), :] for k in range(per)], axis=1)


def row_of(col, size):
    eye = lax.broadcasted_iota(jnp.int32, (size, size), 0) == lax.broadcasted_iota(jnp.int32, (size, size), 1)
    return jnp.sum(jnp.where(eye, jnp.broadcast_to(col, (size, size)), 0.0), axis=0, keepdims=True)


def token_kernel(
    n_stage, tok_ref, lab_ref, emb_hbm, wup_hbm, wdn_hbm,
    st_out, xs_out, gs_out, dx_out, table_out, ids_out, rank_out, starts_out,
    wup, wdn, emb, z_buf, xs, gs, pre, n_all, st_all, gat, n_t, level_t, d_lab_t, table,
    loc_sem, wsend, upr, dnr, xsend, xrecv, gsend, grecv, nsend, nrecv, ssend, srecv, dsend, drecv, tsend, trecv, tloc,
):
    me = lax.axis_index("stage")
    n_chip = n_stage // 2
    chip, core = me // 2, lax.rem(me, 2)
    sib = chip * 2 + (1 - core)
    right = lax.rem(chip + 1, n_chip) * 2 + core
    left = lax.rem(chip + n_chip - 1, n_chip) * 2 + core
    far = lax.rem(chip + 2, n_chip) * 2 + core
    peers = [lax.rem(me + d, n_stage) for d in range(1, n_stage)]
    _, tok_n, dim = n_all.shape
    vocab = emb.shape[0]
    total = n_stage * tok_n
    scale = dim ** -0.5

    load_up = pltpu.make_async_copy(wup_hbm, wup.at[me], loc_sem.at[0])
    load_dn = pltpu.make_async_copy(wdn_hbm, wdn.at[me], loc_sem.at[1])
    load_emb = pltpu.make_async_copy(emb_hbm, emb, loc_sem.at[2])
    load_up.start()
    load_dn.start()
    load_emb.start()

    barrier = pltpu.get_barrier_semaphore()
    for peer in peers:
        pl.semaphore_signal(barrier, inc=1, device_id={"stage": peer}, device_id_type=MESH)
    pl.semaphore_wait(barrier, n_stage - 1)
    load_up.wait()
    load_dn.wait()

    def up_copy(i, slot, dst):
        return pltpu.make_async_remote_copy(
            wup.at[slot], wup.at[slot], wsend.at[i], upr.at[slot], device_id={"stage": dst}, device_id_type=MESH)

    def dn_copy(i, slot, dst):
        return pltpu.make_async_remote_copy(
            wdn.at[slot], wdn.at[slot], wsend.at[i], dnr.at[slot], device_id={"stage": dst}, device_id_type=MESH)

    first = [up_copy(0, me, right), dn_copy(1, me, left), dn_copy(2, me, right), up_copy(3, me, left),
             up_copy(4, me, sib), dn_copy(5, me, sib)]
    for copy in first:
        copy.start()

    tok_row = jnp.concatenate([joined_row(tok_ref, i, tok_n) for i in range(n_stage)], axis=0)
    pos = lax.broadcasted_iota(jnp.int32, (n_stage, tok_n), 0) * tok_n + lax.broadcasted_iota(jnp.int32, (n_stage, tok_n), 1)
    key_row = tok_row * total + pos
    lane = lax.broadcasted_iota(jnp.int32, (tok_n, tok_n), 1)
    key_cols = [column_of(key_row[j:j + 1, :], tok_n) for j in range(n_stage)]
    tok_cols = [column_of(tok_row[j:j + 1, :], tok_n) for j in range(n_stage)]
    rank_rows = []
    for i in range(n_stage):
        acc = jnp.zeros((tok_n, tok_n), jnp.int32)
        for j in range(n_stage):
            acc = acc + jnp.where(key_cols[j] < key_row[i:i + 1, :], 1, 0)
        rank_rows.append(jnp.sum(acc, axis=0, keepdims=True))
    rank_cols = [column_of(r, tok_n) for r in rank_rows]
    for c in range(n_stage):
        acc = jnp.zeros((tok_n, tok_n), jnp.int32)
        for j in range(n_stage):
            acc = acc + jnp.where(rank_cols[j] == lane + c * tok_n, tok_cols[j], 0)
        ids_out[c] = jnp.broadcast_to(jnp.sum(acc, axis=0, keepdims=True), (8, tok_n))
    ids_out[n_stage] = jnp.full((8, tok_n), -1, jnp.int32)
    acc = jnp.zeros((tok_n, tok_n), jnp.int32)
    for j in range(n_stage):
        acc = acc + jnp.where(tok_cols[j] < lane * EMB_BLOCK, 1, 0)
    starts_out[...] = jnp.sum(acc, axis=0, keepdims=True)
    for i in range(n_stage):
        rank_out[i:i + 1, :] = rank_rows[i]

    load_emb.wait()
    pick = jnp.concatenate(
        [column_of(joined_row(tok_ref, me, tok_n), tok_n), column_of(joined_row(lab_ref, me, tok_n), tok_n)], axis=0)
    lane2 = lax.broadcasted_iota(jnp.int32, (2 * tok_n, tok_n), 1)

    def blocks(body):
        full = vocab // HEAD_BLOCK

        def step(i, carry):
            body(pl.multiple_of(i * HEAD_BLOCK, HEAD_BLOCK), HEAD_BLOCK)
            return carry

        lax.fori_loop(0, full, step, 0)
        if vocab % HEAD_BLOCK:
            body(full * HEAD_BLOCK, vocab % HEAD_BLOCK)

    gat[...] = jnp.zeros_like(gat)

    def gather_block(v0, size):
        hot = jnp.concatenate(
            [jnp.where(pick == lane2 + (v0 + j * tok_n), 1.0, 0.0).astype(BF16) for j in range(size // tok_n)], axis=1)
        gat[...] += dot_nn(hot, emb[pl.ds(v0, size), :])

    blocks(gather_block)
    x0 = gat[0:tok_n, :].astype(BF16)
    lab_rows = gat[tok_n:2 * tok_n, :]
    lab_bf = lab_rows.astype(BF16)

    up_copy(0, left, sib).wait_recv()
    second = [up_copy(6, left, right), up_copy(7, left, sib)]
    second[0].start()
    second[1].start()
    dn_copy(0, right, sib).wait_recv()
    second += [dn_copy(8, right, left), dn_copy(9, right, sib)]
    second[2].start()
    second[3].start()
    dn_copy(0, left, sib).wait_recv()
    second.append(dn_copy(10, left, sib))
    second[4].start()
    up_copy(0, right, sib).wait_recv()
    second.append(up_copy(11, right, sib))
    second[5].start()
    up_copy(0, far, sib).wait_recv()
    second.append(up_copy(12, far, sib))
    second[6].start()
    dn_copy(0, far, sib).wait_recv()
    second.append(dn_copy(13, far, sib))
    second[7].start()

    def x_copy(layer):
        return pltpu.make_async_remote_copy(
            xs.at[layer], xs_out.at[me], xsend.at[layer], xrecv.at[me], device_id={"stage": layer}, device_id_type=MESH)

    def g_copy(layer):
        return pltpu.make_async_remote_copy(
            gs.at[layer + 1], gs_out.at[me], gsend.at[layer], grecv.at[me], device_id={"stage": layer}, device_id_type=MESH)

    own_x = pltpu.make_async_copy(xs.at[me], xs_out.at[me], loc_sem.at[0])
    own_g = pltpu.make_async_copy(gs.at[me + 1], gs_out.at[me], loc_sem.at[1])

    xs[0] = x0

    def forward(layer, carry):
        @pl.when(lax.rem(layer, 2) != core)
        def _():
            up_copy(0, layer, sib).wait_recv()
            dn_copy(0, layer, sib).wait_recv()

        x = xs[layer]
        a = dot_nn(x, wup[layer]).astype(BF16)
        pre[layer] = a
        h = gelu_value(a.astype(F32)).astype(BF16)
        xs[layer + 1] = (x.astype(F32) + dot_nn(h, wdn[layer])).astype(BF16)

        @pl.when(layer != me)
        def _():
            x_copy(layer).start()

        @pl.when(layer == me)
        def _():
            own_x.start()

        return carry

    lax.fori_loop(0, n_stage, forward, 0)

    x_last = xs[n_stage].astype(F32)
    inv = lax.rsqrt(jnp.mean(x_last * x_last, axis=-1, keepdims=True) + 1e-6)
    n_val = (x_last * inv).astype(BF16)
    n_all[me] = n_val

    def spread(src, dst, send, recv):
        return [pltpu.make_async_remote_copy(src, dst.at[me], send.at[d], recv.at[me], device_id={"stage": peer},
                                             device_id_type=MESH) for d, peer in enumerate(peers)]

    def stat_block(v0, size):
        z = (dot_nt(n_all[me], emb[pl.ds(v0, size), :]) * scale).astype(BF16)
        z_buf[:, pl.ds(v0, size)] = z
        parts = [z[:, j * tok_n:(j + 1) * tok_n].astype(F32) for j in range(size // tok_n)]
        m_old = gat[0:tok_n, :]
        m_new = functools.reduce(jnp.maximum, parts, m_old)
        s_new = gat[tok_n:2 * tok_n, :] * jnp.exp2((m_old - m_new) * LOG2E)
        for part in parts:
            s_new = s_new + jnp.exp2((part - m_new) * LOG2E)
        gat[0:tok_n, :] = m_new
        gat[tok_n:2 * tok_n, :] = s_new

    gat[0:tok_n, :] = jnp.full((tok_n, dim), -1e30, F32)
    gat[tok_n:2 * tok_n, :] = jnp.zeros((tok_n, dim), F32)
    send_n = spread(n_all.at[me], n_all, nsend, nrecv)
    for copy in send_n:
        copy.start()
    blocks(stat_block)
    m_lane = gat[0:tok_n, :]
    m_tok = jnp.max(m_lane, axis=-1, keepdims=True)
    s_tok = jnp.sum(gat[tok_n:2 * tok_n, :] * jnp.exp2((m_lane - m_tok) * LOG2E), axis=-1, keepdims=True)
    lse = m_tok + jnp.log(s_tok)
    level = lse * LOG2E + math.log2(total)
    z_pair = (dot_nt(n_val, lab_bf) * scale).astype(BF16).astype(F32)
    eye = lax.broadcasted_iota(jnp.int32, (tok_n, tok_n), 0) == lane
    z_lab = jnp.sum(jnp.where(eye, z_pair, 0.0), axis=-1, keepdims=True)
    p_lab = jnp.exp2(z_lab * LOG2E - level)
    d_lab = (p_lab - 1.0 / total).astype(BF16).astype(F32)
    p_lab = p_lab.astype(BF16).astype(F32)
    st_all[me] = jnp.concatenate(
        [row_of(level, tok_n), row_of(d_lab, tok_n), row_of(lse - z_lab, tok_n), jnp.zeros((5, tok_n), F32)], axis=0)
    level_full = jnp.broadcast_to(level, (tok_n, tok_n))

    gat[0:tok_n, :] = (d_lab - p_lab) * lab_rows
    send_s = spread(st_all.at[me], st_all, ssend, srecv)
    for copy in send_s:
        copy.start()

    def grad_block(v0, size):
        parts = []
        for j in range(size // tok_n):
            z = z_buf[:, pl.ds(v0 + j * tok_n, tok_n)].astype(F32)
            parts.append(jnp.exp2(z * LOG2E - level_full).astype(BF16))
        gat[0:tok_n, :] += dot_nn(jnp.concatenate(parts, axis=1), emb[pl.ds(v0, size), :])

    blocks(grad_block)
    dn = (gat[0:tok_n, :] * scale).astype(BF16).astype(F32)
    corr = jnp.mean(dn * x_last, axis=-1, keepdims=True)
    gs[n_stage] = (inv * dn - x_last * (inv * inv * inv * corr)).astype(BF16)

    def backward(i, carry):
        layer = n_stage - 1 - i
        g = gs[layer + 1]
        dh = dot_nt(g, wdn[layer]).astype(BF16).astype(F32)
        da = (dh * gelu_slope(pre[layer].astype(F32))).astype(BF16)
        gs[layer] = (g.astype(F32) + dot_nt(da, wup[layer])).astype(BF16)

        @pl.when(layer != me)
        def _():
            g_copy(layer).start()

        @pl.when(layer == me)
        def _():
            own_g.start()

        return carry

    lax.fori_loop(0, n_stage, backward, 0)
    send_d = spread(gs.at[0], dx_out, dsend, drecv)
    for copy in send_d:
        copy.start()
    own_d = pltpu.make_async_copy(gs.at[0], dx_out.at[me], loc_sem.at[4])
    own_d.start()

    for peer in peers:
        for buf, send, recv in ((n_all, nsend, nrecv), (st_all, ssend, srecv)):
            pltpu.make_async_remote_copy(buf.at[peer], buf.at[peer], send.at[0], recv.at[peer],
                                         device_id={"stage": peer}, device_id_type=MESH).wait_recv()
    own_s = pltpu.make_async_copy(st_all, st_out, loc_sem.at[3])
    own_s.start()
    for i in range(n_stage):
        cols = slice(i * tok_n, (i + 1) * tok_n)
        n_t[:, cols] = jnp.transpose(n_all[i])
        level_t[:, cols] = jnp.broadcast_to(st_all[i, 0:1, :], (8, tok_n))
        d_lab_t[:, cols] = jnp.broadcast_to(st_all[i, 1:2, :], (16, tok_n)).astype(BF16)
    half = vocab // 2
    wide = 2 * tok_n

    def table_copies(j, size):
        local = pl.ds(pl.multiple_of(j * TABLE_BLOCK, 16), size)
        rows = pl.ds(pl.multiple_of(core * half + j * TABLE_BLOCK, 16), size)
        return (pltpu.make_async_remote_copy(table.at[local], table_out.at[rows], tsend.at[j], trecv.at[j],
                                             device_id={"stage": sib}, device_id_type=MESH),
                pltpu.make_async_copy(table.at[local], table_out.at[rows], tloc.at[j]))

    def table_start(j, size):
        for copy in table_copies(j, size):
            copy.start()

    def table_block(j, size):
        base = pl.multiple_of(core * half + j * TABLE_BLOCK, 16)
        e = emb[pl.ds(base, size), :]
        row16 = lax.broadcasted_iota(jnp.int16, (size, wide), 0)
        acc = jnp.zeros((size, dim), F32)
        for t in range(total // wide):
            cols = slice(t * wide, (t + 1) * wide)
            z = (dot_nn(e, n_t[:, cols]) * scale).astype(BF16).astype(F32)
            p = jnp.exp2(z * LOG2E - level_t[0:1, cols]).astype(BF16)
            lab = jnp.concatenate([joined_row(lab_ref, 2 * t, tok_n), joined_row(lab_ref, 2 * t + 1, tok_n)], axis=1) - base
            lab = jnp.broadcast_to(lab, (16, wide)).astype(jnp.int16)
            dz = jnp.where(row16 == lab[0:1, :], d_lab_t[0:1, cols], p)
            acc = acc + dot_nn(dz, jnp.concatenate([n_all[2 * t], n_all[2 * t + 1]], axis=0))
        table[pl.ds(pl.multiple_of(j * TABLE_BLOCK, 16), size), :] = acc * scale

    full, tail = half // TABLE_BLOCK, half % TABLE_BLOCK

    def table_step(j, carry):
        @pl.when(j > 0)
        def _():
            table_start(j - 1, TABLE_BLOCK)

        table_block(j, TABLE_BLOCK)
        return carry

    lax.fori_loop(0, full, table_step, 0)
    table_start(full - 1, TABLE_BLOCK)
    if tail:
        table_block(full, tail)

    for copy in first + second + send_n + send_s:
        copy.wait_send()
    for copy in (own_x, own_g, own_s, own_d):
        copy.wait()
    for peer in peers:
        pltpu.make_async_remote_copy(xs.at[peer], xs_out.at[peer], xsend.at[peer], xrecv.at[peer],
                                     device_id={"stage": peer}, device_id_type=MESH).wait()
        pltpu.make_async_remote_copy(gs.at[peer + 1], gs_out.at[peer], gsend.at[peer], grecv.at[peer],
                                     device_id={"stage": peer}, device_id_type=MESH).wait()
        pltpu.make_async_remote_copy(gs.at[0], dx_out.at[peer], dsend.at[0], drecv.at[peer],
                                     device_id={"stage": peer}, device_id_type=MESH).wait_recv()
    for copy in send_d:
        copy.wait_send()
    if tail:
        table_start(full, tail)

    def table_wait(j, size):
        remote, local = table_copies(j, size)
        remote.wait_send()
        local.wait()
        rows = pl.ds(pl.multiple_of((1 - core) * half + j * TABLE_BLOCK, 16), size)
        pltpu.make_async_remote_copy(table.at[pl.ds(pl.multiple_of(j * TABLE_BLOCK, 16), size)], table_out.at[rows],
                                     tsend.at[j], trecv.at[j], device_id={"stage": sib}, device_id_type=MESH).wait_recv()

    def wait_step(j, carry):
        table_wait(j, TABLE_BLOCK)
        return carry

    lax.fori_loop(0, full, wait_step, 0)
    if tail:
        table_wait(full, tail)


def finish_kernel(
    starts_sm, part_hbm, x_ref, g_ref, wup_ref, wdn_ref, st_ref, dx_ref, ids_ref, rank_ref,
    out_hbm, gup_hbm, gdn_hbm, loss_ref,
    buf, dxs, hid, da, gup, gdn, read_sem, write_sem, grad_sem,
):
    n_chunk, tok_n, dim = dx_ref.shape
    vocab = buf.shape[0]
    ffn = hid.shape[1]
    full, tail = vocab // EMB_BLOCK, vocab % EMB_BLOCK

    def span(j, size):
        return pl.ds(pl.multiple_of(j * EMB_BLOCK, 16), size)

    def read(j, size):
        return pltpu.make_async_copy(part_hbm.at[span(j, size)], buf.at[span(j, size)], read_sem.at[j])

    def write(j, size):
        return pltpu.make_async_copy(buf.at[span(j, size)], out_hbm.at[span(j, size)], write_sem.at[j])

    def each(fn):
        def step(j, carry):
            fn(j, EMB_BLOCK)
            return carry

        lax.fori_loop(0, full, step, 0)
        if tail:
            fn(full, tail)

    each(lambda j, size: read(j, size).start())

    step_n = 2 * tok_n
    for i in range(n_chunk // 2):
        x = jnp.concatenate([x_ref[2 * i], x_ref[2 * i + 1]], axis=0)
        g = jnp.concatenate([g_ref[2 * i], g_ref[2 * i + 1]], axis=0)
        a = dot_nn(x, wup_ref[...]).astype(BF16).astype(F32)
        sq = a * a
        t = jnp.tanh(GELU_C * (a + 0.044715 * (sq * a)))
        cdf = 0.5 * (1.0 + t)
        hid[i * step_n:(i + 1) * step_n, :] = (a * cdf).astype(BF16)
        slope = cdf + (0.5 * a) * (1.0 - t * t) * (GELU_C * (1.0 + (3.0 * 0.044715) * sq))
        dh = dot_nt(g, wdn_ref[...]).astype(BF16).astype(F32)
        da[i * step_n:(i + 1) * step_n, :] = (dh * slope).astype(BF16)
    gup[...] = dot_tn(x_ref[...].reshape(n_chunk * tok_n, dim), da[...])
    gdn[...] = jnp.transpose(dot_tn(g_ref[...].reshape(n_chunk * tok_n, dim), hid[...]))
    grads = [pltpu.make_async_copy(gup, gup_hbm, grad_sem.at[0]), pltpu.make_async_copy(gdn, gdn_hbm, grad_sem.at[1])]
    for copy in grads:
        copy.start()
    loss_ref[0] = jnp.sum(st_ref[:, 2, :]) * (1.0 / (n_chunk * tok_n))

    row_id = lax.broadcasted_iota(jnp.int32, (tok_n, tok_n), 0)
    for c in range(n_chunk):
        acc = jnp.zeros((tok_n, dim), F32)
        for i in range(n_chunk):
            hot = jnp.where(rank_ref[i:i + 1, :] == row_id + c * tok_n, 1.0, 0.0).astype(BF16)
            acc = acc + dot_nn(hot, dx_ref[i])
        dxs[c] = acc.astype(BF16)
    dxs[n_chunk] = jnp.zeros((tok_n, dim), BF16)

    def add_tokens(j, size):
        read(j, size).wait()
        rows = span(j, size)
        row16 = lax.broadcasted_iota(jnp.int16, (size, tok_n), 0)

        def hot_rows(c):
            ids = jnp.broadcast_to(ids_ref[c, 0:1, :] - j * EMB_BLOCK, (16, tok_n)).astype(jnp.int16)
            return jnp.where(row16 == ids[0:1, :], jnp.ones((), BF16), jnp.zeros((), BF16))

        first = jnp.minimum(starts_sm[0, j] // tok_n, n_chunk - 1)
        last = (starts_sm[0, j + 1] + tok_n - 1) // tok_n
        buf[rows, :] += dot_nn(jnp.concatenate([hot_rows(first), hot_rows(first + 1)], axis=1),
                               jnp.concatenate([dxs[first], dxs[first + 1]], axis=0))

        def more(c, carry):
            buf[rows, :] += dot_nn(hot_rows(c), dxs[c])
            return carry

        lax.fori_loop(first + 2, last, more, 0)
        write(j, size).start()

    each(add_tokens)
    each(lambda j, size: write(j, size).wait())
    for copy in grads:
        copy.wait()


def solution(mesh):
    n_stage = mesh.shape["stage"]

    def device_fn(tokens, labels, emb_table, w_up, w_down):
        vocab, dim = emb_table.shape
        ffn = w_up.shape[2]
        total = tokens.shape[0] * tokens.shape[1]
        tok_n = total // n_stage
        w_up, w_down = w_up[0], w_down[0]
        vmem = pl.BlockSpec(memory_space=pltpu.VMEM)
        hbm = pl.BlockSpec(memory_space=pl.ANY)
        dma = pltpu.SemaphoreType.DMA
        act = jax.ShapeDtypeStruct((n_stage, tok_n, dim), BF16)
        st_all, xs_all, gs_all, dx_all, part, ids, rank, starts = pl.pallas_call(
            functools.partial(token_kernel, n_stage),
            out_shape=[jax.ShapeDtypeStruct((n_stage, 8, tok_n), F32), act, act, act,
                       jax.ShapeDtypeStruct((vocab, dim), F32),
                       jax.ShapeDtypeStruct((n_stage + 1, 8, tok_n), jnp.int32),
                       jax.ShapeDtypeStruct((n_stage, tok_n), jnp.int32), jax.ShapeDtypeStruct((1, tok_n), jnp.int32)],
            in_specs=[vmem, vmem, hbm, hbm, hbm],
            out_specs=[hbm] * 5 + [vmem] * 3,
            scratch_shapes=[
                pltpu.VMEM((n_stage, dim, ffn), BF16), pltpu.VMEM((n_stage, ffn, dim), BF16),
                pltpu.VMEM((vocab, dim), BF16), pltpu.VMEM((tok_n, vocab), BF16),
                pltpu.VMEM((n_stage + 1, tok_n, dim), BF16), pltpu.VMEM((n_stage + 1, tok_n, dim), BF16),
                pltpu.VMEM((n_stage, tok_n, ffn), BF16), pltpu.VMEM((n_stage, tok_n, dim), BF16),
                pltpu.VMEM((n_stage, 8, tok_n), F32), pltpu.VMEM((2 * tok_n, dim), F32),
                pltpu.VMEM((dim, total), BF16), pltpu.VMEM((8, total), F32), pltpu.VMEM((16, total), BF16),
                pltpu.VMEM((vocab // 2, dim), F32),
                dma((5,)), dma((14,))] + [dma((n_stage,))] * 12 + [dma((pl.cdiv(vocab // 2, TABLE_BLOCK),))] * 3,
            compiler_params=pltpu.CompilerParams(collective_id=0, has_side_effects=True, vmem_limit_bytes=VMEM_BYTES),
            name="token_pass",
        )(tokens, labels, emb_table, w_up, w_down)

        smem = pl.BlockSpec(memory_space=pltpu.SMEM)
        n_blk = pl.cdiv(vocab, EMB_BLOCK)
        grad_emb, grad_up, grad_down, loss = pl.pallas_call(
            finish_kernel,
            out_shape=[jax.ShapeDtypeStruct((vocab, dim), F32), jax.ShapeDtypeStruct((dim, ffn), F32),
                       jax.ShapeDtypeStruct((ffn, dim), F32), jax.ShapeDtypeStruct((1,), F32)],
            in_specs=[smem, hbm] + [vmem] * 8, out_specs=[hbm, hbm, hbm, smem],
            scratch_shapes=[
                pltpu.VMEM((vocab, dim), F32), pltpu.VMEM((n_stage + 1, tok_n, dim), BF16),
                pltpu.VMEM((total, ffn), BF16), pltpu.VMEM((total, ffn), BF16),
                pltpu.VMEM((dim, ffn), F32), pltpu.VMEM((ffn, dim), F32), dma((n_blk,)), dma((n_blk,)), dma((2,))],
            compiler_params=pltpu.CompilerParams(vmem_limit_bytes=VMEM_BYTES),
            name="finish",
        )(starts, part, xs_all, gs_all, w_up, w_down, st_all, dx_all, ids, rank)
        return loss, grad_up[None], grad_down[None], grad_emb

    return jax.shard_map(
        device_fn, mesh=mesh,
        in_specs=(P("dp", None), P("dp", None), P(None, None), P("stage", None, None), P("stage", None, None)),
        out_specs=(P("dp"), P(("dp", "stage"), None, None), P(("dp", "stage"), None, None), P("dp", None)),
        check_vma=False)
```

```python
import functools
import math

import jax
import jax.numpy as jnp
from jax import lax
from jax.experimental import pallas as pl
from jax.experimental.pallas import tpu as pltpu
from jax.sharding import PartitionSpec as P

MESH = pl.DeviceIdType.MESH
F32 = jnp.float32
BF16 = jnp.bfloat16
LOG2E = math.log2(math.e)
LN2 = math.log(2.0)
GELU_C = math.sqrt(2.0 / math.pi)
HEAD_BLOCK = 4096
TABLE_BLOCK = 2048
EMB_BLOCK = 2048
VMEM_BYTES = 60 * 1024 * 1024


def dot_nn(a, b):
    return lax.dot_general(a, b, (((1,), (0,)), ((), ())), preferred_element_type=F32)


def dot_nt(a, b):
    return lax.dot_general(a, b, (((1,), (1,)), ((), ())), preferred_element_type=F32)


def dot_tn(a, b):
    return lax.dot_general(a, b, (((0,), (0,)), ((), ())), preferred_element_type=F32)


def gelu_value(a):
    return a * (0.5 * (1.0 + jnp.tanh(GELU_C * (a + 0.044715 * (a * a * a)))))


def gelu_slope(a):
    sq = a * a
    t = jnp.tanh(GELU_C * (a + 0.044715 * (sq * a)))
    return 0.5 * (1.0 + t) + (0.5 * a) * (1.0 - t * t) * (GELU_C * (1.0 + (3.0 * 0.044715) * sq))


def column_of(row, size):
    return jnp.transpose(jnp.broadcast_to(row, (size, size)))


def joined_row(ref, i, size):
    per = size // ref.shape[1]
    return jnp.concatenate([ref[pl.ds(i * per + k, 1), :] for k in range(per)], axis=1)


def row_of(col, size):
    eye = lax.broadcasted_iota(jnp.int32, (size, size), 0) == lax.broadcasted_iota(jnp.int32, (size, size), 1)
    return jnp.sum(jnp.where(eye, jnp.broadcast_to(col, (size, size)), 0.0), axis=0, keepdims=True)


def token_kernel(
    n_stage, tok_hbm, lab_hbm, emb_hbm, wup_hbm, wdn_hbm,
    st_out, xs_out, gs_out, dx_out, table_out, ids_hbm, rank_hbm, starts_hbm,
    tok_ref, lab_ref, ids_out, rank_out, starts_out,
    wup, wdn, emb, z_buf, xs, gs, pre, n_all, st_all, gat, n_t, level_t, d_lab_t, table,
    loc_sem, wsend, upr, dnr, xsend, xrecv, gsend, grecv, nsend, nrecv, ssend, srecv, dsend, drecv, tsend, trecv, tloc,
):
    me = lax.axis_index("stage")
    n_chip = n_stage // 2
    chip, core = me // 2, lax.rem(me, 2)
    sib = chip * 2 + (1 - core)
    right = lax.rem(chip + 1, n_chip) * 2 + core
    left = lax.rem(chip + n_chip - 1, n_chip) * 2 + core
    far = lax.rem(chip + 2, n_chip) * 2 + core
    peers = [lax.rem(me + d, n_stage) for d in range(1, n_stage)]
    _, tok_n, dim = n_all.shape
    vocab = emb.shape[0]
    total = n_stage * tok_n
    scale = dim ** -0.5

    load_up = pltpu.make_async_copy(wup_hbm, wup.at[me], loc_sem.at[0])
    load_dn = pltpu.make_async_copy(wdn_hbm, wdn.at[me], loc_sem.at[1])
    load_emb = pltpu.make_async_copy(emb_hbm, emb, loc_sem.at[2])
    load_tok = pltpu.make_async_copy(tok_hbm, tok_ref, loc_sem.at[3])
    load_lab = pltpu.make_async_copy(lab_hbm, lab_ref, loc_sem.at[4])
    for copy in (load_up, load_dn, load_tok, load_lab, load_emb):
        copy.start()

    barrier = pltpu.get_barrier_semaphore()
    for peer in (right, left, sib):
        pl.semaphore_signal(barrier, inc=1, device_id={"stage": peer}, device_id_type=MESH)
    pl.semaphore_wait(barrier, 3)
    load_up.wait()
    load_dn.wait()

    def up_copy(i, slot, dst):
        return pltpu.make_async_remote_copy(
            wup.at[slot], wup.at[slot], wsend.at[i], upr.at[slot], device_id={"stage": dst}, device_id_type=MESH)

    def dn_copy(i, slot, dst):
        return pltpu.make_async_remote_copy(
            wdn.at[slot], wdn.at[slot], wsend.at[i], dnr.at[slot], device_id={"stage": dst}, device_id_type=MESH)

    first = [up_copy(0, me, right), dn_copy(1, me, left), dn_copy(2, me, right), up_copy(3, me, left),
             up_copy(4, me, sib), dn_copy(5, me, sib)]
    for copy in first:
        copy.start()

    load_tok.wait()
    load_lab.wait()
    tok_row = jnp.concatenate([joined_row(tok_ref, i, tok_n) for i in range(n_stage)], axis=0)
    pos = lax.broadcasted_iota(jnp.int32, (n_stage, tok_n), 0) * tok_n + lax.broadcasted_iota(jnp.int32, (n_stage, tok_n), 1)
    key_row = tok_row * total + pos
    lane = lax.broadcasted_iota(jnp.int32, (tok_n, tok_n), 1)
    key_cols = [column_of(key_row[j:j + 1, :], tok_n) for j in range(n_stage)]
    tok_cols = [column_of(tok_row[j:j + 1, :], tok_n) for j in range(n_stage)]
    rank_rows = []
    for i in range(n_stage):
        acc = jnp.zeros((tok_n, tok_n), jnp.int32)
        for j in range(n_stage):
            acc = acc + jnp.where(key_cols[j] < key_row[i:i + 1, :], 1, 0)
        rank_rows.append(jnp.sum(acc, axis=0, keepdims=True))
    rank_cols = [column_of(r, tok_n) for r in rank_rows]
    for c in range(n_stage):
        acc = jnp.zeros((tok_n, tok_n), jnp.int32)
        for j in range(n_stage):
            acc = acc + jnp.where(rank_cols[j] == lane + c * tok_n, tok_cols[j], 0)
        ids_out[c] = jnp.broadcast_to(jnp.sum(acc, axis=0, keepdims=True), (8, tok_n))
    ids_out[n_stage] = jnp.full((8, tok_n), -1, jnp.int32)
    acc = jnp.zeros((tok_n, tok_n), jnp.int32)
    for j in range(n_stage):
        acc = acc + jnp.where(tok_cols[j] < lane * EMB_BLOCK, 1, 0)
    starts_out[...] = jnp.sum(acc, axis=0, keepdims=True)
    for i in range(n_stage):
        rank_out[i:i + 1, :] = rank_rows[i]
    own_i = [pltpu.make_async_copy(ids_out, ids_hbm, loc_sem.at[5]), pltpu.make_async_copy(rank_out, rank_hbm, loc_sem.at[6]),
             pltpu.make_async_copy(starts_out, starts_hbm, loc_sem.at[7])]

    load_emb.wait()
    for copy in own_i:
        copy.start()
    pick = jnp.concatenate(
        [column_of(joined_row(tok_ref, me, tok_n), tok_n), column_of(joined_row(lab_ref, me, tok_n), tok_n)], axis=0)
    lane2 = lax.broadcasted_iota(jnp.int32, (2 * tok_n, tok_n), 1)

    def blocks(body):
        full = vocab // HEAD_BLOCK

        def step(i, carry):
            body(pl.multiple_of(i * HEAD_BLOCK, HEAD_BLOCK), HEAD_BLOCK)
            return carry

        lax.fori_loop(0, full, step, 0)
        if vocab % HEAD_BLOCK:
            body(full * HEAD_BLOCK, vocab % HEAD_BLOCK)

    gat[...] = jnp.zeros_like(gat)

    def gather_block(v0, size):
        hot = jnp.concatenate(
            [jnp.where(pick == lane2 + (v0 + j * tok_n), 1.0, 0.0).astype(BF16) for j in range(size // tok_n)], axis=1)
        gat[...] += dot_nn(hot, emb[pl.ds(v0, size), :])

    blocks(gather_block)
    x0 = gat[0:tok_n, :].astype(BF16)
    lab_rows = gat[tok_n:2 * tok_n, :]
    lab_bf = lab_rows.astype(BF16)

    up_copy(0, left, sib).wait_recv()
    second = [up_copy(6, left, right), up_copy(7, left, sib)]
    second[0].start()
    second[1].start()
    dn_copy(0, right, sib).wait_recv()
    second += [dn_copy(8, right, left), dn_copy(9, right, sib)]
    second[2].start()
    second[3].start()
    dn_copy(0, left, sib).wait_recv()
    second.append(dn_copy(10, left, sib))
    second[4].start()
    up_copy(0, right, sib).wait_recv()
    second.append(up_copy(11, right, sib))
    second[5].start()
    up_copy(0, far, sib).wait_recv()
    second.append(up_copy(12, far, sib))
    second[6].start()
    dn_copy(0, far, sib).wait_recv()
    second.append(dn_copy(13, far, sib))
    second[7].start()

    def x_copy(layer):
        return pltpu.make_async_remote_copy(
            xs.at[layer], xs_out.at[me], xsend.at[layer], xrecv.at[me], device_id={"stage": layer}, device_id_type=MESH)

    def g_copy(layer):
        return pltpu.make_async_remote_copy(
            gs.at[layer + 1], gs_out.at[me], gsend.at[layer], grecv.at[me], device_id={"stage": layer}, device_id_type=MESH)

    own_x = pltpu.make_async_copy(xs.at[me], xs_out.at[me], loc_sem.at[0])
    own_g = pltpu.make_async_copy(gs.at[me + 1], gs_out.at[me], loc_sem.at[1])

    xs[0] = x0

    def forward(layer, carry):
        @pl.when(lax.rem(layer, 2) != core)
        def _():
            up_copy(0, layer, sib).wait_recv()
            dn_copy(0, layer, sib).wait_recv()

        x = xs[layer]
        a = dot_nn(x, wup[layer]).astype(BF16)
        pre[layer] = a
        h = gelu_value(a.astype(F32)).astype(BF16)
        xs[layer + 1] = (x.astype(F32) + dot_nn(h, wdn[layer])).astype(BF16)

        @pl.when(layer != me)
        def _():
            x_copy(layer).start()

        @pl.when(layer == me)
        def _():
            own_x.start()

        return carry

    lax.fori_loop(0, n_stage, forward, 0)

    x_last = xs[n_stage].astype(F32)
    inv = lax.rsqrt(jnp.mean(x_last * x_last, axis=-1, keepdims=True) + 1e-6)
    n_val = (x_last * inv).astype(BF16)
    n_all[me] = n_val

    def spread(src, dst, send, recv):
        return [pltpu.make_async_remote_copy(src, dst.at[me], send.at[d], recv.at[me], device_id={"stage": peer},
                                             device_id_type=MESH) for d, peer in enumerate(peers)]

    def stat_block(v0, size):
        z = (dot_nt(n_all[me], emb[pl.ds(v0, size), :]) * scale).astype(BF16)
        z_buf[:, pl.ds(v0, size)] = z
        parts = [z[:, j * tok_n:(j + 1) * tok_n].astype(F32) for j in range(size // tok_n)]
        m_old = gat[0:tok_n, :]
        m_new = functools.reduce(jnp.maximum, parts, m_old)
        s_new = gat[tok_n:2 * tok_n, :] * jnp.exp2((m_old - m_new) * LOG2E)
        for part in parts:
            s_new = s_new + jnp.exp2((part - m_new) * LOG2E)
        gat[0:tok_n, :] = m_new
        gat[tok_n:2 * tok_n, :] = s_new

    gat[0:tok_n, :] = jnp.full((tok_n, dim), -1e30, F32)
    gat[tok_n:2 * tok_n, :] = jnp.zeros((tok_n, dim), F32)
    send_n = spread(n_all.at[me], n_all, nsend, nrecv)
    for copy in send_n:
        copy.start()
    blocks(stat_block)
    m_lane = gat[0:tok_n, :]
    m_tok = jnp.max(m_lane, axis=-1, keepdims=True)
    s_tok = jnp.sum(gat[tok_n:2 * tok_n, :] * jnp.exp2((m_lane - m_tok) * LOG2E), axis=-1, keepdims=True)
    lse = m_tok + jnp.log(s_tok)
    level = lse * LOG2E + math.log2(total)
    z_pair = (dot_nt(n_val, lab_bf) * scale).astype(BF16).astype(F32)
    eye = lax.broadcasted_iota(jnp.int32, (tok_n, tok_n), 0) == lane
    z_lab = jnp.sum(jnp.where(eye, z_pair, 0.0), axis=-1, keepdims=True)
    p_lab = jnp.exp2(z_lab * LOG2E - level)
    d_lab = (p_lab - 1.0 / total).astype(BF16).astype(F32)
    p_lab = p_lab.astype(BF16).astype(F32)
    st_all[me] = jnp.concatenate(
        [row_of(level, tok_n), row_of(d_lab, tok_n), row_of(lse - z_lab, tok_n), jnp.zeros((5, tok_n), F32)], axis=0)
    level_full = jnp.broadcast_to(level, (tok_n, tok_n))

    gat[0:tok_n, :] = (d_lab - p_lab) * lab_rows
    send_s = spread(st_all.at[me], st_all, ssend, srecv)
    for copy in send_s:
        copy.start()

    def grad_block(v0, size):
        parts = []
        for j in range(size // tok_n):
            z = z_buf[:, pl.ds(v0 + j * tok_n, tok_n)].astype(F32)
            parts.append(jnp.exp2(z * LOG2E - level_full).astype(BF16))
        gat[0:tok_n, :] += dot_nn(jnp.concatenate(parts, axis=1), emb[pl.ds(v0, size), :])

    blocks(grad_block)
    dn = (gat[0:tok_n, :] * scale).astype(BF16).astype(F32)
    corr = jnp.mean(dn * x_last, axis=-1, keepdims=True)
    gs[n_stage] = (inv * dn - x_last * (inv * inv * inv * corr)).astype(BF16)

    def backward(i, carry):
        layer = n_stage - 1 - i
        g = gs[layer + 1]
        dh = dot_nt(g, wdn[layer]).astype(BF16).astype(F32)
        da = (dh * gelu_slope(pre[layer].astype(F32))).astype(BF16)
        gs[layer] = (g.astype(F32) + dot_nt(da, wup[layer])).astype(BF16)

        @pl.when(layer != me)
        def _():
            g_copy(layer).start()

        @pl.when(layer == me)
        def _():
            own_g.start()

        return carry

    lax.fori_loop(0, n_stage, backward, 0)
    send_d = spread(gs.at[0], dx_out, dsend, drecv)
    for copy in send_d:
        copy.start()
    own_d = pltpu.make_async_copy(gs.at[0], dx_out.at[me], loc_sem.at[4])
    own_d.start()

    for peer in peers:
        for buf, send, recv in ((n_all, nsend, nrecv), (st_all, ssend, srecv)):
            pltpu.make_async_remote_copy(buf.at[peer], buf.at[peer], send.at[0], recv.at[peer],
                                         device_id={"stage": peer}, device_id_type=MESH).wait_recv()
    own_s = pltpu.make_async_copy(st_all, st_out, loc_sem.at[3])
    own_s.start()
    for i in range(n_stage):
        cols = slice(i * tok_n, (i + 1) * tok_n)
        n_t[:, cols] = jnp.transpose(n_all[i])
        level_t[:, cols] = jnp.broadcast_to(st_all[i, 0:1, :], (8, tok_n))
        d_lab_t[:, cols] = jnp.broadcast_to(st_all[i, 1:2, :], (16, tok_n)).astype(BF16)
    half = vocab // 2
    wide = 2 * tok_n

    def table_copies(j, size):
        local = pl.ds(pl.multiple_of(j * TABLE_BLOCK, 16), size)
        rows = pl.ds(pl.multiple_of(core * half + j * TABLE_BLOCK, 16), size)
        return (pltpu.make_async_remote_copy(table.at[local], table_out.at[rows], tsend.at[j], trecv.at[j],
                                             device_id={"stage": sib}, device_id_type=MESH),
                pltpu.make_async_copy(table.at[local], table_out.at[rows], tloc.at[j]))

    def table_start(j, size):
        for copy in table_copies(j, size):
            copy.start()

    def table_block(j, size):
        base = pl.multiple_of(core * half + j * TABLE_BLOCK, 16)
        e = emb[pl.ds(base, size), :]
        row16 = lax.broadcasted_iota(jnp.int16, (size, wide), 0)
        acc = jnp.zeros((size, dim), F32)
        for t in range(total // wide):
            cols = slice(t * wide, (t + 1) * wide)
            z = (dot_nn(e, n_t[:, cols]) * scale).astype(BF16).astype(F32)
            p = jnp.exp2(z * LOG2E - level_t[0:1, cols]).astype(BF16)
            lab = jnp.concatenate([joined_row(lab_ref, 2 * t, tok_n), joined_row(lab_ref, 2 * t + 1, tok_n)], axis=1) - base
            lab = jnp.broadcast_to(lab, (16, wide)).astype(jnp.int16)
            dz = jnp.where(row16 == lab[0:1, :], d_lab_t[0:1, cols], p)
            acc = acc + dot_nn(dz, jnp.concatenate([n_all[2 * t], n_all[2 * t + 1]], axis=0))
        table[pl.ds(pl.multiple_of(j * TABLE_BLOCK, 16), size), :] = acc * scale

    full, tail = half // TABLE_BLOCK, half % TABLE_BLOCK

    def table_step(j, carry):
        @pl.when(j > 0)
        def _():
            table_start(j - 1, TABLE_BLOCK)

        table_block(j, TABLE_BLOCK)
        return carry

    lax.fori_loop(0, full, table_step, 0)
    table_start(full - 1, TABLE_BLOCK)
    if tail:
        table_block(full, tail)

    for copy in first + second + send_n + send_s:
        copy.wait_send()
    for copy in (own_x, own_g, own_s, own_d, *own_i):
        copy.wait()
    for peer in peers:
        pltpu.make_async_remote_copy(xs.at[peer], xs_out.at[peer], xsend.at[peer], xrecv.at[peer],
                                     device_id={"stage": peer}, device_id_type=MESH).wait()
        pltpu.make_async_remote_copy(gs.at[peer + 1], gs_out.at[peer], gsend.at[peer], grecv.at[peer],
                                     device_id={"stage": peer}, device_id_type=MESH).wait()
        pltpu.make_async_remote_copy(gs.at[0], dx_out.at[peer], dsend.at[0], drecv.at[peer],
                                     device_id={"stage": peer}, device_id_type=MESH).wait_recv()
    for copy in send_d:
        copy.wait_send()
    if tail:
        table_start(full, tail)

    def table_wait(j, size):
        remote, local = table_copies(j, size)
        remote.wait_send()
        local.wait()
        rows = pl.ds(pl.multiple_of((1 - core) * half + j * TABLE_BLOCK, 16), size)
        pltpu.make_async_remote_copy(table.at[pl.ds(pl.multiple_of(j * TABLE_BLOCK, 16), size)], table_out.at[rows],
                                     tsend.at[j], trecv.at[j], device_id={"stage": sib}, device_id_type=MESH).wait_recv()

    def wait_step(j, carry):
        table_wait(j, TABLE_BLOCK)
        return carry

    lax.fori_loop(0, full, wait_step, 0)
    if tail:
        table_wait(full, tail)


def finish_kernel(
    starts_sm, part_hbm, x_hbm, g_hbm, wup_hbm, wdn_hbm, st_hbm, dx_hbm, ids_hbm, rank_hbm,
    out_hbm, gup_hbm, gdn_hbm, loss_ref,
    x_ref, g_ref, wup_ref, wdn_ref, st_ref, dx_ref, ids_ref, rank_ref,
    buf, dxs, hid, da, gup, gdn, read_sem, write_sem, grad_sem, load_sem,
):
    n_chunk, tok_n, dim = dx_ref.shape
    vocab = buf.shape[0]
    ffn = hid.shape[1]
    full, tail = vocab // EMB_BLOCK, vocab % EMB_BLOCK

    def span(j, size):
        return pl.ds(pl.multiple_of(j * EMB_BLOCK, 16), size)

    def read(j, size):
        return pltpu.make_async_copy(part_hbm.at[span(j, size)], buf.at[span(j, size)], read_sem.at[j])

    def write(j, size):
        return pltpu.make_async_copy(buf.at[span(j, size)], out_hbm.at[span(j, size)], write_sem.at[j])

    def each(fn):
        def step(j, carry):
            fn(j, EMB_BLOCK)
            return carry

        lax.fori_loop(0, full, step, 0)
        if tail:
            fn(full, tail)

    loads = [pltpu.make_async_copy(src, dst, load_sem.at[i]) for i, (src, dst) in enumerate((
        (x_hbm, x_ref), (wup_hbm, wup_ref), (g_hbm, g_ref), (wdn_hbm, wdn_ref), (st_hbm, st_ref), (dx_hbm, dx_ref),
        (ids_hbm, ids_ref), (rank_hbm, rank_ref)))]
    for copy in loads:
        copy.start()
    each(lambda j, size: read(j, size).start())
    for copy in loads:
        copy.wait()

    step_n = 2 * tok_n
    for i in range(n_chunk // 2):
        x = jnp.concatenate([x_ref[2 * i], x_ref[2 * i + 1]], axis=0)
        g = jnp.concatenate([g_ref[2 * i], g_ref[2 * i + 1]], axis=0)
        a = dot_nn(x, wup_ref[...]).astype(BF16).astype(F32)
        sq = a * a
        t = jnp.tanh(GELU_C * (a + 0.044715 * (sq * a)))
        cdf = 0.5 * (1.0 + t)
        hid[i * step_n:(i + 1) * step_n, :] = (a * cdf).astype(BF16)
        slope = cdf + (0.5 * a) * (1.0 - t * t) * (GELU_C * (1.0 + (3.0 * 0.044715) * sq))
        dh = dot_nt(g, wdn_ref[...]).astype(BF16).astype(F32)
        da[i * step_n:(i + 1) * step_n, :] = (dh * slope).astype(BF16)
    gup[...] = dot_tn(x_ref[...].reshape(n_chunk * tok_n, dim), da[...])
    gdn[...] = jnp.transpose(dot_tn(g_ref[...].reshape(n_chunk * tok_n, dim), hid[...]))
    grads = [pltpu.make_async_copy(gup, gup_hbm, grad_sem.at[0]), pltpu.make_async_copy(gdn, gdn_hbm, grad_sem.at[1])]
    for copy in grads:
        copy.start()
    loss_ref[0] = jnp.sum(st_ref[:, 2, :]) * (1.0 / (n_chunk * tok_n))

    row_id = lax.broadcasted_iota(jnp.int32, (tok_n, tok_n), 0)
    for c in range(n_chunk):
        acc = jnp.zeros((tok_n, dim), F32)
        for i in range(n_chunk):
            hot = jnp.where(rank_ref[i:i + 1, :] == row_id + c * tok_n, 1.0, 0.0).astype(BF16)
            acc = acc + dot_nn(hot, dx_ref[i])
        dxs[c] = acc.astype(BF16)
    dxs[n_chunk] = jnp.zeros((tok_n, dim), BF16)

    def add_tokens(j, size):
        read(j, size).wait()
        rows = span(j, size)
        row16 = lax.broadcasted_iota(jnp.int16, (size, tok_n), 0)

        def hot_rows(c):
            ids = jnp.broadcast_to(ids_ref[c, 0:1, :] - j * EMB_BLOCK, (16, tok_n)).astype(jnp.int16)
            return jnp.where(row16 == ids[0:1, :], jnp.ones((), BF16), jnp.zeros((), BF16))

        first = jnp.minimum(starts_sm[0, j] // tok_n, n_chunk - 1)
        last = (starts_sm[0, j + 1] + tok_n - 1) // tok_n
        buf[rows, :] += dot_nn(jnp.concatenate([hot_rows(first), hot_rows(first + 1)], axis=1),
                               jnp.concatenate([dxs[first], dxs[first + 1]], axis=0))

        def more(c, carry):
            buf[rows, :] += dot_nn(hot_rows(c), dxs[c])
            return carry

        lax.fori_loop(first + 2, last, more, 0)
        write(j, size).start()

    each(add_tokens)
    each(lambda j, size: write(j, size).wait())
    for copy in grads:
        copy.wait()


def solution(mesh):
    n_stage = mesh.shape["stage"]

    def device_fn(tokens, labels, emb_table, w_up, w_down):
        vocab, dim = emb_table.shape
        ffn = w_up.shape[2]
        total = tokens.shape[0] * tokens.shape[1]
        tok_n = total // n_stage
        w_up, w_down = w_up[0], w_down[0]
        hbm = pl.BlockSpec(memory_space=pl.ANY)
        dma = pltpu.SemaphoreType.DMA
        act = jax.ShapeDtypeStruct((n_stage, tok_n, dim), BF16)
        st_all, xs_all, gs_all, dx_all, part, ids, rank, starts = pl.pallas_call(
            functools.partial(token_kernel, n_stage),
            out_shape=[jax.ShapeDtypeStruct((n_stage, 8, tok_n), F32), act, act, act,
                       jax.ShapeDtypeStruct((vocab, dim), F32),
                       jax.ShapeDtypeStruct((n_stage + 1, 8, tok_n), jnp.int32),
                       jax.ShapeDtypeStruct((n_stage, tok_n), jnp.int32), jax.ShapeDtypeStruct((1, tok_n), jnp.int32)],
            in_specs=[hbm] * 5,
            out_specs=[hbm] * 8,
            scratch_shapes=[
                pltpu.VMEM(tokens.shape, jnp.int32), pltpu.VMEM(labels.shape, jnp.int32),
                pltpu.VMEM((n_stage + 1, 8, tok_n), jnp.int32), pltpu.VMEM((n_stage, tok_n), jnp.int32),
                pltpu.VMEM((1, tok_n), jnp.int32),
                pltpu.VMEM((n_stage, dim, ffn), BF16), pltpu.VMEM((n_stage, ffn, dim), BF16),
                pltpu.VMEM((vocab, dim), BF16), pltpu.VMEM((tok_n, vocab), BF16),
                pltpu.VMEM((n_stage + 1, tok_n, dim), BF16), pltpu.VMEM((n_stage + 1, tok_n, dim), BF16),
                pltpu.VMEM((n_stage, tok_n, ffn), BF16), pltpu.VMEM((n_stage, tok_n, dim), BF16),
                pltpu.VMEM((n_stage, 8, tok_n), F32), pltpu.VMEM((2 * tok_n, dim), F32),
                pltpu.VMEM((dim, total), BF16), pltpu.VMEM((8, total), F32), pltpu.VMEM((16, total), BF16),
                pltpu.VMEM((vocab // 2, dim), F32),
                dma((8,)), dma((14,))] + [dma((n_stage,))] * 12 + [dma((pl.cdiv(vocab // 2, TABLE_BLOCK),))] * 3,
            compiler_params=pltpu.CompilerParams(collective_id=0, has_side_effects=True, vmem_limit_bytes=VMEM_BYTES),
            name="token_pass",
        )(tokens, labels, emb_table, w_up, w_down)

        smem = pl.BlockSpec(memory_space=pltpu.SMEM)
        n_blk = pl.cdiv(vocab, EMB_BLOCK)
        grad_emb, grad_up, grad_down, loss = pl.pallas_call(
            finish_kernel,
            out_shape=[jax.ShapeDtypeStruct((vocab, dim), F32), jax.ShapeDtypeStruct((dim, ffn), F32),
                       jax.ShapeDtypeStruct((ffn, dim), F32), jax.ShapeDtypeStruct((1,), F32)],
            in_specs=[smem] + [hbm] * 9, out_specs=[hbm, hbm, hbm, smem],
            scratch_shapes=[
                pltpu.VMEM((n_stage, tok_n, dim), BF16), pltpu.VMEM((n_stage, tok_n, dim), BF16),
                pltpu.VMEM((dim, ffn), BF16), pltpu.VMEM((ffn, dim), BF16), pltpu.VMEM((n_stage, 8, tok_n), F32),
                pltpu.VMEM((n_stage, tok_n, dim), BF16), pltpu.VMEM((n_stage + 1, 8, tok_n), jnp.int32),
                pltpu.VMEM((n_stage, tok_n), jnp.int32),
                pltpu.VMEM((vocab, dim), F32), pltpu.VMEM((n_stage + 1, tok_n, dim), BF16),
                pltpu.VMEM((total, ffn), BF16), pltpu.VMEM((total, ffn), BF16),
                pltpu.VMEM((dim, ffn), F32), pltpu.VMEM((ffn, dim), F32), dma((n_blk,)), dma((n_blk,)), dma((2,)),
                dma((8,))],
            compiler_params=pltpu.CompilerParams(vmem_limit_bytes=VMEM_BYTES),
            name="finish",
        )(starts, part, xs_all, gs_all, w_up, w_down, st_all, dx_all, ids, rank)
        return loss, grad_up[None], grad_down[None], grad_emb

    return jax.shard_map(
        device_fn, mesh=mesh,
        in_specs=(P("dp", None), P("dp", None), P(None, None), P("stage", None, None), P("stage", None, None)),
        out_specs=(P("dp"), P(("dp", "stage"), None, None), P(("dp", "stage"), None, None), P("dp", None)),
        check_vma=False)
```

```python
import functools
import math

import jax
import jax.numpy as jnp
from jax import lax
from jax.experimental import pallas as pl
from jax.experimental.pallas import tpu as pltpu
from jax.sharding import PartitionSpec as P

MESH = pl.DeviceIdType.MESH
F32 = jnp.float32
BF16 = jnp.bfloat16
LOG2E = math.log2(math.e)
LN2 = math.log(2.0)
GELU_C = math.sqrt(2.0 / math.pi)
HEAD_BLOCK = 4096
TABLE_BLOCK = 2048
EMB_BLOCK = 2048
TOKEN_VMEM = 46 * 1024 * 1024
FINISH_VMEM = 28 * 1024 * 1024


def dot_nn(a, b):
    return lax.dot_general(a, b, (((1,), (0,)), ((), ())), preferred_element_type=F32)


def dot_nt(a, b):
    return lax.dot_general(a, b, (((1,), (1,)), ((), ())), preferred_element_type=F32)


def dot_tn(a, b):
    return lax.dot_general(a, b, (((0,), (0,)), ((), ())), preferred_element_type=F32)


def gelu_value(a):
    return a * (0.5 * (1.0 + jnp.tanh(GELU_C * (a + 0.044715 * (a * a * a)))))


def gelu_slope(a):
    sq = a * a
    t = jnp.tanh(GELU_C * (a + 0.044715 * (sq * a)))
    return 0.5 * (1.0 + t) + (0.5 * a) * (1.0 - t * t) * (GELU_C * (1.0 + (3.0 * 0.044715) * sq))


def column_of(row, size):
    return jnp.transpose(jnp.broadcast_to(row, (size, size)))


def joined_row(ref, i, size):
    per = size // ref.shape[1]
    return jnp.concatenate([ref[pl.ds(i * per + k, 1), :] for k in range(per)], axis=1)


def row_of(col, size):
    eye = lax.broadcasted_iota(jnp.int32, (size, size), 0) == lax.broadcasted_iota(jnp.int32, (size, size), 1)
    return jnp.sum(jnp.where(eye, jnp.broadcast_to(col, (size, size)), 0.0), axis=0, keepdims=True)


def token_kernel(
    n_stage, tok_hbm, lab_hbm, emb_hbm, wup_hbm, wdn_hbm,
    st_all, xs_out, gs_out, dx_out, table_out, ids_out, rank_out, wup_out, wdn_out, starts_out,
    tok_ref, lab_ref,
    wup, wdn, emb, z_buf, xs, gs, pre, n_all, gat, n_t, level_t, d_lab_t,
    loc_sem, wsend, upr, dnr, xsend, xrecv, gsend, grecv, nsend, nrecv, ssend, srecv, dsend, drecv, tsend, trecv,
):
    me = lax.axis_index("stage")
    n_chip = n_stage // 2
    chip, core = me // 2, lax.rem(me, 2)
    sib = chip * 2 + (1 - core)
    right = lax.rem(chip + 1, n_chip) * 2 + core
    left = lax.rem(chip + n_chip - 1, n_chip) * 2 + core
    far = lax.rem(chip + 2, n_chip) * 2 + core
    peers = [lax.rem(me + d, n_stage) for d in range(1, n_stage)]
    _, tok_n, dim = n_all.shape
    vocab = emb.shape[0]
    total = n_stage * tok_n
    scale = dim ** -0.5

    load_up = pltpu.make_async_copy(wup_hbm, wup.at[me], loc_sem.at[0])
    load_dn = pltpu.make_async_copy(wdn_hbm, wdn.at[me], loc_sem.at[1])
    load_emb = pltpu.make_async_copy(emb_hbm, emb, loc_sem.at[2])
    load_tok = pltpu.make_async_copy(tok_hbm, tok_ref, loc_sem.at[3])
    load_lab = pltpu.make_async_copy(lab_hbm, lab_ref, loc_sem.at[4])
    for copy in (load_up, load_dn, load_tok, load_lab, load_emb):
        copy.start()

    barrier = pltpu.get_barrier_semaphore()
    for peer in (right, left, sib):
        pl.semaphore_signal(barrier, inc=1, device_id={"stage": peer}, device_id_type=MESH)
    pl.semaphore_wait(barrier, 3)
    load_up.wait()
    load_dn.wait()

    def up_copy(i, slot, dst):
        return pltpu.make_async_remote_copy(
            wup.at[slot], wup.at[slot], wsend.at[i], upr.at[slot], device_id={"stage": dst}, device_id_type=MESH)

    def dn_copy(i, slot, dst):
        return pltpu.make_async_remote_copy(
            wdn.at[slot], wdn.at[slot], wsend.at[i], dnr.at[slot], device_id={"stage": dst}, device_id_type=MESH)

    first = [up_copy(0, me, right), dn_copy(1, me, left), dn_copy(2, me, right), up_copy(3, me, left),
             up_copy(4, me, sib), dn_copy(5, me, sib)]
    for copy in first:
        copy.start()

    load_tok.wait()
    load_lab.wait()
    tok_row = jnp.concatenate([joined_row(tok_ref, i, tok_n) for i in range(n_stage)], axis=0)
    pos = lax.broadcasted_iota(jnp.int32, (n_stage, tok_n), 0) * tok_n + lax.broadcasted_iota(jnp.int32, (n_stage, tok_n), 1)
    key_row = tok_row * total + pos
    lane = lax.broadcasted_iota(jnp.int32, (tok_n, tok_n), 1)
    key_cols = [column_of(key_row[j:j + 1, :], tok_n) for j in range(n_stage)]
    tok_cols = [column_of(tok_row[j:j + 1, :], tok_n) for j in range(n_stage)]
    rank_rows = []
    for i in range(n_stage):
        acc = jnp.zeros((tok_n, tok_n), jnp.int32)
        for j in range(n_stage):
            acc = acc + jnp.where(key_cols[j] < key_row[i:i + 1, :], 1, 0)
        rank_rows.append(jnp.sum(acc, axis=0, keepdims=True))
    rank_cols = [column_of(r, tok_n) for r in rank_rows]
    for c in range(n_stage):
        acc = jnp.zeros((tok_n, tok_n), jnp.int32)
        for j in range(n_stage):
            acc = acc + jnp.where(rank_cols[j] == lane + c * tok_n, tok_cols[j], 0)
        ids_out[c] = jnp.broadcast_to(jnp.sum(acc, axis=0, keepdims=True), (8, tok_n))
    ids_out[n_stage] = jnp.full((8, tok_n), -1, jnp.int32)
    acc = jnp.zeros((tok_n, tok_n), jnp.int32)
    for j in range(n_stage):
        acc = acc + jnp.where(tok_cols[j] < lane * EMB_BLOCK, 1, 0)
    starts_out[...] = jnp.sum(acc, axis=0, keepdims=True)
    for i in range(n_stage):
        rank_out[i:i + 1, :] = rank_rows[i]
    wup_out[...] = wup[me]
    wdn_out[...] = wdn[me]

    load_emb.wait()
    pick = jnp.concatenate(
        [column_of(joined_row(tok_ref, me, tok_n), tok_n), column_of(joined_row(lab_ref, me, tok_n), tok_n)], axis=0)
    lane2 = lax.broadcasted_iota(jnp.int32, (2 * tok_n, tok_n), 1)

    head_full = vocab // HEAD_BLOCK

    def blocks(body, lo=0, hi=head_full):
        def step(i, carry):
            body(pl.multiple_of(i * HEAD_BLOCK, HEAD_BLOCK), HEAD_BLOCK)
            return carry

        lax.fori_loop(lo, hi, step, 0)
        if hi == head_full and vocab % HEAD_BLOCK:
            body(head_full * HEAD_BLOCK, vocab % HEAD_BLOCK)

    gat[...] = jnp.zeros_like(gat)

    def gather_block(v0, size):
        hot = jnp.concatenate(
            [jnp.where(pick == lane2 + (v0 + j * tok_n), 1.0, 0.0).astype(BF16) for j in range(size // tok_n)], axis=1)
        gat[...] += dot_nn(hot, emb[pl.ds(v0, size), :])

    blocks(gather_block, 0, head_full // 2)

    up_copy(0, left, sib).wait_recv()
    second = [up_copy(6, left, right), up_copy(7, left, sib)]
    second[0].start()
    second[1].start()
    dn_copy(0, right, sib).wait_recv()
    second += [dn_copy(8, right, left), dn_copy(9, right, sib)]
    second[2].start()
    second[3].start()

    blocks(gather_block, head_full // 2, head_full)
    x0 = gat[0:tok_n, :].astype(BF16)
    lab_rows = gat[tok_n:2 * tok_n, :]
    lab_bf = lab_rows.astype(BF16)

    dn_copy(0, left, sib).wait_recv()
    second.append(dn_copy(10, left, sib))
    second[4].start()
    up_copy(0, right, sib).wait_recv()
    second.append(up_copy(11, right, sib))
    second[5].start()
    up_copy(0, far, sib).wait_recv()
    second.append(up_copy(12, far, sib))
    second[6].start()
    dn_copy(0, far, sib).wait_recv()
    second.append(dn_copy(13, far, sib))
    second[7].start()

    def x_copy(layer):
        return pltpu.make_async_remote_copy(
            xs.at[layer], xs_out.at[me], xsend.at[layer], xrecv.at[me], device_id={"stage": layer}, device_id_type=MESH)

    def g_copy(layer):
        return pltpu.make_async_remote_copy(
            gs.at[layer + 1], gs_out.at[me], gsend.at[layer], grecv.at[me], device_id={"stage": layer}, device_id_type=MESH)


    xs[0] = x0

    def forward(layer, carry):
        @pl.when(lax.rem(layer, 2) != core)
        def _():
            up_copy(0, layer, sib).wait_recv()
            dn_copy(0, layer, sib).wait_recv()

        x = xs[layer]
        a = dot_nn(x, wup[layer]).astype(BF16)
        pre[layer] = a
        h = gelu_value(a.astype(F32)).astype(BF16)
        xs[layer + 1] = (x.astype(F32) + dot_nn(h, wdn[layer])).astype(BF16)

        @pl.when(layer != me)
        def _():
            x_copy(layer).start()

        @pl.when(layer == me)
        def _():
            xs_out[me] = x

        return carry

    lax.fori_loop(0, n_stage, forward, 0)

    x_last = xs[n_stage].astype(F32)
    inv = lax.rsqrt(jnp.mean(x_last * x_last, axis=-1, keepdims=True) + 1e-6)
    n_val = (x_last * inv).astype(BF16)
    n_all[me] = n_val

    def spread(src, dst, send, recv):
        return [pltpu.make_async_remote_copy(src, dst.at[me], send.at[d], recv.at[me], device_id={"stage": peer},
                                             device_id_type=MESH) for d, peer in enumerate(peers)]

    def stat_block(v0, size):
        z = (dot_nt(n_all[me], emb[pl.ds(v0, size), :]) * scale).astype(BF16)
        z_buf[:, pl.ds(v0, size)] = z
        parts = [z[:, j * tok_n:(j + 1) * tok_n].astype(F32) for j in range(size // tok_n)]
        m_old = gat[0:tok_n, :]
        m_new = functools.reduce(jnp.maximum, parts, m_old)
        s_new = gat[tok_n:2 * tok_n, :] * jnp.exp2((m_old - m_new) * LOG2E)
        for part in parts:
            s_new = s_new + jnp.exp2((part - m_new) * LOG2E)
        gat[0:tok_n, :] = m_new
        gat[tok_n:2 * tok_n, :] = s_new

    gat[0:tok_n, :] = jnp.full((tok_n, dim), -1e30, F32)
    gat[tok_n:2 * tok_n, :] = jnp.zeros((tok_n, dim), F32)
    send_n = spread(n_all.at[me], n_all, nsend, nrecv)
    for copy in send_n:
        copy.start()
    blocks(stat_block)
    m_lane = gat[0:tok_n, :]
    m_tok = jnp.max(m_lane, axis=-1, keepdims=True)
    s_tok = jnp.sum(gat[tok_n:2 * tok_n, :] * jnp.exp2((m_lane - m_tok) * LOG2E), axis=-1, keepdims=True)
    lse = m_tok + jnp.log(s_tok)
    level = lse * LOG2E + math.log2(total)
    z_pair = (dot_nt(n_val, lab_bf) * scale).astype(BF16).astype(F32)
    eye = lax.broadcasted_iota(jnp.int32, (tok_n, tok_n), 0) == lane
    z_lab = jnp.sum(jnp.where(eye, z_pair, 0.0), axis=-1, keepdims=True)
    p_lab = jnp.exp2(z_lab * LOG2E - level)
    d_lab = (p_lab - 1.0 / total).astype(BF16).astype(F32)
    p_lab = p_lab.astype(BF16).astype(F32)
    st_all[me] = jnp.concatenate(
        [row_of(level, tok_n), row_of(d_lab, tok_n), row_of(lse - z_lab, tok_n), jnp.zeros((5, tok_n), F32)], axis=0)
    level_full = jnp.broadcast_to(level, (tok_n, tok_n))

    gat[0:tok_n, :] = (d_lab - p_lab) * lab_rows
    send_s = spread(st_all.at[me], st_all, ssend, srecv)
    for copy in send_s:
        copy.start()

    def grad_block(v0, size):
        parts = []
        for j in range(size // tok_n):
            z = z_buf[:, pl.ds(v0 + j * tok_n, tok_n)].astype(F32)
            parts.append(jnp.exp2(z * LOG2E - level_full).astype(BF16))
        gat[0:tok_n, :] += dot_nn(jnp.concatenate(parts, axis=1), emb[pl.ds(v0, size), :])

    blocks(grad_block)
    dn = (gat[0:tok_n, :] * scale).astype(BF16).astype(F32)
    corr = jnp.mean(dn * x_last, axis=-1, keepdims=True)
    gs[n_stage] = (inv * dn - x_last * (inv * inv * inv * corr)).astype(BF16)

    def backward(i, carry):
        layer = n_stage - 1 - i
        g = gs[layer + 1]
        dh = dot_nt(g, wdn[layer]).astype(BF16).astype(F32)
        da = (dh * gelu_slope(pre[layer].astype(F32))).astype(BF16)
        gs[layer] = (g.astype(F32) + dot_nt(da, wup[layer])).astype(BF16)

        @pl.when(layer != me)
        def _():
            g_copy(layer).start()

        @pl.when(layer == me)
        def _():
            gs_out[me] = g

        return carry

    lax.fori_loop(0, n_stage, backward, 0)
    send_d = spread(gs.at[0], dx_out, dsend, drecv)
    for copy in send_d:
        copy.start()
    dx_out[me] = gs[0]

    for peer in peers:
        for buf, send, recv in ((n_all, nsend, nrecv), (st_all, ssend, srecv)):
            pltpu.make_async_remote_copy(buf.at[peer], buf.at[peer], send.at[0], recv.at[peer],
                                         device_id={"stage": peer}, device_id_type=MESH).wait_recv()
    for i in range(n_stage):
        cols = slice(i * tok_n, (i + 1) * tok_n)
        n_t[:, cols] = jnp.transpose(n_all[i])
        level_t[:, cols] = jnp.broadcast_to(st_all[i, 0:1, :], (8, tok_n))
        d_lab_t[:, cols] = jnp.broadcast_to(st_all[i, 1:2, :], (16, tok_n)).astype(BF16)
    half = vocab // 2
    wide = 2 * tok_n

    def table_copies(j, size):
        rows = pl.ds(pl.multiple_of(core * half + j * TABLE_BLOCK, 16), size)
        return (pltpu.make_async_remote_copy(table_out.at[rows], table_out.at[rows], tsend.at[j], trecv.at[j],
                                             device_id={"stage": sib}, device_id_type=MESH),)

    def table_start(j, size):
        for copy in table_copies(j, size):
            copy.start()

    def table_block(j, size):
        base = pl.multiple_of(core * half + j * TABLE_BLOCK, 16)
        e = emb[pl.ds(base, size), :]
        row16 = lax.broadcasted_iota(jnp.int16, (size, wide), 0)
        acc = jnp.zeros((size, dim), F32)
        for t in range(total // wide):
            cols = slice(t * wide, (t + 1) * wide)
            z = (dot_nn(e, n_t[:, cols]) * scale).astype(BF16).astype(F32)
            p = jnp.exp2(z * LOG2E - level_t[0:1, cols]).astype(BF16)
            lab = jnp.concatenate([joined_row(lab_ref, 2 * t, tok_n), joined_row(lab_ref, 2 * t + 1, tok_n)], axis=1) - base
            lab = jnp.broadcast_to(lab, (16, wide)).astype(jnp.int16)
            dz = jnp.where(row16 == lab[0:1, :], d_lab_t[0:1, cols], p)
            acc = acc + dot_nn(dz, jnp.concatenate([n_all[2 * t], n_all[2 * t + 1]], axis=0))
        table_out[pl.ds(base, size), :] = acc * scale

    full, tail = half // TABLE_BLOCK, half % TABLE_BLOCK

    def table_step(j, carry):
        @pl.when(j > 0)
        def _():
            table_start(j - 1, TABLE_BLOCK)

        table_block(j, TABLE_BLOCK)
        return carry

    lax.fori_loop(0, full, table_step, 0)
    table_start(full - 1, TABLE_BLOCK)
    if tail:
        table_block(full, tail)

    for copy in first + second + send_n + send_s:
        copy.wait_send()
    for peer in peers:
        pltpu.make_async_remote_copy(xs.at[peer], xs_out.at[peer], xsend.at[peer], xrecv.at[peer],
                                     device_id={"stage": peer}, device_id_type=MESH).wait()
        pltpu.make_async_remote_copy(gs.at[peer + 1], gs_out.at[peer], gsend.at[peer], grecv.at[peer],
                                     device_id={"stage": peer}, device_id_type=MESH).wait()
        pltpu.make_async_remote_copy(gs.at[0], dx_out.at[peer], dsend.at[0], drecv.at[peer],
                                     device_id={"stage": peer}, device_id_type=MESH).wait_recv()
    for copy in send_d:
        copy.wait_send()
    if tail:
        table_start(full, tail)

    def table_wait(j, size):
        table_copies(j, size)[0].wait_send()
        rows = pl.ds(pl.multiple_of((1 - core) * half + j * TABLE_BLOCK, 16), size)
        pltpu.make_async_remote_copy(table_out.at[rows], table_out.at[rows],
                                     tsend.at[j], trecv.at[j], device_id={"stage": sib}, device_id_type=MESH).wait_recv()

    def wait_step(j, carry):
        table_wait(j, TABLE_BLOCK)
        return carry

    lax.fori_loop(0, full, wait_step, 0)
    if tail:
        table_wait(full, tail)


def finish_kernel(
    starts_ref, part_ref, x_ref, g_ref, wup_ref, wdn_ref, st_ref, dx_ref, ids_ref, rank_ref,
    out_hbm, gup_hbm, gdn_hbm, loss_ref,
    starts_sm, buf, dxs, hid, da, gup, gdn, write_sem, grad_sem,
):
    n_chunk, tok_n, dim = dx_ref.shape
    vocab = buf.shape[0]
    ffn = hid.shape[1]
    full, tail = vocab // EMB_BLOCK, vocab % EMB_BLOCK

    def span(j, size):
        return pl.ds(pl.multiple_of(j * EMB_BLOCK, 16), size)

    def write(j, size):
        return pltpu.make_async_copy(buf.at[span(j, size)], out_hbm.at[span(j, size)], write_sem.at[j])

    def each(fn):
        def step(j, carry):
            fn(j, EMB_BLOCK)
            return carry

        lax.fori_loop(0, full, step, 0)
        if tail:
            fn(full, tail)

    load_starts = pltpu.make_async_copy(starts_ref, starts_sm, grad_sem.at[2])
    load_starts.start()

    step_n = 2 * tok_n
    for i in range(n_chunk // 2):
        x = jnp.concatenate([x_ref[2 * i], x_ref[2 * i + 1]], axis=0)
        g = jnp.concatenate([g_ref[2 * i], g_ref[2 * i + 1]], axis=0)
        a = dot_nn(x, wup_ref[...]).astype(BF16).astype(F32)
        sq = a * a
        t = jnp.tanh(GELU_C * (a + 0.044715 * (sq * a)))
        cdf = 0.5 * (1.0 + t)
        hid[i * step_n:(i + 1) * step_n, :] = (a * cdf).astype(BF16)
        slope = cdf + (0.5 * a) * (1.0 - t * t) * (GELU_C * (1.0 + (3.0 * 0.044715) * sq))
        dh = dot_nt(g, wdn_ref[...]).astype(BF16).astype(F32)
        da[i * step_n:(i + 1) * step_n, :] = (dh * slope).astype(BF16)
    gup[...] = dot_tn(x_ref[...].reshape(n_chunk * tok_n, dim), da[...])
    gdn[...] = jnp.transpose(dot_tn(g_ref[...].reshape(n_chunk * tok_n, dim), hid[...]))
    grads = [pltpu.make_async_copy(gup, gup_hbm, grad_sem.at[0]), pltpu.make_async_copy(gdn, gdn_hbm, grad_sem.at[1])]
    for copy in grads:
        copy.start()
    loss_ref[0] = jnp.sum(st_ref[:, 2, :]) * (1.0 / (n_chunk * tok_n))

    row_id = lax.broadcasted_iota(jnp.int32, (tok_n, tok_n), 0)
    for c in range(n_chunk):
        acc = jnp.zeros((tok_n, dim), F32)
        for i in range(n_chunk):
            hot = jnp.where(rank_ref[i:i + 1, :] == row_id + c * tok_n, 1.0, 0.0).astype(BF16)
            acc = acc + dot_nn(hot, dx_ref[i])
        dxs[c] = acc.astype(BF16)
    dxs[n_chunk] = jnp.zeros((tok_n, dim), BF16)

    def add_tokens(j, size):
        rows = span(j, size)
        row16 = lax.broadcasted_iota(jnp.int16, (size, tok_n), 0)

        def hot_rows(c):
            ids = jnp.broadcast_to(ids_ref[c, 0:1, :] - j * EMB_BLOCK, (16, tok_n)).astype(jnp.int16)
            return jnp.where(row16 == ids[0:1, :], jnp.ones((), BF16), jnp.zeros((), BF16))

        first = jnp.minimum(starts_sm[0, j] // tok_n, n_chunk - 1)
        last = (starts_sm[0, j + 1] + tok_n - 1) // tok_n
        buf[rows, :] = part_ref[rows, :] + dot_nn(jnp.concatenate([hot_rows(first), hot_rows(first + 1)], axis=1),
                               jnp.concatenate([dxs[first], dxs[first + 1]], axis=0))

        def more(c, carry):
            buf[rows, :] += dot_nn(hot_rows(c), dxs[c])
            return carry

        lax.fori_loop(first + 2, last, more, 0)
        write(j, size).start()

    load_starts.wait()
    each(add_tokens)
    each(lambda j, size: write(j, size).wait())
    for copy in grads:
        copy.wait()


def solution(mesh):
    n_stage = mesh.shape["stage"]

    def device_fn(tokens, labels, emb_table, w_up, w_down):
        vocab, dim = emb_table.shape
        ffn = w_up.shape[2]
        total = tokens.shape[0] * tokens.shape[1]
        tok_n = total // n_stage
        w_up, w_down = w_up[0], w_down[0]
        hbm = pl.BlockSpec(memory_space=pl.ANY)
        vmem = pl.BlockSpec(memory_space=pltpu.VMEM)
        dma = pltpu.SemaphoreType.DMA
        act = pltpu.VMEM((n_stage, tok_n, dim), BF16)
        st_all, xs_all, gs_all, dx_all, part, ids, rank, wup_own, wdn_own, starts = pl.pallas_call(
            functools.partial(token_kernel, n_stage),
            out_shape=[pltpu.VMEM((n_stage, 8, tok_n), F32), act, act, act, pltpu.VMEM((vocab, dim), F32),
                       pltpu.VMEM((n_stage + 1, 8, tok_n), jnp.int32), pltpu.VMEM((n_stage, tok_n), jnp.int32),
                       pltpu.VMEM((dim, ffn), BF16), pltpu.VMEM((ffn, dim), BF16),
                       pltpu.VMEM((1, tok_n), jnp.int32)],
            in_specs=[hbm] * 5,
            out_specs=[vmem] * 10,
            scratch_shapes=[
                pltpu.VMEM(tokens.shape, jnp.int32), pltpu.VMEM(labels.shape, jnp.int32),
                pltpu.VMEM((n_stage, dim, ffn), BF16), pltpu.VMEM((n_stage, ffn, dim), BF16),
                pltpu.VMEM((vocab, dim), BF16), pltpu.VMEM((tok_n, vocab), BF16),
                pltpu.VMEM((n_stage + 1, tok_n, dim), BF16), pltpu.VMEM((n_stage + 1, tok_n, dim), BF16),
                pltpu.VMEM((n_stage, tok_n, ffn), BF16), pltpu.VMEM((n_stage, tok_n, dim), BF16),
                pltpu.VMEM((2 * tok_n, dim), F32),
                pltpu.VMEM((dim, total), BF16), pltpu.VMEM((8, total), F32), pltpu.VMEM((16, total), BF16),
                dma((5,)), dma((14,))] + [dma((n_stage,))] * 12 + [dma((pl.cdiv(vocab // 2, TABLE_BLOCK),))] * 2,
            compiler_params=pltpu.CompilerParams(collective_id=0, has_side_effects=True, vmem_limit_bytes=TOKEN_VMEM),
            name="token_pass",
        )(tokens, labels, emb_table, w_up, w_down)

        smem = pl.BlockSpec(memory_space=pltpu.SMEM)
        n_blk = pl.cdiv(vocab, EMB_BLOCK)
        grad_emb, grad_up, grad_down, loss = pl.pallas_call(
            finish_kernel,
            out_shape=[jax.ShapeDtypeStruct((vocab, dim), F32), jax.ShapeDtypeStruct((dim, ffn), F32),
                       jax.ShapeDtypeStruct((ffn, dim), F32), jax.ShapeDtypeStruct((1,), F32)],
            in_specs=[vmem] * 10, out_specs=[hbm, hbm, hbm, smem],
            scratch_shapes=[
                pltpu.SMEM((1, tok_n), jnp.int32),
                pltpu.VMEM((vocab, dim), F32), pltpu.VMEM((n_stage + 1, tok_n, dim), BF16),
                pltpu.VMEM((total, ffn), BF16), pltpu.VMEM((total, ffn), BF16),
                pltpu.VMEM((dim, ffn), F32), pltpu.VMEM((ffn, dim), F32), dma((n_blk,)), dma((3,))],
            compiler_params=pltpu.CompilerParams(vmem_limit_bytes=FINISH_VMEM),
            name="finish",
        )(starts, part, xs_all, gs_all, wup_own, wdn_own, st_all, dx_all, ids, rank)
        return loss, grad_up[None], grad_down[None], grad_emb

    return jax.shard_map(
        device_fn, mesh=mesh,
        in_specs=(P("dp", None), P("dp", None), P(None, None), P("stage", None, None), P("stage", None, None)),
        out_specs=(P("dp"), P(("dp", "stage"), None, None), P(("dp", "stage"), None, None), P("dp", None)),
        check_vma=False)
```

```python
import functools
import math

import jax
import jax.numpy as jnp
from jax import lax
from jax.experimental import pallas as pl
from jax.experimental.pallas import tpu as pltpu
from jax.sharding import PartitionSpec as P

MESH = pl.DeviceIdType.MESH
F32 = jnp.float32
BF16 = jnp.bfloat16
LOG2E = math.log2(math.e)
LN2 = math.log(2.0)
GELU_C = math.sqrt(2.0 / math.pi)
HEAD_BLOCK = 4096
TABLE_BLOCK = 2048
EMB_BLOCK = 2048
TOKEN_VMEM = 46 * 1024 * 1024
FINISH_VMEM = 28 * 1024 * 1024


def dot_nn(a, b):
    return lax.dot_general(a, b, (((1,), (0,)), ((), ())), preferred_element_type=F32)


def dot_nt(a, b):
    return lax.dot_general(a, b, (((1,), (1,)), ((), ())), preferred_element_type=F32)


def dot_tn(a, b):
    return lax.dot_general(a, b, (((0,), (0,)), ((), ())), preferred_element_type=F32)


def gelu_value(a):
    return a * (0.5 * (1.0 + jnp.tanh(GELU_C * (a + 0.044715 * (a * a * a)))))


def gelu_slope(a):
    sq = a * a
    t = jnp.tanh(GELU_C * (a + 0.044715 * (sq * a)))
    return 0.5 * (1.0 + t) + (0.5 * a) * (1.0 - t * t) * (GELU_C * (1.0 + (3.0 * 0.044715) * sq))


def column_of(row, size):
    return jnp.transpose(jnp.broadcast_to(row, (size, size)))


def joined_row(ref, i, size):
    per = size // ref.shape[1]
    return jnp.concatenate([ref[pl.ds(i * per + k, 1), :] for k in range(per)], axis=1)


def row_of(col, size):
    eye = lax.broadcasted_iota(jnp.int32, (size, size), 0) == lax.broadcasted_iota(jnp.int32, (size, size), 1)
    return jnp.sum(jnp.where(eye, jnp.broadcast_to(col, (size, size)), 0.0), axis=0, keepdims=True)


def token_kernel(
    n_stage, tok_hbm, lab_hbm, emb_hbm, wup_hbm, wdn_hbm,
    st_all, table_out, ids_out, starts_out, dxs, gup_out, gdn_out,
    tok_ref, lab_ref, rank_out, xs_out, gs_out, dx_out, hid, da_buf,
    wup, wdn, emb, z_buf, xs, gs, pre, n_all, gat, n_t, level_t, d_lab_t,
    loc_sem, wsend, upr, dnr, xsend, xrecv, gsend, grecv, nsend, nrecv, ssend, srecv, dsend, drecv, tsend, trecv,
):
    me = lax.axis_index("stage")
    n_chip = n_stage // 2
    chip, core = me // 2, lax.rem(me, 2)
    sib = chip * 2 + (1 - core)
    right = lax.rem(chip + 1, n_chip) * 2 + core
    left = lax.rem(chip + n_chip - 1, n_chip) * 2 + core
    far = lax.rem(chip + 2, n_chip) * 2 + core
    peers = [lax.rem(me + d, n_stage) for d in range(1, n_stage)]
    _, tok_n, dim = n_all.shape
    vocab = emb.shape[0]
    total = n_stage * tok_n
    scale = dim ** -0.5

    load_up = pltpu.make_async_copy(wup_hbm, wup.at[me], loc_sem.at[0])
    load_dn = pltpu.make_async_copy(wdn_hbm, wdn.at[me], loc_sem.at[1])
    load_emb = pltpu.make_async_copy(emb_hbm, emb, loc_sem.at[2])
    load_tok = pltpu.make_async_copy(tok_hbm, tok_ref, loc_sem.at[3])
    load_lab = pltpu.make_async_copy(lab_hbm, lab_ref, loc_sem.at[4])
    for copy in (load_up, load_dn, load_tok, load_lab, load_emb):
        copy.start()

    barrier = pltpu.get_barrier_semaphore()
    for peer in (right, left, sib):
        pl.semaphore_signal(barrier, inc=1, device_id={"stage": peer}, device_id_type=MESH)
    pl.semaphore_wait(barrier, 3)
    load_up.wait()
    load_dn.wait()

    def up_copy(i, slot, dst):
        return pltpu.make_async_remote_copy(
            wup.at[slot], wup.at[slot], wsend.at[i], upr.at[slot], device_id={"stage": dst}, device_id_type=MESH)

    def dn_copy(i, slot, dst):
        return pltpu.make_async_remote_copy(
            wdn.at[slot], wdn.at[slot], wsend.at[i], dnr.at[slot], device_id={"stage": dst}, device_id_type=MESH)

    first = [up_copy(0, me, right), dn_copy(1, me, left), dn_copy(2, me, right), up_copy(3, me, left),
             up_copy(4, me, sib), dn_copy(5, me, sib)]
    for copy in first:
        copy.start()

    load_tok.wait()
    load_lab.wait()
    tok_row = jnp.concatenate([joined_row(tok_ref, i, tok_n) for i in range(n_stage)], axis=0)
    pos = lax.broadcasted_iota(jnp.int32, (n_stage, tok_n), 0) * tok_n + lax.broadcasted_iota(jnp.int32, (n_stage, tok_n), 1)
    key_row = tok_row * total + pos
    lane = lax.broadcasted_iota(jnp.int32, (tok_n, tok_n), 1)
    key_cols = [column_of(key_row[j:j + 1, :], tok_n) for j in range(n_stage)]
    tok_cols = [column_of(tok_row[j:j + 1, :], tok_n) for j in range(n_stage)]
    rank_rows = []
    for i in range(n_stage):
        acc = jnp.zeros((tok_n, tok_n), jnp.int32)
        for j in range(n_stage):
            acc = acc + jnp.where(key_cols[j] < key_row[i:i + 1, :], 1, 0)
        rank_rows.append(jnp.sum(acc, axis=0, keepdims=True))
    rank_cols = [column_of(r, tok_n) for r in rank_rows]
    for c in range(n_stage):
        acc = jnp.zeros((tok_n, tok_n), jnp.int32)
        for j in range(n_stage):
            acc = acc + jnp.where(rank_cols[j] == lane + c * tok_n, tok_cols[j], 0)
        ids_out[c] = jnp.broadcast_to(jnp.sum(acc, axis=0, keepdims=True), (8, tok_n))
    ids_out[n_stage] = jnp.full((8, tok_n), -1, jnp.int32)
    acc = jnp.zeros((tok_n, tok_n), jnp.int32)
    for j in range(n_stage):
        acc = acc + jnp.where(tok_cols[j] < lane * EMB_BLOCK, 1, 0)
    starts_out[...] = jnp.sum(acc, axis=0, keepdims=True)
    for i in range(n_stage):
        rank_out[i:i + 1, :] = rank_rows[i]

    load_emb.wait()
    pick = jnp.concatenate(
        [column_of(joined_row(tok_ref, me, tok_n), tok_n), column_of(joined_row(lab_ref, me, tok_n), tok_n)], axis=0)
    lane2 = lax.broadcasted_iota(jnp.int32, (2 * tok_n, tok_n), 1)

    head_full = vocab // HEAD_BLOCK

    def blocks(body, lo=0, hi=head_full):
        def step(i, carry):
            body(pl.multiple_of(i * HEAD_BLOCK, HEAD_BLOCK), HEAD_BLOCK)
            return carry

        lax.fori_loop(lo, hi, step, 0)
        if hi == head_full and vocab % HEAD_BLOCK:
            body(head_full * HEAD_BLOCK, vocab % HEAD_BLOCK)

    gat[...] = jnp.zeros_like(gat)

    def gather_block(v0, size):
        hot = jnp.concatenate(
            [jnp.where(pick == lane2 + (v0 + j * tok_n), 1.0, 0.0).astype(BF16) for j in range(size // tok_n)], axis=1)
        gat[...] += dot_nn(hot, emb[pl.ds(v0, size), :])

    blocks(gather_block, 0, head_full // 2)

    up_copy(0, left, sib).wait_recv()
    second = [up_copy(6, left, right), up_copy(7, left, sib)]
    second[0].start()
    second[1].start()
    dn_copy(0, right, sib).wait_recv()
    second += [dn_copy(8, right, left), dn_copy(9, right, sib)]
    second[2].start()
    second[3].start()

    blocks(gather_block, head_full // 2, head_full)
    x0 = gat[0:tok_n, :].astype(BF16)
    lab_rows = gat[tok_n:2 * tok_n, :]
    lab_bf = lab_rows.astype(BF16)

    dn_copy(0, left, sib).wait_recv()
    second.append(dn_copy(10, left, sib))
    second[4].start()
    up_copy(0, right, sib).wait_recv()
    second.append(up_copy(11, right, sib))
    second[5].start()
    up_copy(0, far, sib).wait_recv()
    second.append(up_copy(12, far, sib))
    second[6].start()
    dn_copy(0, far, sib).wait_recv()
    second.append(dn_copy(13, far, sib))
    second[7].start()

    def x_copy(layer):
        return pltpu.make_async_remote_copy(
            xs.at[layer], xs_out.at[me], xsend.at[layer], xrecv.at[me], device_id={"stage": layer}, device_id_type=MESH)

    def g_copy(layer):
        return pltpu.make_async_remote_copy(
            gs.at[layer + 1], gs_out.at[me], gsend.at[layer], grecv.at[me], device_id={"stage": layer}, device_id_type=MESH)


    xs[0] = x0

    def forward(layer, carry):
        @pl.when(lax.rem(layer, 2) != core)
        def _():
            up_copy(0, layer, sib).wait_recv()
            dn_copy(0, layer, sib).wait_recv()

        x = xs[layer]
        a = dot_nn(x, wup[layer]).astype(BF16)
        pre[layer] = a
        h = gelu_value(a.astype(F32)).astype(BF16)
        xs[layer + 1] = (x.astype(F32) + dot_nn(h, wdn[layer])).astype(BF16)

        @pl.when(layer != me)
        def _():
            x_copy(layer).start()

        @pl.when(layer == me)
        def _():
            xs_out[me] = x

        return carry

    lax.fori_loop(0, n_stage, forward, 0)

    x_last = xs[n_stage].astype(F32)
    inv = lax.rsqrt(jnp.mean(x_last * x_last, axis=-1, keepdims=True) + 1e-6)
    n_val = (x_last * inv).astype(BF16)
    n_all[me] = n_val

    def spread(src, dst, send, recv):
        return [pltpu.make_async_remote_copy(src, dst.at[me], send.at[d], recv.at[me], device_id={"stage": peer},
                                             device_id_type=MESH) for d, peer in enumerate(peers)]

    def stat_block(v0, size):
        z = (dot_nt(n_all[me], emb[pl.ds(v0, size), :]) * scale).astype(BF16)
        z_buf[:, pl.ds(v0, size)] = z
        parts = [z[:, j * tok_n:(j + 1) * tok_n].astype(F32) for j in range(size // tok_n)]
        m_old = gat[0:tok_n, :]
        m_new = functools.reduce(jnp.maximum, parts, m_old)
        s_new = gat[tok_n:2 * tok_n, :] * jnp.exp2((m_old - m_new) * LOG2E)
        for part in parts:
            s_new = s_new + jnp.exp2((part - m_new) * LOG2E)
        gat[0:tok_n, :] = m_new
        gat[tok_n:2 * tok_n, :] = s_new

    gat[0:tok_n, :] = jnp.full((tok_n, dim), -1e30, F32)
    gat[tok_n:2 * tok_n, :] = jnp.zeros((tok_n, dim), F32)
    send_n = spread(n_all.at[me], n_all, nsend, nrecv)
    for copy in send_n:
        copy.start()
    blocks(stat_block)
    m_lane = gat[0:tok_n, :]
    m_tok = jnp.max(m_lane, axis=-1, keepdims=True)
    s_tok = jnp.sum(gat[tok_n:2 * tok_n, :] * jnp.exp2((m_lane - m_tok) * LOG2E), axis=-1, keepdims=True)
    lse = m_tok + jnp.log(s_tok)
    level = lse * LOG2E + math.log2(total)
    z_pair = (dot_nt(n_val, lab_bf) * scale).astype(BF16).astype(F32)
    eye = lax.broadcasted_iota(jnp.int32, (tok_n, tok_n), 0) == lane
    z_lab = jnp.sum(jnp.where(eye, z_pair, 0.0), axis=-1, keepdims=True)
    p_lab = jnp.exp2(z_lab * LOG2E - level)
    d_lab = (p_lab - 1.0 / total).astype(BF16).astype(F32)
    p_lab = p_lab.astype(BF16).astype(F32)
    st_all[me] = jnp.concatenate(
        [row_of(level, tok_n), row_of(d_lab, tok_n), row_of(lse - z_lab, tok_n), jnp.zeros((5, tok_n), F32)], axis=0)
    level_full = jnp.broadcast_to(level, (tok_n, tok_n))

    gat[0:tok_n, :] = (d_lab - p_lab) * lab_rows
    send_s = spread(st_all.at[me], st_all, ssend, srecv)
    for copy in send_s:
        copy.start()

    def grad_block(v0, size):
        parts = []
        for j in range(size // tok_n):
            z = z_buf[:, pl.ds(v0 + j * tok_n, tok_n)].astype(F32)
            parts.append(jnp.exp2(z * LOG2E - level_full).astype(BF16))
        gat[0:tok_n, :] += dot_nn(jnp.concatenate(parts, axis=1), emb[pl.ds(v0, size), :])

    blocks(grad_block)
    dn = (gat[0:tok_n, :] * scale).astype(BF16).astype(F32)
    corr = jnp.mean(dn * x_last, axis=-1, keepdims=True)
    gs[n_stage] = (inv * dn - x_last * (inv * inv * inv * corr)).astype(BF16)

    def backward(layer):
        g = gs[layer + 1]
        dh = dot_nt(g, wdn[layer]).astype(BF16).astype(F32)
        da = (dh * gelu_slope(pre[layer].astype(F32))).astype(BF16)
        gs[layer] = (g.astype(F32) + dot_nt(da, wup[layer])).astype(BF16)

    def send_g(layer):
        @pl.when(layer != me)
        def _():
            g_copy(layer).start()

        @pl.when(layer == me)
        def _():
            gs_out[me] = gs[layer + 1]

    def back_step(i, carry):
        layer = n_stage - 1 - i
        backward(layer)
        send_g(layer)
        return carry

    lax.fori_loop(0, n_stage, back_step, 0)
    send_d = spread(gs.at[0], dx_out, dsend, drecv)
    for copy in send_d:
        copy.start()
    dx_out[me] = gs[0]

    for peer in peers:
        for buf, send, recv in ((n_all, nsend, nrecv), (st_all, ssend, srecv)):
            pltpu.make_async_remote_copy(buf.at[peer], buf.at[peer], send.at[0], recv.at[peer],
                                         device_id={"stage": peer}, device_id_type=MESH).wait_recv()
    for i in range(n_stage):
        cols = slice(i * tok_n, (i + 1) * tok_n)
        n_t[:, cols] = jnp.transpose(n_all[i])
        level_t[:, cols] = jnp.broadcast_to(st_all[i, 0:1, :], (8, tok_n))
        d_lab_t[:, cols] = jnp.broadcast_to(st_all[i, 1:2, :], (16, tok_n)).astype(BF16)
    half = vocab // 2
    wide = 2 * tok_n

    def table_copies(j, size):
        rows = pl.ds(pl.multiple_of(core * half + j * TABLE_BLOCK, 16), size)
        return (pltpu.make_async_remote_copy(table_out.at[rows], table_out.at[rows], tsend.at[j], trecv.at[j],
                                             device_id={"stage": sib}, device_id_type=MESH),)

    def table_start(j, size):
        for copy in table_copies(j, size):
            copy.start()

    def table_block(j, size):
        base = pl.multiple_of(core * half + j * TABLE_BLOCK, 16)
        e = emb[pl.ds(base, size), :]
        row16 = lax.broadcasted_iota(jnp.int16, (size, wide), 0)
        acc = jnp.zeros((size, dim), F32)
        for t in range(total // wide):
            cols = slice(t * wide, (t + 1) * wide)
            z = (dot_nn(e, n_t[:, cols]) * scale).astype(BF16).astype(F32)
            p = jnp.exp2(z * LOG2E - level_t[0:1, cols]).astype(BF16)
            lab = jnp.concatenate([joined_row(lab_ref, 2 * t, tok_n), joined_row(lab_ref, 2 * t + 1, tok_n)], axis=1) - base
            lab = jnp.broadcast_to(lab, (16, wide)).astype(jnp.int16)
            dz = jnp.where(row16 == lab[0:1, :], d_lab_t[0:1, cols], p)
            acc = acc + dot_nn(dz, jnp.concatenate([n_all[2 * t], n_all[2 * t + 1]], axis=0))
        table_out[pl.ds(base, size), :] = acc * scale

    full, tail = half // TABLE_BLOCK, half % TABLE_BLOCK
    grad_tok = 2 * tok_n

    def table_step(j, carry):
        @pl.when(j > 0)
        def _():
            table_start(j - 1, TABLE_BLOCK)

        table_block(j, TABLE_BLOCK)
        return carry

    lax.fori_loop(0, full, table_step, 0)
    table_start(full - 1, TABLE_BLOCK)
    if tail:
        table_block(full, tail)
        table_start(full, tail)

    for peer in peers:
        pltpu.make_async_remote_copy(xs.at[peer], xs_out.at[peer], xsend.at[peer], xrecv.at[peer],
                                     device_id={"stage": peer}, device_id_type=MESH).wait()
        pltpu.make_async_remote_copy(gs.at[peer + 1], gs_out.at[peer], gsend.at[peer], grecv.at[peer],
                                     device_id={"stage": peer}, device_id_type=MESH).wait()
        pltpu.make_async_remote_copy(gs.at[0], dx_out.at[peer], dsend.at[0], drecv.at[peer],
                                     device_id={"stage": peer}, device_id_type=MESH).wait_recv()

    def weight_part(i):
        x = jnp.concatenate([xs_out[2 * i], xs_out[2 * i + 1]], axis=0)
        g = jnp.concatenate([gs_out[2 * i], gs_out[2 * i + 1]], axis=0)
        a = dot_nn(x, wup[me]).astype(BF16).astype(F32)
        sq = a * a
        t = jnp.tanh(GELU_C * (a + 0.044715 * (sq * a)))
        cdf = 0.5 * (1.0 + t)
        rows = slice(i * grad_tok, (i + 1) * grad_tok)
        hid[rows, :] = (a * cdf).astype(BF16)
        slope = cdf + (0.5 * a) * (1.0 - t * t) * (GELU_C * (1.0 + (3.0 * 0.044715) * sq))
        dh = dot_nt(g, wdn[me]).astype(BF16).astype(F32)
        da_buf[rows, :] = (dh * slope).astype(BF16)

    for i in range(n_stage // 2):
        weight_part(i)
    gup_out[...] = dot_tn(xs_out[...].reshape(total, dim), da_buf[...])
    gdn_out[...] = jnp.transpose(dot_tn(gs_out[...].reshape(total, dim), hid[...]))
    row_id = lax.broadcasted_iota(jnp.int32, (tok_n, tok_n), 0)
    for c in range(n_stage):
        acc = jnp.zeros((tok_n, dim), F32)
        for i in range(n_stage):
            hot = jnp.where(rank_out[i:i + 1, :] == row_id + c * tok_n, 1.0, 0.0).astype(BF16)
            acc = acc + dot_nn(hot, dx_out[i])
        dxs[c] = acc.astype(BF16)
    dxs[n_stage] = jnp.zeros((tok_n, dim), BF16)

    for copy in first + second + send_n + send_s:
        copy.wait_send()
    for copy in send_d:
        copy.wait_send()

    def table_wait(j, size):
        table_copies(j, size)[0].wait_send()
        rows = pl.ds(pl.multiple_of((1 - core) * half + j * TABLE_BLOCK, 16), size)
        pltpu.make_async_remote_copy(table_out.at[rows], table_out.at[rows],
                                     tsend.at[j], trecv.at[j], device_id={"stage": sib}, device_id_type=MESH).wait_recv()

    def wait_step(j, carry):
        table_wait(j, TABLE_BLOCK)
        return carry

    lax.fori_loop(0, full, wait_step, 0)
    if tail:
        table_wait(full, tail)


def finish_kernel(
    starts_ref, part_ref, st_ref, ids_ref, dxs, gup_ref, gdn_ref,
    out_hbm, gup_hbm, gdn_hbm, loss_ref,
    starts_sm, buf, write_sem, grad_sem,
):
    n_chunk, tok_n, _ = dxs.shape
    n_chunk = n_chunk - 1
    vocab = buf.shape[0]
    full, tail = vocab // EMB_BLOCK, vocab % EMB_BLOCK

    def span(j, size):
        return pl.ds(pl.multiple_of(j * EMB_BLOCK, 16), size)

    def write(j, size):
        return pltpu.make_async_copy(buf.at[span(j, size)], out_hbm.at[span(j, size)], write_sem.at[j])

    def each(fn):
        def step(j, carry):
            fn(j, EMB_BLOCK)
            return carry

        lax.fori_loop(0, full, step, 0)
        if tail:
            fn(full, tail)

    load_starts = pltpu.make_async_copy(starts_ref, starts_sm, grad_sem.at[2])
    load_starts.start()

    grads = [pltpu.make_async_copy(gup_ref, gup_hbm, grad_sem.at[0]), pltpu.make_async_copy(gdn_ref, gdn_hbm, grad_sem.at[1])]
    for copy in grads:
        copy.start()
    loss_ref[0] = jnp.sum(st_ref[:, 2, :]) * (1.0 / (n_chunk * tok_n))

    def add_tokens(j, size):
        rows = span(j, size)
        row16 = lax.broadcasted_iota(jnp.int16, (size, tok_n), 0)

        def hot_rows(c):
            ids = jnp.broadcast_to(ids_ref[c, 0:1, :] - j * EMB_BLOCK, (16, tok_n)).astype(jnp.int16)
            return jnp.where(row16 == ids[0:1, :], jnp.ones((), BF16), jnp.zeros((), BF16))

        first = jnp.minimum(starts_sm[0, j] // tok_n, n_chunk - 1)
        last = (starts_sm[0, j + 1] + tok_n - 1) // tok_n
        buf[rows, :] = part_ref[rows, :] + dot_nn(jnp.concatenate([hot_rows(first), hot_rows(first + 1)], axis=1),
                               jnp.concatenate([dxs[first], dxs[first + 1]], axis=0))

        def more(c, carry):
            buf[rows, :] += dot_nn(hot_rows(c), dxs[c])
            return carry

        lax.fori_loop(first + 2, last, more, 0)
        write(j, size).start()

    load_starts.wait()
    each(add_tokens)
    each(lambda j, size: write(j, size).wait())
    for copy in grads:
        copy.wait()


def solution(mesh):
    n_stage = mesh.shape["stage"]

    def device_fn(tokens, labels, emb_table, w_up, w_down):
        vocab, dim = emb_table.shape
        ffn = w_up.shape[2]
        total = tokens.shape[0] * tokens.shape[1]
        tok_n = total // n_stage
        w_up, w_down = w_up[0], w_down[0]
        hbm = pl.BlockSpec(memory_space=pl.ANY)
        vmem = pl.BlockSpec(memory_space=pltpu.VMEM)
        dma = pltpu.SemaphoreType.DMA
        act = pltpu.VMEM((n_stage, tok_n, dim), BF16)
        st_all, part, ids, starts, dxs, gup, gdn = pl.pallas_call(
            functools.partial(token_kernel, n_stage),
            out_shape=[pltpu.VMEM((n_stage, 8, tok_n), F32), pltpu.VMEM((vocab, dim), F32),
                       pltpu.VMEM((n_stage + 1, 8, tok_n), jnp.int32), pltpu.VMEM((1, tok_n), jnp.int32),
                       pltpu.VMEM((n_stage + 1, tok_n, dim), BF16), pltpu.VMEM((dim, ffn), F32), pltpu.VMEM((ffn, dim), F32)],
            in_specs=[hbm] * 5,
            out_specs=[vmem] * 7,
            scratch_shapes=[
                pltpu.VMEM(tokens.shape, jnp.int32), pltpu.VMEM(labels.shape, jnp.int32), pltpu.VMEM((n_stage, tok_n), jnp.int32),
                act, act, act, pltpu.VMEM((total, ffn), BF16), pltpu.VMEM((total, ffn), BF16),
                pltpu.VMEM((n_stage, dim, ffn), BF16), pltpu.VMEM((n_stage, ffn, dim), BF16),
                pltpu.VMEM((vocab, dim), BF16), pltpu.VMEM((tok_n, vocab), BF16),
                pltpu.VMEM((n_stage + 1, tok_n, dim), BF16), pltpu.VMEM((n_stage + 1, tok_n, dim), BF16),
                pltpu.VMEM((n_stage, tok_n, ffn), BF16), pltpu.VMEM((n_stage, tok_n, dim), BF16),
                pltpu.VMEM((2 * tok_n, dim), F32),
                pltpu.VMEM((dim, total), BF16), pltpu.VMEM((8, total), F32), pltpu.VMEM((16, total), BF16),
                dma((5,)), dma((14,))] + [dma((n_stage,))] * 12 + [dma((pl.cdiv(vocab // 2, TABLE_BLOCK),))] * 2,
            compiler_params=pltpu.CompilerParams(collective_id=0, has_side_effects=True, vmem_limit_bytes=TOKEN_VMEM),
            name="token_pass",
        )(tokens, labels, emb_table, w_up, w_down)

        smem = pl.BlockSpec(memory_space=pltpu.SMEM)
        n_blk = pl.cdiv(vocab, EMB_BLOCK)
        grad_emb, grad_up, grad_down, loss = pl.pallas_call(
            finish_kernel,
            out_shape=[jax.ShapeDtypeStruct((vocab, dim), F32), jax.ShapeDtypeStruct((dim, ffn), F32),
                       jax.ShapeDtypeStruct((ffn, dim), F32), jax.ShapeDtypeStruct((1,), F32)],
            in_specs=[vmem] * 7, out_specs=[hbm, hbm, hbm, smem],
            scratch_shapes=[
                pltpu.SMEM((1, tok_n), jnp.int32), pltpu.VMEM((vocab, dim), F32), dma((n_blk,)), dma((3,))],
            compiler_params=pltpu.CompilerParams(vmem_limit_bytes=FINISH_VMEM),
            name="finish",
        )(starts, part, st_all, ids, dxs, gup, gdn)
        return loss, grad_up[None], grad_down[None], grad_emb

    return jax.shard_map(
        device_fn, mesh=mesh,
        in_specs=(P("dp", None), P("dp", None), P(None, None), P("stage", None, None), P("stage", None, None)),
        out_specs=(P("dp"), P(("dp", "stage"), None, None), P(("dp", "stage"), None, None), P("dp", None)),
        check_vma=False)
```

```python
import functools
import math

import jax
import jax.numpy as jnp
from jax import lax
from jax.experimental import pallas as pl
from jax.experimental.pallas import tpu as pltpu
from jax.sharding import PartitionSpec as P

MESH = pl.DeviceIdType.MESH
F32 = jnp.float32
BF16 = jnp.bfloat16
LOG2E = math.log2(math.e)
LN2 = math.log(2.0)
GELU_C = math.sqrt(2.0 / math.pi)
HEAD_BLOCK = 8192
TABLE_BLOCK = 3648
EMB_BLOCK = 2048
WRITE_PARTS = 4
TOKEN_VMEM = 46 * 1024 * 1024
FINISH_VMEM = 28 * 1024 * 1024


def dot_nn(a, b):
    return lax.dot_general(a, b, (((1,), (0,)), ((), ())), preferred_element_type=F32)


def dot_nt(a, b):
    return lax.dot_general(a, b, (((1,), (1,)), ((), ())), preferred_element_type=F32)


def dot_tn(a, b):
    return lax.dot_general(a, b, (((0,), (0,)), ((), ())), preferred_element_type=F32)


def gelu_value(a):
    return a * (0.5 * (1.0 + jnp.tanh(GELU_C * (a + 0.044715 * (a * a * a)))))


def gelu_slope(a):
    sq = a * a
    t = jnp.tanh(GELU_C * (a + 0.044715 * (sq * a)))
    return 0.5 * (1.0 + t) + (0.5 * a) * (1.0 - t * t) * (GELU_C * (1.0 + (3.0 * 0.044715) * sq))


def column_of(row, size):
    return jnp.transpose(jnp.broadcast_to(row, (size, size)))


def joined_row(ref, i, size):
    per = size // ref.shape[1]
    return jnp.concatenate([ref[pl.ds(i * per + k, 1), :] for k in range(per)], axis=1)


def row_of(col, size):
    eye = lax.broadcasted_iota(jnp.int32, (size, size), 0) == lax.broadcasted_iota(jnp.int32, (size, size), 1)
    return jnp.sum(jnp.where(eye, jnp.broadcast_to(col, (size, size)), 0.0), axis=0, keepdims=True)


def token_kernel(
    n_stage, tok_hbm, lab_hbm, emb_hbm, wup_hbm, wdn_hbm,
    st_all, table_out, ids_out, starts_out, dxs, gup_out, gdn_out,
    tok_ref, lab_ref, rank_out, xs_out, gs_out, dx_out, hid, da_buf,
    wup, wdn, emb, z_buf, xs, gs, pre, n_all, gat, n_t, level_t, d_lab_t,
    loc_sem, wsend, upr, dnr, xsend, xrecv, gsend, grecv, nsend, nrecv, ssend, srecv, dsend, drecv, tsend, trecv,
):
    me = lax.axis_index("stage")
    n_chip = n_stage // 2
    chip, core = me // 2, lax.rem(me, 2)
    sib = chip * 2 + (1 - core)
    right = lax.rem(chip + 1, n_chip) * 2 + core
    left = lax.rem(chip + n_chip - 1, n_chip) * 2 + core
    far = lax.rem(chip + 2, n_chip) * 2 + core
    peers = [lax.rem(me + d, n_stage) for d in range(1, n_stage)]
    _, tok_n, dim = n_all.shape
    vocab = emb.shape[0]
    total = n_stage * tok_n
    scale = dim ** -0.5

    load_up = pltpu.make_async_copy(wup_hbm, wup.at[me], loc_sem.at[0])
    load_dn = pltpu.make_async_copy(wdn_hbm, wdn.at[me], loc_sem.at[1])
    load_emb = pltpu.make_async_copy(emb_hbm, emb, loc_sem.at[2])
    load_tok = pltpu.make_async_copy(tok_hbm, tok_ref, loc_sem.at[3])
    load_lab = pltpu.make_async_copy(lab_hbm, lab_ref, loc_sem.at[4])
    for copy in (load_up, load_dn, load_tok, load_lab, load_emb):
        copy.start()

    barrier = pltpu.get_barrier_semaphore()
    for peer in (right, left, sib):
        pl.semaphore_signal(barrier, inc=1, device_id={"stage": peer}, device_id_type=MESH)
    pl.semaphore_wait(barrier, 3)
    load_up.wait()
    load_dn.wait()

    def up_copy(i, slot, dst):
        return pltpu.make_async_remote_copy(
            wup.at[slot], wup.at[slot], wsend.at[i], upr.at[slot], device_id={"stage": dst}, device_id_type=MESH)

    def dn_copy(i, slot, dst):
        return pltpu.make_async_remote_copy(
            wdn.at[slot], wdn.at[slot], wsend.at[i], dnr.at[slot], device_id={"stage": dst}, device_id_type=MESH)

    first = [up_copy(0, me, right), dn_copy(1, me, left), dn_copy(2, me, right), up_copy(3, me, left),
             up_copy(4, me, sib), dn_copy(5, me, sib)]
    for copy in first:
        copy.start()

    load_tok.wait()
    load_lab.wait()
    tok_row = jnp.concatenate([joined_row(tok_ref, i, tok_n) for i in range(n_stage)], axis=0)
    pos = lax.broadcasted_iota(jnp.int32, (n_stage, tok_n), 0) * tok_n + lax.broadcasted_iota(jnp.int32, (n_stage, tok_n), 1)
    key_row = tok_row * total + pos
    lane = lax.broadcasted_iota(jnp.int32, (tok_n, tok_n), 1)
    key_cols = [column_of(key_row[j:j + 1, :], tok_n) for j in range(n_stage)]
    tok_cols = [column_of(tok_row[j:j + 1, :], tok_n) for j in range(n_stage)]
    rank_rows = []
    for i in range(n_stage):
        acc = jnp.zeros((tok_n, tok_n), jnp.int32)
        for j in range(n_stage):
            acc = acc + jnp.where(key_cols[j] < key_row[i:i + 1, :], 1, 0)
        rank_rows.append(jnp.sum(acc, axis=0, keepdims=True))
    rank_cols = [column_of(r, tok_n) for r in rank_rows]
    for c in range(n_stage):
        acc = jnp.zeros((tok_n, tok_n), jnp.int32)
        for j in range(n_stage):
            acc = acc + jnp.where(rank_cols[j] == lane + c * tok_n, tok_cols[j], 0)
        ids_out[c] = jnp.broadcast_to(jnp.sum(acc, axis=0, keepdims=True), (8, tok_n))
    ids_out[n_stage] = jnp.full((8, tok_n), -1, jnp.int32)
    acc = jnp.zeros((tok_n, tok_n), jnp.int32)
    for j in range(n_stage):
        acc = acc + jnp.where(tok_cols[j] < lane * EMB_BLOCK, 1, 0)
    starts_out[...] = jnp.sum(acc, axis=0, keepdims=True)
    for i in range(n_stage):
        rank_out[i:i + 1, :] = rank_rows[i]

    load_emb.wait()
    pick = jnp.concatenate(
        [column_of(joined_row(tok_ref, me, tok_n), tok_n), column_of(joined_row(lab_ref, me, tok_n), tok_n)], axis=0)
    lane2 = lax.broadcasted_iota(jnp.int32, (2 * tok_n, tok_n), 1)

    head_full = vocab // HEAD_BLOCK

    def blocks(body, lo=0, hi=head_full):
        def step(i, carry):
            body(pl.multiple_of(i * HEAD_BLOCK, HEAD_BLOCK), HEAD_BLOCK)
            return carry

        lax.fori_loop(lo, hi, step, 0)
        if hi == head_full and vocab % HEAD_BLOCK:
            body(head_full * HEAD_BLOCK, vocab % HEAD_BLOCK)

    gat[...] = jnp.zeros_like(gat)

    def gather_block(v0, size):
        hot = jnp.concatenate(
            [jnp.where(pick == lane2 + (v0 + j * tok_n), 1.0, 0.0).astype(BF16) for j in range(size // tok_n)], axis=1)
        gat[...] += dot_nn(hot, emb[pl.ds(v0, size), :])

    blocks(gather_block, 0, head_full // 2)

    up_copy(0, left, sib).wait_recv()
    second = [up_copy(6, left, right), up_copy(7, left, sib)]
    second[0].start()
    second[1].start()
    dn_copy(0, right, sib).wait_recv()
    second += [dn_copy(8, right, left), dn_copy(9, right, sib)]
    second[2].start()
    second[3].start()

    blocks(gather_block, head_full // 2, head_full)
    x0 = gat[0:tok_n, :].astype(BF16)
    lab_rows = gat[tok_n:2 * tok_n, :]
    lab_bf = lab_rows.astype(BF16)

    dn_copy(0, left, sib).wait_recv()
    second.append(dn_copy(10, left, sib))
    second[4].start()
    up_copy(0, right, sib).wait_recv()
    second.append(up_copy(11, right, sib))
    second[5].start()
    up_copy(0, far, sib).wait_recv()
    second.append(up_copy(12, far, sib))
    second[6].start()
    dn_copy(0, far, sib).wait_recv()
    second.append(dn_copy(13, far, sib))
    second[7].start()

    def x_copy(layer):
        return pltpu.make_async_remote_copy(
            xs.at[layer], xs_out.at[me], xsend.at[layer], xrecv.at[me], device_id={"stage": layer}, device_id_type=MESH)

    def g_copy(layer):
        return pltpu.make_async_remote_copy(
            gs.at[layer + 1], gs_out.at[me], gsend.at[layer], grecv.at[me], device_id={"stage": layer}, device_id_type=MESH)


    xs[0] = x0

    def forward(layer, carry):
        @pl.when(lax.rem(layer, 2) != core)
        def _():
            up_copy(0, layer, sib).wait_recv()
            dn_copy(0, layer, sib).wait_recv()

        x = xs[layer]
        a = dot_nn(x, wup[layer]).astype(BF16)
        pre[layer] = a
        h = gelu_value(a.astype(F32)).astype(BF16)
        xs[layer + 1] = (x.astype(F32) + dot_nn(h, wdn[layer])).astype(BF16)

        @pl.when(layer != me)
        def _():
            x_copy(layer).start()

        @pl.when(layer == me)
        def _():
            xs_out[me] = x

        return carry

    lax.fori_loop(0, n_stage, forward, 0)

    x_last = xs[n_stage].astype(F32)
    inv = lax.rsqrt(jnp.mean(x_last * x_last, axis=-1, keepdims=True) + 1e-6)
    n_val = (x_last * inv).astype(BF16)
    n_all[me] = n_val

    def spread(src, dst, send, recv):
        return [pltpu.make_async_remote_copy(src, dst.at[me], send.at[d], recv.at[me], device_id={"stage": peer},
                                             device_id_type=MESH) for d, peer in enumerate(peers)]

    def stat_block(v0, size):
        z = (dot_nt(n_all[me], emb[pl.ds(v0, size), :]) * scale).astype(BF16)
        z_buf[:, pl.ds(v0, size)] = z
        parts = [z[:, j * tok_n:(j + 1) * tok_n].astype(F32) for j in range(size // tok_n)]
        m_old = gat[0:tok_n, :]
        m_new = functools.reduce(jnp.maximum, parts, m_old)
        s_new = gat[tok_n:2 * tok_n, :] * jnp.exp2((m_old - m_new) * LOG2E)
        for part in parts:
            s_new = s_new + jnp.exp2((part - m_new) * LOG2E)
        gat[0:tok_n, :] = m_new
        gat[tok_n:2 * tok_n, :] = s_new

    gat[0:tok_n, :] = jnp.full((tok_n, dim), -1e30, F32)
    gat[tok_n:2 * tok_n, :] = jnp.zeros((tok_n, dim), F32)
    send_n = spread(n_all.at[me], n_all, nsend, nrecv)
    for copy in send_n:
        copy.start()
    blocks(stat_block)
    m_lane = gat[0:tok_n, :]
    m_tok = jnp.max(m_lane, axis=-1, keepdims=True)
    s_tok = jnp.sum(gat[tok_n:2 * tok_n, :] * jnp.exp2((m_lane - m_tok) * LOG2E), axis=-1, keepdims=True)
    lse = m_tok + jnp.log(s_tok)
    level = lse * LOG2E + math.log2(total)
    z_pair = (dot_nt(n_val, lab_bf) * scale).astype(BF16).astype(F32)
    eye = lax.broadcasted_iota(jnp.int32, (tok_n, tok_n), 0) == lane
    z_lab = jnp.sum(jnp.where(eye, z_pair, 0.0), axis=-1, keepdims=True)
    p_lab = jnp.exp2(z_lab * LOG2E - level)
    d_lab = (p_lab - 1.0 / total).astype(BF16).astype(F32)
    p_lab = p_lab.astype(BF16).astype(F32)
    st_all[me] = jnp.concatenate(
        [row_of(level, tok_n), row_of(d_lab, tok_n), row_of(lse - z_lab, tok_n), jnp.zeros((5, tok_n), F32)], axis=0)
    level_full = jnp.broadcast_to(level, (tok_n, tok_n))

    gat[0:tok_n, :] = (d_lab - p_lab) * lab_rows
    send_s = spread(st_all.at[me], st_all, ssend, srecv)
    for copy in send_s:
        copy.start()

    def grad_block(v0, size):
        parts = []
        for j in range(size // tok_n):
            z = z_buf[:, pl.ds(v0 + j * tok_n, tok_n)].astype(F32)
            parts.append(jnp.exp2(z * LOG2E - level_full).astype(BF16))
        gat[0:tok_n, :] += dot_nn(jnp.concatenate(parts, axis=1), emb[pl.ds(v0, size), :])

    blocks(grad_block)
    dn = (gat[0:tok_n, :] * scale).astype(BF16).astype(F32)
    corr = jnp.mean(dn * x_last, axis=-1, keepdims=True)
    gs[n_stage] = (inv * dn - x_last * (inv * inv * inv * corr)).astype(BF16)

    def backward(layer):
        g = gs[layer + 1]
        dh = dot_nt(g, wdn[layer]).astype(BF16).astype(F32)
        da = (dh * gelu_slope(pre[layer].astype(F32))).astype(BF16)
        gs[layer] = (g.astype(F32) + dot_nt(da, wup[layer])).astype(BF16)

    def send_g(layer):
        @pl.when(layer != me)
        def _():
            g_copy(layer).start()

        @pl.when(layer == me)
        def _():
            gs_out[me] = gs[layer + 1]

    def back_step(i, carry):
        layer = n_stage - 1 - i
        backward(layer)
        send_g(layer)
        return carry

    lax.fori_loop(0, n_stage, back_step, 0)
    send_d = spread(gs.at[0], dx_out, dsend, drecv)
    for copy in send_d:
        copy.start()
    dx_out[me] = gs[0]

    for peer in peers:
        for buf, send, recv in ((n_all, nsend, nrecv), (st_all, ssend, srecv)):
            pltpu.make_async_remote_copy(buf.at[peer], buf.at[peer], send.at[0], recv.at[peer],
                                         device_id={"stage": peer}, device_id_type=MESH).wait_recv()
    for i in range(n_stage):
        cols = slice(i * tok_n, (i + 1) * tok_n)
        n_t[:, cols] = jnp.transpose(n_all[i])
        level_t[:, cols] = jnp.broadcast_to(st_all[i, 0:1, :], (8, tok_n))
        d_lab_t[:, cols] = jnp.broadcast_to(st_all[i, 1:2, :], (16, tok_n)).astype(BF16)
    half = vocab // 2
    wide = 2 * tok_n

    def table_copies(j, size):
        rows = pl.ds(pl.multiple_of(core * half + j * TABLE_BLOCK, 16), size)
        return (pltpu.make_async_remote_copy(table_out.at[rows], table_out.at[rows], tsend.at[j], trecv.at[j],
                                             device_id={"stage": sib}, device_id_type=MESH),)

    def table_start(j, size):
        for copy in table_copies(j, size):
            copy.start()

    def table_block(j, size):
        base = pl.multiple_of(core * half + j * TABLE_BLOCK, 16)
        for r in range(0, size, 608):
            table_rows(base, j * TABLE_BLOCK + r, r, min(608, size - r))

    def table_rows(base, at, r, size):
        e = emb[pl.ds(pl.multiple_of(base + r, 16), size), :]
        row16 = lax.broadcasted_iota(jnp.int16, (size, wide), 0)
        acc = jnp.zeros((size, dim), F32)
        for t in range(total // wide):
            cols = slice(t * wide, (t + 1) * wide)
            z = (dot_nn(e, n_t[:, cols]) * scale).astype(BF16).astype(F32)
            p = jnp.exp2(z * LOG2E - level_t[0:1, cols]).astype(BF16)
            lab = jnp.concatenate([joined_row(lab_ref, 2 * t, tok_n), joined_row(lab_ref, 2 * t + 1, tok_n)], axis=1) - (base + r)
            lab = jnp.broadcast_to(lab, (16, wide)).astype(jnp.int16)
            dz = jnp.where(row16 == lab[0:1, :], d_lab_t[0:1, cols], p)
            acc = acc + dot_nn(dz, jnp.concatenate([n_all[2 * t], n_all[2 * t + 1]], axis=0))
        table_out[pl.ds(pl.multiple_of(base + r, 16), size), :] = acc * scale

    full, tail = half // TABLE_BLOCK, half % TABLE_BLOCK
    grad_tok = 2 * tok_n

    def table_step(j, carry):
        @pl.when(j > 0)
        def _():
            table_start(j - 1, TABLE_BLOCK)

        table_block(j, TABLE_BLOCK)
        return carry

    lax.fori_loop(0, full, table_step, 0)
    table_start(full - 1, TABLE_BLOCK)
    if tail:
        table_block(full, tail)
        table_start(full, tail)

    for peer in peers:
        pltpu.make_async_remote_copy(xs.at[peer], xs_out.at[peer], xsend.at[peer], xrecv.at[peer],
                                     device_id={"stage": peer}, device_id_type=MESH).wait()
        pltpu.make_async_remote_copy(gs.at[peer + 1], gs_out.at[peer], gsend.at[peer], grecv.at[peer],
                                     device_id={"stage": peer}, device_id_type=MESH).wait()
        pltpu.make_async_remote_copy(gs.at[0], dx_out.at[peer], dsend.at[0], drecv.at[peer],
                                     device_id={"stage": peer}, device_id_type=MESH).wait_recv()

    def weight_part(i):
        x = jnp.concatenate([xs_out[2 * i], xs_out[2 * i + 1]], axis=0)
        g = jnp.concatenate([gs_out[2 * i], gs_out[2 * i + 1]], axis=0)
        a = dot_nn(x, wup[me]).astype(BF16).astype(F32)
        sq = a * a
        t = jnp.tanh(GELU_C * (a + 0.044715 * (sq * a)))
        cdf = 0.5 * (1.0 + t)
        rows = slice(i * grad_tok, (i + 1) * grad_tok)
        hid[rows, :] = (a * cdf).astype(BF16)
        slope = cdf + (0.5 * a) * (1.0 - t * t) * (GELU_C * (1.0 + (3.0 * 0.044715) * sq))
        dh = dot_nt(g, wdn[me]).astype(BF16).astype(F32)
        da_buf[rows, :] = (dh * slope).astype(BF16)

    for i in range(n_stage // 2):
        weight_part(i)
    gup_out[...] = dot_tn(xs_out[...].reshape(total, dim), da_buf[...])
    gdn_out[...] = jnp.transpose(dot_tn(gs_out[...].reshape(total, dim), hid[...]))
    row_id = lax.broadcasted_iota(jnp.int32, (tok_n, tok_n), 0)
    for c in range(n_stage):
        acc = jnp.zeros((tok_n, dim), F32)
        for i in range(n_stage):
            hot = jnp.where(rank_out[i:i + 1, :] == row_id + c * tok_n, 1.0, 0.0).astype(BF16)
            acc = acc + dot_nn(hot, dx_out[i])
        dxs[c] = acc.astype(BF16)
    dxs[n_stage] = jnp.zeros((tok_n, dim), BF16)

    for copy in first + second + send_n + send_s:
        copy.wait_send()
    for copy in send_d:
        copy.wait_send()

    def table_wait(j, size):
        table_copies(j, size)[0].wait_send()
        rows = pl.ds(pl.multiple_of((1 - core) * half + j * TABLE_BLOCK, 16), size)
        pltpu.make_async_remote_copy(table_out.at[rows], table_out.at[rows],
                                     tsend.at[j], trecv.at[j], device_id={"stage": sib}, device_id_type=MESH).wait_recv()

    def wait_step(j, carry):
        table_wait(j, TABLE_BLOCK)
        return carry

    lax.fori_loop(0, full, wait_step, 0)
    if tail:
        table_wait(full, tail)


def finish_kernel(
    starts_ref, part_ref, st_ref, ids_ref, dxs, gup_ref, gdn_ref,
    out_hbm, gup_hbm, gdn_hbm, loss_ref,
    starts_sm, buf, write_sem, grad_sem,
):
    n_chunk, tok_n, _ = dxs.shape
    n_chunk = n_chunk - 1
    vocab = buf.shape[0]
    full, tail = vocab // EMB_BLOCK, vocab % EMB_BLOCK

    def span(j, size):
        return pl.ds(pl.multiple_of(j * EMB_BLOCK, 16), size)

    def write(j, size):
        part = size // WRITE_PARTS
        return [pltpu.make_async_copy(
            buf.at[pl.ds(pl.multiple_of(j * EMB_BLOCK + k * part, 8), part)],
            out_hbm.at[pl.ds(pl.multiple_of(j * EMB_BLOCK + k * part, 8), part)], write_sem.at[j, k]) for k in range(WRITE_PARTS)]

    def write_start(j, size):
        for k, copy in enumerate(write(j, size)):
            copy.start(priority=k % 2)

    def write_wait(j, size):
        for copy in write(j, size):
            copy.wait()

    def each(fn):
        def step(j, carry):
            fn(j, EMB_BLOCK)
            return carry

        lax.fori_loop(0, full, step, 0)
        if tail:
            fn(full, tail)

    load_starts = pltpu.make_async_copy(starts_ref, starts_sm, grad_sem.at[2])
    load_starts.start()

    grads = [pltpu.make_async_copy(gup_ref, gup_hbm, grad_sem.at[0]), pltpu.make_async_copy(gdn_ref, gdn_hbm, grad_sem.at[1])]
    for copy in grads:
        copy.start()
    loss_ref[0] = jnp.sum(st_ref[:, 2, :]) * (1.0 / (n_chunk * tok_n))

    def add_tokens(j, size):
        rows = span(j, size)
        row16 = lax.broadcasted_iota(jnp.int16, (size, tok_n), 0)

        def hot_rows(c):
            ids = jnp.broadcast_to(ids_ref[c, 0:1, :] - j * EMB_BLOCK, (16, tok_n)).astype(jnp.int16)
            return jnp.where(row16 == ids[0:1, :], jnp.ones((), BF16), jnp.zeros((), BF16))

        first = jnp.minimum(starts_sm[0, j] // tok_n, n_chunk - 1)
        last = (starts_sm[0, j + 1] + tok_n - 1) // tok_n
        buf[rows, :] = part_ref[rows, :] + dot_nn(jnp.concatenate([hot_rows(first), hot_rows(first + 1)], axis=1),
                               jnp.concatenate([dxs[first], dxs[first + 1]], axis=0))

        def more(c, carry):
            buf[rows, :] += dot_nn(hot_rows(c), dxs[c])
            return carry

        lax.fori_loop(first + 2, last, more, 0)
        write_start(j, size)

    load_starts.wait()
    each(add_tokens)
    each(write_wait)
    for copy in grads:
        copy.wait()


def solution(mesh):
    n_stage = mesh.shape["stage"]

    def device_fn(tokens, labels, emb_table, w_up, w_down):
        vocab, dim = emb_table.shape
        ffn = w_up.shape[2]
        total = tokens.shape[0] * tokens.shape[1]
        tok_n = total // n_stage
        w_up, w_down = w_up[0], w_down[0]
        hbm = pl.BlockSpec(memory_space=pl.ANY)
        vmem = pl.BlockSpec(memory_space=pltpu.VMEM)
        dma = pltpu.SemaphoreType.DMA
        act = pltpu.VMEM((n_stage, tok_n, dim), BF16)
        st_all, part, ids, starts, dxs, gup, gdn = pl.pallas_call(
            functools.partial(token_kernel, n_stage),
            out_shape=[pltpu.VMEM((n_stage, 8, tok_n), F32), pltpu.VMEM((vocab, dim), F32),
                       pltpu.VMEM((n_stage + 1, 8, tok_n), jnp.int32), pltpu.VMEM((1, tok_n), jnp.int32),
                       pltpu.VMEM((n_stage + 1, tok_n, dim), BF16), pltpu.VMEM((dim, ffn), F32), pltpu.VMEM((ffn, dim), F32)],
            in_specs=[hbm] * 5,
            out_specs=[vmem] * 7,
            scratch_shapes=[
                pltpu.VMEM(tokens.shape, jnp.int32), pltpu.VMEM(labels.shape, jnp.int32), pltpu.VMEM((n_stage, tok_n), jnp.int32),
                act, act, act, pltpu.VMEM((total, ffn), BF16), pltpu.VMEM((total, ffn), BF16),
                pltpu.VMEM((n_stage, dim, ffn), BF16), pltpu.VMEM((n_stage, ffn, dim), BF16),
                pltpu.VMEM((vocab, dim), BF16), pltpu.VMEM((tok_n, vocab), BF16),
                pltpu.VMEM((n_stage + 1, tok_n, dim), BF16), pltpu.VMEM((n_stage + 1, tok_n, dim), BF16),
                pltpu.VMEM((n_stage, tok_n, ffn), BF16), pltpu.VMEM((n_stage, tok_n, dim), BF16),
                pltpu.VMEM((2 * tok_n, dim), F32),
                pltpu.VMEM((dim, total), BF16), pltpu.VMEM((8, total), F32), pltpu.VMEM((16, total), BF16),
                dma((5,)), dma((14,))] + [dma((n_stage,))] * 12 + [dma((pl.cdiv(vocab // 2, TABLE_BLOCK),))] * 2,
            compiler_params=pltpu.CompilerParams(collective_id=0, has_side_effects=True, vmem_limit_bytes=TOKEN_VMEM),
            name="token_pass",
        )(tokens, labels, emb_table, w_up, w_down)

        smem = pl.BlockSpec(memory_space=pltpu.SMEM)
        n_blk = pl.cdiv(vocab, EMB_BLOCK)
        grad_emb, grad_up, grad_down, loss = pl.pallas_call(
            finish_kernel,
            out_shape=[jax.ShapeDtypeStruct((vocab, dim), F32), jax.ShapeDtypeStruct((dim, ffn), F32),
                       jax.ShapeDtypeStruct((ffn, dim), F32), jax.ShapeDtypeStruct((1,), F32)],
            in_specs=[vmem] * 7, out_specs=[hbm, hbm, hbm, smem],
            scratch_shapes=[
                pltpu.SMEM((1, tok_n), jnp.int32), pltpu.VMEM((vocab, dim), F32), dma((n_blk, WRITE_PARTS)), dma((3,))],
            compiler_params=pltpu.CompilerParams(vmem_limit_bytes=FINISH_VMEM),
            name="finish",
        )(starts, part, st_all, ids, dxs, gup, gdn)
        return loss, grad_up[None], grad_down[None], grad_emb

    return jax.shard_map(
        device_fn, mesh=mesh,
        in_specs=(P("dp", None), P("dp", None), P(None, None), P("stage", None, None), P("stage", None, None)),
        out_specs=(P("dp"), P(("dp", "stage"), None, None), P(("dp", "stage"), None, None), P("dp", None)),
        check_vma=False)
```

```python
import functools
import math

import jax
import jax.numpy as jnp
from jax import lax
from jax.experimental import pallas as pl
from jax.experimental.pallas import tpu as pltpu
from jax.sharding import PartitionSpec as P

MESH = pl.DeviceIdType.MESH
F32 = jnp.float32
BF16 = jnp.bfloat16
LOG2E = math.log2(math.e)
LN2 = math.log(2.0)
GELU_C = math.sqrt(2.0 / math.pi)
HEAD_BLOCK = 8192
TABLE_BLOCK = 3648
EMB_BLOCK = 2048
WRITE_PARTS = 1
TOKEN_VMEM = 46 * 1024 * 1024
FINISH_VMEM = 28 * 1024 * 1024


def dot_nn(a, b):
    return lax.dot_general(a, b, (((1,), (0,)), ((), ())), preferred_element_type=F32)


def dot_nt(a, b):
    return lax.dot_general(a, b, (((1,), (1,)), ((), ())), preferred_element_type=F32)


def dot_tn(a, b):
    return lax.dot_general(a, b, (((0,), (0,)), ((), ())), preferred_element_type=F32)


def gelu_value(a):
    return a * (0.5 * (1.0 + jnp.tanh(GELU_C * (a + 0.044715 * (a * a * a)))))


def gelu_slope(a):
    sq = a * a
    t = jnp.tanh(GELU_C * (a + 0.044715 * (sq * a)))
    return 0.5 * (1.0 + t) + (0.5 * a) * (1.0 - t * t) * (GELU_C * (1.0 + (3.0 * 0.044715) * sq))


def column_of(row, size):
    return jnp.transpose(jnp.broadcast_to(row, (size, size)))


def joined_row(ref, i, size):
    per = size // ref.shape[1]
    return jnp.concatenate([ref[pl.ds(i * per + k, 1), :] for k in range(per)], axis=1)


def row_of(col, size):
    eye = lax.broadcasted_iota(jnp.int32, (size, size), 0) == lax.broadcasted_iota(jnp.int32, (size, size), 1)
    return jnp.sum(jnp.where(eye, jnp.broadcast_to(col, (size, size)), 0.0), axis=0, keepdims=True)


def token_kernel(
    n_stage, tok_hbm, lab_hbm, emb_hbm, wup_hbm, wdn_hbm,
    st_all, table_out, ids_out, starts_out, dxs, gup_out, gdn_out,
    tok_ref, lab_ref, rank_out, xs_out, gs_out, dx_out, hid, da_buf,
    wup, wdn, emb, z_buf, xs, gs, pre, n_all, gat, n_t, level_t, d_lab_t,
    loc_sem, wsend, upr, dnr, xsend, xrecv, gsend, grecv, nsend, nrecv, ssend, srecv, dsend, drecv, tsend, trecv,
):
    me = lax.axis_index("stage")
    n_chip = n_stage // 2
    chip, core = me // 2, lax.rem(me, 2)
    sib = chip * 2 + (1 - core)
    right = lax.rem(chip + 1, n_chip) * 2 + core
    left = lax.rem(chip + n_chip - 1, n_chip) * 2 + core
    far = lax.rem(chip + 2, n_chip) * 2 + core
    peers = [lax.rem(me + d, n_stage) for d in range(1, n_stage)]
    _, tok_n, dim = n_all.shape
    vocab = emb.shape[0]
    total = n_stage * tok_n
    scale = dim ** -0.5

    load_up = pltpu.make_async_copy(wup_hbm, wup.at[me], loc_sem.at[0])
    load_dn = pltpu.make_async_copy(wdn_hbm, wdn.at[me], loc_sem.at[1])
    load_emb = pltpu.make_async_copy(emb_hbm, emb, loc_sem.at[2])
    load_tok = pltpu.make_async_copy(tok_hbm, tok_ref, loc_sem.at[3])
    load_lab = pltpu.make_async_copy(lab_hbm, lab_ref, loc_sem.at[4])
    for copy in (load_up, load_dn, load_tok, load_lab, load_emb):
        copy.start()

    barrier = pltpu.get_barrier_semaphore()
    for peer in (right, left, sib):
        pl.semaphore_signal(barrier, inc=1, device_id={"stage": peer}, device_id_type=MESH)
    pl.semaphore_wait(barrier, 3)
    load_up.wait()
    load_dn.wait()

    def up_copy(i, slot, dst):
        return pltpu.make_async_remote_copy(
            wup.at[slot], wup.at[slot], wsend.at[i], upr.at[slot], device_id={"stage": dst}, device_id_type=MESH)

    def dn_copy(i, slot, dst):
        return pltpu.make_async_remote_copy(
            wdn.at[slot], wdn.at[slot], wsend.at[i], dnr.at[slot], device_id={"stage": dst}, device_id_type=MESH)

    first = [up_copy(0, me, right), dn_copy(1, me, left), dn_copy(2, me, right), up_copy(3, me, left),
             up_copy(4, me, sib), dn_copy(5, me, sib)]
    for copy in first:
        copy.start()

    load_tok.wait()
    load_lab.wait()
    tok_row = jnp.concatenate([joined_row(tok_ref, i, tok_n) for i in range(n_stage)], axis=0)
    pos = lax.broadcasted_iota(jnp.int32, (n_stage, tok_n), 0) * tok_n + lax.broadcasted_iota(jnp.int32, (n_stage, tok_n), 1)
    key_row = tok_row * total + pos
    lane = lax.broadcasted_iota(jnp.int32, (tok_n, tok_n), 1)
    key_cols = [column_of(key_row[j:j + 1, :], tok_n) for j in range(n_stage)]
    tok_cols = [column_of(tok_row[j:j + 1, :], tok_n) for j in range(n_stage)]
    rank_rows = []
    for i in range(n_stage):
        acc = jnp.zeros((tok_n, tok_n), jnp.int32)
        for j in range(n_stage):
            acc = acc + jnp.where(key_cols[j] < key_row[i:i + 1, :], 1, 0)
        rank_rows.append(jnp.sum(acc, axis=0, keepdims=True))
    rank_cols = [column_of(r, tok_n) for r in rank_rows]
    for c in range(n_stage):
        acc = jnp.zeros((tok_n, tok_n), jnp.int32)
        for j in range(n_stage):
            acc = acc + jnp.where(rank_cols[j] == lane + c * tok_n, tok_cols[j], 0)
        ids_out[c] = jnp.broadcast_to(jnp.sum(acc, axis=0, keepdims=True), (8, tok_n))
    ids_out[n_stage] = jnp.full((8, tok_n), -1, jnp.int32)
    acc = jnp.zeros((tok_n, tok_n), jnp.int32)
    for j in range(n_stage):
        acc = acc + jnp.where(tok_cols[j] < lane * EMB_BLOCK, 1, 0)
    starts_out[...] = jnp.sum(acc, axis=0, keepdims=True)
    for i in range(n_stage):
        rank_out[i:i + 1, :] = rank_rows[i]

    load_emb.wait()
    pick = jnp.concatenate(
        [column_of(joined_row(tok_ref, me, tok_n), tok_n), column_of(joined_row(lab_ref, me, tok_n), tok_n)], axis=0)
    lane2 = lax.broadcasted_iota(jnp.int32, (2 * tok_n, tok_n), 1)

    head_full = vocab // HEAD_BLOCK

    def blocks(body, lo=0, hi=head_full):
        def step(i, carry):
            body(pl.multiple_of(i * HEAD_BLOCK, HEAD_BLOCK), HEAD_BLOCK)
            return carry

        lax.fori_loop(lo, hi, step, 0)
        if hi == head_full and vocab % HEAD_BLOCK:
            body(head_full * HEAD_BLOCK, vocab % HEAD_BLOCK)

    gat[...] = jnp.zeros_like(gat)
    zero = jnp.minimum(joined_row(tok_ref, 0, tok_n), 0).astype(F32)
    one = zero + 1.0

    def gather_block(v0, size):
        hot = jnp.concatenate(
            [jnp.where(pick == lane2 + (v0 + j * tok_n), one, zero).astype(BF16) for j in range(size // tok_n)], axis=1)
        gat[...] += dot_nn(hot, emb[pl.ds(v0, size), :])

    blocks(gather_block, 0, head_full // 2)

    up_copy(0, left, sib).wait_recv()
    second = [up_copy(6, left, right), up_copy(7, left, sib)]
    second[0].start()
    second[1].start()
    dn_copy(0, right, sib).wait_recv()
    second += [dn_copy(8, right, left), dn_copy(9, right, sib)]
    second[2].start()
    second[3].start()

    blocks(gather_block, head_full // 2, head_full)
    x0 = gat[0:tok_n, :].astype(BF16)
    lab_rows = gat[tok_n:2 * tok_n, :]
    lab_bf = lab_rows.astype(BF16)

    dn_copy(0, left, sib).wait_recv()
    second.append(dn_copy(10, left, sib))
    second[4].start()
    up_copy(0, right, sib).wait_recv()
    second.append(up_copy(11, right, sib))
    second[5].start()
    up_copy(0, far, sib).wait_recv()
    second.append(up_copy(12, far, sib))
    second[6].start()
    dn_copy(0, far, sib).wait_recv()
    second.append(dn_copy(13, far, sib))
    second[7].start()

    def x_copy(layer):
        return pltpu.make_async_remote_copy(
            xs.at[layer], xs_out.at[me], xsend.at[layer], xrecv.at[me], device_id={"stage": layer}, device_id_type=MESH)

    def g_copy(layer):
        return pltpu.make_async_remote_copy(
            gs.at[layer + 1], gs_out.at[me], gsend.at[layer], grecv.at[me], device_id={"stage": layer}, device_id_type=MESH)


    xs[0] = x0

    def forward(layer, carry):
        @pl.when(lax.rem(layer, 2) != core)
        def _():
            up_copy(0, layer, sib).wait_recv()
            dn_copy(0, layer, sib).wait_recv()

        x = xs[layer]
        a = dot_nn(x, wup[layer]).astype(BF16)
        pre[layer] = a
        h = gelu_value(a.astype(F32)).astype(BF16)
        xs[layer + 1] = (x.astype(F32) + dot_nn(h, wdn[layer])).astype(BF16)

        @pl.when(layer != me)
        def _():
            x_copy(layer).start()

        @pl.when(layer == me)
        def _():
            xs_out[me] = x

        return carry

    lax.fori_loop(0, n_stage, forward, 0)

    x_last = xs[n_stage].astype(F32)
    inv = lax.rsqrt(jnp.mean(x_last * x_last, axis=-1, keepdims=True) + 1e-6)
    n_val = (x_last * inv).astype(BF16)
    n_all[me] = n_val

    def spread(src, dst, send, recv):
        return [pltpu.make_async_remote_copy(src, dst.at[me], send.at[d], recv.at[me], device_id={"stage": peer},
                                             device_id_type=MESH) for d, peer in enumerate(peers)]

    def stat_block(v0, size):
        z = (dot_nt(n_all[me], emb[pl.ds(v0, size), :]) * scale).astype(BF16)
        z_buf[:, pl.ds(v0, size)] = z
        parts = [z[:, j * tok_n:(j + 1) * tok_n].astype(F32) for j in range(size // tok_n)]
        m_old = gat[0:tok_n, :]
        m_new = functools.reduce(jnp.maximum, parts, m_old)
        s_new = gat[tok_n:2 * tok_n, :] * jnp.exp2((m_old - m_new) * LOG2E)
        for part in parts:
            s_new = s_new + jnp.exp2((part - m_new) * LOG2E)
        gat[0:tok_n, :] = m_new
        gat[tok_n:2 * tok_n, :] = s_new

    gat[0:tok_n, :] = jnp.full((tok_n, dim), -1e30, F32)
    gat[tok_n:2 * tok_n, :] = jnp.zeros((tok_n, dim), F32)
    send_n = spread(n_all.at[me], n_all, nsend, nrecv)
    for copy in send_n:
        copy.start()
    blocks(stat_block)
    m_lane = gat[0:tok_n, :]
    m_tok = jnp.max(m_lane, axis=-1, keepdims=True)
    s_tok = jnp.sum(gat[tok_n:2 * tok_n, :] * jnp.exp2((m_lane - m_tok) * LOG2E), axis=-1, keepdims=True)
    lse = m_tok + jnp.log(s_tok)
    level = lse * LOG2E + math.log2(total)
    z_pair = (dot_nt(n_val, lab_bf) * scale).astype(BF16).astype(F32)
    eye = lax.broadcasted_iota(jnp.int32, (tok_n, tok_n), 0) == lane
    z_lab = jnp.sum(jnp.where(eye, z_pair, 0.0), axis=-1, keepdims=True)
    p_lab = jnp.exp2(z_lab * LOG2E - level)
    d_lab = (p_lab - 1.0 / total).astype(BF16).astype(F32)
    p_lab = p_lab.astype(BF16).astype(F32)
    st_all[me] = jnp.concatenate(
        [row_of(level, tok_n), row_of(d_lab, tok_n), row_of(lse - z_lab, tok_n), jnp.zeros((5, tok_n), F32)], axis=0)
    level_full = jnp.broadcast_to(level, (tok_n, tok_n))

    gat[0:tok_n, :] = (d_lab - p_lab) * lab_rows
    send_s = spread(st_all.at[me], st_all, ssend, srecv)
    for copy in send_s:
        copy.start()

    def grad_block(v0, size):
        parts = []
        for j in range(size // tok_n):
            z = z_buf[:, pl.ds(v0 + j * tok_n, tok_n)].astype(F32)
            parts.append(jnp.exp2(z * LOG2E - level_full).astype(BF16))
        gat[0:tok_n, :] += dot_nn(jnp.concatenate(parts, axis=1), emb[pl.ds(v0, size), :])

    blocks(grad_block)
    dn = (gat[0:tok_n, :] * scale).astype(BF16).astype(F32)
    corr = jnp.mean(dn * x_last, axis=-1, keepdims=True)
    gs[n_stage] = (inv * dn - x_last * (inv * inv * inv * corr)).astype(BF16)

    def backward(layer):
        g = gs[layer + 1]
        dh = dot_nt(g, wdn[layer]).astype(BF16).astype(F32)
        da = (dh * gelu_slope(pre[layer].astype(F32))).astype(BF16)
        gs[layer] = (g.astype(F32) + dot_nt(da, wup[layer])).astype(BF16)

    def send_g(layer):
        @pl.when(layer != me)
        def _():
            g_copy(layer).start()

        @pl.when(layer == me)
        def _():
            gs_out[me] = gs[layer + 1]

    def back_step(i, carry):
        layer = n_stage - 1 - i
        backward(layer)
        send_g(layer)
        return carry

    lax.fori_loop(0, n_stage, back_step, 0)
    send_d = spread(gs.at[0], dx_out, dsend, drecv)
    for copy in send_d:
        copy.start()
    dx_out[me] = gs[0]

    for peer in peers:
        for buf, send, recv in ((n_all, nsend, nrecv), (st_all, ssend, srecv)):
            pltpu.make_async_remote_copy(buf.at[peer], buf.at[peer], send.at[0], recv.at[peer],
                                         device_id={"stage": peer}, device_id_type=MESH).wait_recv()
    for i in range(n_stage):
        cols = slice(i * tok_n, (i + 1) * tok_n)
        n_t[:, cols] = jnp.transpose(n_all[i])
        level_t[:, cols] = jnp.broadcast_to(st_all[i, 0:1, :], (8, tok_n))
        d_lab_t[:, cols] = jnp.broadcast_to(st_all[i, 1:2, :], (16, tok_n)).astype(BF16)
    half = vocab // 2
    wide = 2 * tok_n

    def table_copies(j, size):
        rows = pl.ds(pl.multiple_of(core * half + j * TABLE_BLOCK, 16), size)
        return (pltpu.make_async_remote_copy(table_out.at[rows], table_out.at[rows], tsend.at[j], trecv.at[j],
                                             device_id={"stage": sib}, device_id_type=MESH),)

    def table_start(j, size):
        for copy in table_copies(j, size):
            copy.start()

    def table_block(j, size):
        base = pl.multiple_of(core * half + j * TABLE_BLOCK, 16)
        for r in range(0, size, 608):
            table_rows(base, j * TABLE_BLOCK + r, r, min(608, size - r))

    def table_rows(base, at, r, size):
        e = emb[pl.ds(pl.multiple_of(base + r, 16), size), :]
        row16 = lax.broadcasted_iota(jnp.int16, (size, wide), 0)
        acc = jnp.zeros((size, dim), F32)
        for t in range(total // wide):
            cols = slice(t * wide, (t + 1) * wide)
            z = (dot_nn(e, n_t[:, cols]) * scale).astype(BF16).astype(F32)
            p = jnp.exp2(z * LOG2E - level_t[0:1, cols]).astype(BF16)
            lab = jnp.concatenate([joined_row(lab_ref, 2 * t, tok_n), joined_row(lab_ref, 2 * t + 1, tok_n)], axis=1) - (base + r)
            lab = jnp.broadcast_to(lab, (16, wide)).astype(jnp.int16)
            dz = jnp.where(row16 == lab[0:1, :], d_lab_t[0:1, cols], p)
            acc = acc + dot_nn(dz, jnp.concatenate([n_all[2 * t], n_all[2 * t + 1]], axis=0))
        table_out[pl.ds(pl.multiple_of(base + r, 16), size), :] = acc * scale

    full, tail = half // TABLE_BLOCK, half % TABLE_BLOCK
    grad_tok = 2 * tok_n

    def table_step(j, carry):
        @pl.when(j > 0)
        def _():
            table_start(j - 1, TABLE_BLOCK)

        table_block(j, TABLE_BLOCK)
        return carry

    lax.fori_loop(0, full, table_step, 0)
    table_start(full - 1, TABLE_BLOCK)
    if tail:
        table_block(full, tail)
        table_start(full, tail)

    for peer in peers:
        pltpu.make_async_remote_copy(xs.at[peer], xs_out.at[peer], xsend.at[peer], xrecv.at[peer],
                                     device_id={"stage": peer}, device_id_type=MESH).wait()
        pltpu.make_async_remote_copy(gs.at[peer + 1], gs_out.at[peer], gsend.at[peer], grecv.at[peer],
                                     device_id={"stage": peer}, device_id_type=MESH).wait()
        pltpu.make_async_remote_copy(gs.at[0], dx_out.at[peer], dsend.at[0], drecv.at[peer],
                                     device_id={"stage": peer}, device_id_type=MESH).wait_recv()

    def weight_part(i):
        x = jnp.concatenate([xs_out[2 * i], xs_out[2 * i + 1]], axis=0)
        g = jnp.concatenate([gs_out[2 * i], gs_out[2 * i + 1]], axis=0)
        a = dot_nn(x, wup[me]).astype(BF16).astype(F32)
        sq = a * a
        t = jnp.tanh(GELU_C * (a + 0.044715 * (sq * a)))
        cdf = 0.5 * (1.0 + t)
        rows = slice(i * grad_tok, (i + 1) * grad_tok)
        hid[rows, :] = (a * cdf).astype(BF16)
        slope = cdf + (0.5 * a) * (1.0 - t * t) * (GELU_C * (1.0 + (3.0 * 0.044715) * sq))
        dh = dot_nt(g, wdn[me]).astype(BF16).astype(F32)
        da_buf[rows, :] = (dh * slope).astype(BF16)

    for i in range(n_stage // 2):
        weight_part(i)
    gup_out[...] = dot_tn(xs_out[...].reshape(total, dim), da_buf[...])
    gdn_out[...] = jnp.transpose(dot_tn(gs_out[...].reshape(total, dim), hid[...]))
    row_id = lax.broadcasted_iota(jnp.int32, (tok_n, tok_n), 0)
    for c in range(n_stage):
        acc = jnp.zeros((tok_n, dim), F32)
        for i in range(n_stage):
            hot = jnp.where(rank_out[i:i + 1, :] == row_id + c * tok_n, one, zero).astype(BF16)
            acc = acc + dot_nn(hot, dx_out[i])
        dxs[c] = acc.astype(BF16)
    dxs[n_stage] = jnp.zeros((tok_n, dim), BF16)

    for copy in first + second + send_n + send_s:
        copy.wait_send()
    for copy in send_d:
        copy.wait_send()

    def table_wait(j, size):
        table_copies(j, size)[0].wait_send()
        rows = pl.ds(pl.multiple_of((1 - core) * half + j * TABLE_BLOCK, 16), size)
        pltpu.make_async_remote_copy(table_out.at[rows], table_out.at[rows],
                                     tsend.at[j], trecv.at[j], device_id={"stage": sib}, device_id_type=MESH).wait_recv()

    def wait_step(j, carry):
        table_wait(j, TABLE_BLOCK)
        return carry

    lax.fori_loop(0, full, wait_step, 0)
    if tail:
        table_wait(full, tail)


def finish_kernel(
    starts_ref, part_ref, st_ref, ids_ref, dxs, gup_ref, gdn_ref,
    out_hbm, gup_hbm, gdn_hbm, loss_ref,
    starts_sm, buf, write_sem, grad_sem,
):
    n_chunk, tok_n, _ = dxs.shape
    n_chunk = n_chunk - 1
    vocab = buf.shape[0]
    full, tail = vocab // EMB_BLOCK, vocab % EMB_BLOCK

    def span(j, size):
        return pl.ds(pl.multiple_of(j * EMB_BLOCK, 16), size)

    def write(j, size):
        part = size // WRITE_PARTS
        return [pltpu.make_async_copy(
            buf.at[pl.ds(pl.multiple_of(j * EMB_BLOCK + k * part, 8), part)],
            out_hbm.at[pl.ds(pl.multiple_of(j * EMB_BLOCK + k * part, 8), part)], write_sem.at[j, k]) for k in range(WRITE_PARTS)]

    def write_start(j, size):
        for k, copy in enumerate(write(j, size)):
            copy.start(priority=k % 2)

    def write_wait(j, size):
        for copy in write(j, size):
            copy.wait()

    def each(fn):
        def step(j, carry):
            fn(j, EMB_BLOCK)
            return carry

        lax.fori_loop(0, full, step, 0)
        if tail:
            fn(full, tail)

    load_starts = pltpu.make_async_copy(starts_ref, starts_sm, grad_sem.at[2])
    load_starts.start()

    grads = [pltpu.make_async_copy(gup_ref, gup_hbm, grad_sem.at[0]), pltpu.make_async_copy(gdn_ref, gdn_hbm, grad_sem.at[1])]
    for copy in grads:
        copy.start()
    loss_ref[0] = jnp.sum(st_ref[:, 2, :]) * (1.0 / (n_chunk * tok_n))

    mark = jnp.broadcast_to(ids_ref[n_chunk, 0:1, :].astype(F32), (16, tok_n))
    one, zero = (-mark).astype(BF16)[0:1, :], (mark + 1.0).astype(BF16)[0:1, :]

    def add_tokens(j, size):
        rows = span(j, size)
        row16 = lax.broadcasted_iota(jnp.int16, (size, tok_n), 0)

        def hot_rows(c):
            ids = jnp.broadcast_to(ids_ref[c, 0:1, :] - j * EMB_BLOCK, (16, tok_n)).astype(jnp.int16)
            return jnp.where(row16 == ids[0:1, :], one, zero)

        first = jnp.minimum(starts_sm[0, j] // tok_n, n_chunk - 1)
        last = (starts_sm[0, j + 1] + tok_n - 1) // tok_n
        buf[rows, :] = part_ref[rows, :] + dot_nn(jnp.concatenate([hot_rows(first), hot_rows(first + 1)], axis=1),
                               jnp.concatenate([dxs[first], dxs[first + 1]], axis=0))

        def more(c, carry):
            buf[rows, :] += dot_nn(hot_rows(c), dxs[c])
            return carry

        lax.fori_loop(first + 2, last, more, 0)
        write_start(j, size)

    load_starts.wait()
    each(add_tokens)
    each(write_wait)
    for copy in grads:
        copy.wait()


def solution(mesh):
    n_stage = mesh.shape["stage"]

    def device_fn(tokens, labels, emb_table, w_up, w_down):
        vocab, dim = emb_table.shape
        ffn = w_up.shape[2]
        total = tokens.shape[0] * tokens.shape[1]
        tok_n = total // n_stage
        w_up, w_down = w_up[0], w_down[0]
        hbm = pl.BlockSpec(memory_space=pl.ANY)
        vmem = pl.BlockSpec(memory_space=pltpu.VMEM)
        dma = pltpu.SemaphoreType.DMA
        act = pltpu.VMEM((n_stage, tok_n, dim), BF16)
        st_all, part, ids, starts, dxs, gup, gdn = pl.pallas_call(
            functools.partial(token_kernel, n_stage),
            out_shape=[pltpu.VMEM((n_stage, 8, tok_n), F32), pltpu.VMEM((vocab, dim), F32),
                       pltpu.VMEM((n_stage + 1, 8, tok_n), jnp.int32), pltpu.VMEM((1, tok_n), jnp.int32),
                       pltpu.VMEM((n_stage + 1, tok_n, dim), BF16), pltpu.VMEM((dim, ffn), F32), pltpu.VMEM((ffn, dim), F32)],
            in_specs=[hbm] * 5,
            out_specs=[vmem] * 7,
            scratch_shapes=[
                pltpu.VMEM(tokens.shape, jnp.int32), pltpu.VMEM(labels.shape, jnp.int32), pltpu.VMEM((n_stage, tok_n), jnp.int32),
                act, act, act, pltpu.VMEM((total, ffn), BF16), pltpu.VMEM((total, ffn), BF16),
                pltpu.VMEM((n_stage, dim, ffn), BF16), pltpu.VMEM((n_stage, ffn, dim), BF16),
                pltpu.VMEM((vocab, dim), BF16), pltpu.VMEM((tok_n, vocab), BF16),
                pltpu.VMEM((n_stage + 1, tok_n, dim), BF16), pltpu.VMEM((n_stage + 1, tok_n, dim), BF16),
                pltpu.VMEM((n_stage, tok_n, ffn), BF16), pltpu.VMEM((n_stage, tok_n, dim), BF16),
                pltpu.VMEM((2 * tok_n, dim), F32),
                pltpu.VMEM((dim, total), BF16), pltpu.VMEM((8, total), F32), pltpu.VMEM((16, total), BF16),
                dma((5,)), dma((14,))] + [dma((n_stage,))] * 12 + [dma((pl.cdiv(vocab // 2, TABLE_BLOCK),))] * 2,
            compiler_params=pltpu.CompilerParams(collective_id=0, has_side_effects=True, vmem_limit_bytes=TOKEN_VMEM),
            name="token_pass",
        )(tokens, labels, emb_table, w_up, w_down)

        smem = pl.BlockSpec(memory_space=pltpu.SMEM)
        n_blk = pl.cdiv(vocab, EMB_BLOCK)
        grad_emb, grad_up, grad_down, loss = pl.pallas_call(
            finish_kernel,
            out_shape=[jax.ShapeDtypeStruct((vocab, dim), F32), jax.ShapeDtypeStruct((dim, ffn), F32),
                       jax.ShapeDtypeStruct((ffn, dim), F32), jax.ShapeDtypeStruct((1,), F32)],
            in_specs=[vmem] * 7, out_specs=[hbm, hbm, hbm, smem],
            scratch_shapes=[
                pltpu.SMEM((1, tok_n), jnp.int32), pltpu.VMEM((vocab, dim), F32), dma((n_blk, WRITE_PARTS)), dma((3,))],
            compiler_params=pltpu.CompilerParams(vmem_limit_bytes=FINISH_VMEM),
            name="finish",
        )(starts, part, st_all, ids, dxs, gup, gdn)
        return loss, grad_up[None], grad_down[None], grad_emb

    return jax.shard_map(
        device_fn, mesh=mesh,
        in_specs=(P("dp", None), P("dp", None), P(None, None), P("stage", None, None), P("stage", None, None)),
        out_specs=(P("dp"), P(("dp", "stage"), None, None), P(("dp", "stage"), None, None), P("dp", None)),
        check_vma=False)
```

```python
import functools
import math

import jax
import jax.numpy as jnp
from jax import lax
from jax.experimental import pallas as pl
from jax.experimental.pallas import tpu as pltpu
from jax.sharding import PartitionSpec as P

MESH = pl.DeviceIdType.MESH
F32 = jnp.float32
BF16 = jnp.bfloat16
LOG2E = math.log2(math.e)
LN2 = math.log(2.0)
GELU_C = math.sqrt(2.0 / math.pi)
HEAD_BLOCK = 8192
TABLE_BLOCK = 3648
EMB_BLOCK = 1024
WRITE_PARTS = 1
TOKEN_VMEM = 46 * 1024 * 1024
FINISH_VMEM = 28 * 1024 * 1024


def dot_nn(a, b):
    return lax.dot_general(a, b, (((1,), (0,)), ((), ())), preferred_element_type=F32)


def dot_nt(a, b):
    return lax.dot_general(a, b, (((1,), (1,)), ((), ())), preferred_element_type=F32)


def dot_tn(a, b):
    return lax.dot_general(a, b, (((0,), (0,)), ((), ())), preferred_element_type=F32)


def gelu_value(a):
    return a * (0.5 * (1.0 + jnp.tanh(GELU_C * (a + 0.044715 * (a * a * a)))))


def gelu_slope(a):
    sq = a * a
    t = jnp.tanh(GELU_C * (a + 0.044715 * (sq * a)))
    return 0.5 * (1.0 + t) + (0.5 * a) * (1.0 - t * t) * (GELU_C * (1.0 + (3.0 * 0.044715) * sq))


def column_of(row, size):
    return jnp.transpose(jnp.broadcast_to(row, (size, size)))


def joined_row(ref, i, size):
    per = size // ref.shape[1]
    return jnp.concatenate([ref[pl.ds(i * per + k, 1), :] for k in range(per)], axis=1)


def row_of(col, size):
    eye = lax.broadcasted_iota(jnp.int32, (size, size), 0) == lax.broadcasted_iota(jnp.int32, (size, size), 1)
    return jnp.sum(jnp.where(eye, jnp.broadcast_to(col, (size, size)), 0.0), axis=0, keepdims=True)


def token_kernel(
    n_stage, tok_hbm, lab_hbm, emb_hbm, wup_hbm, wdn_hbm,
    st_all, table_out, ids_out, starts_out, dxs, gup_out, gdn_out,
    tok_ref, lab_ref, rank_out, xs_out, gs_out, dx_out, hid, da_buf,
    wup, wdn, emb, z_buf, xs, gs, pre, n_all, gat, n_t, level_t, d_lab_t,
    loc_sem, wsend, upr, dnr, xsend, xrecv, gsend, grecv, nsend, nrecv, ssend, srecv, dsend, drecv, tsend, trecv,
):
    me = lax.axis_index("stage")
    n_chip = n_stage // 2
    chip, core = me // 2, lax.rem(me, 2)
    sib = chip * 2 + (1 - core)
    right = lax.rem(chip + 1, n_chip) * 2 + core
    left = lax.rem(chip + n_chip - 1, n_chip) * 2 + core
    far = lax.rem(chip + 2, n_chip) * 2 + core
    peers = [lax.rem(me + d, n_stage) for d in range(1, n_stage)]
    _, tok_n, dim = n_all.shape
    vocab = emb.shape[0]
    total = n_stage * tok_n
    scale = dim ** -0.5

    load_up = pltpu.make_async_copy(wup_hbm, wup.at[me], loc_sem.at[0])
    load_dn = pltpu.make_async_copy(wdn_hbm, wdn.at[me], loc_sem.at[1])
    load_emb = pltpu.make_async_copy(emb_hbm, emb, loc_sem.at[2])
    load_tok = pltpu.make_async_copy(tok_hbm, tok_ref, loc_sem.at[3])
    load_lab = pltpu.make_async_copy(lab_hbm, lab_ref, loc_sem.at[4])
    for copy in (load_up, load_dn, load_tok, load_lab, load_emb):
        copy.start()

    barrier = pltpu.get_barrier_semaphore()
    for peer in (right, left, sib):
        pl.semaphore_signal(barrier, inc=1, device_id={"stage": peer}, device_id_type=MESH)
    pl.semaphore_wait(barrier, 3)
    load_up.wait()
    load_dn.wait()

    def up_copy(i, slot, dst):
        return pltpu.make_async_remote_copy(
            wup.at[slot], wup.at[slot], wsend.at[i], upr.at[slot], device_id={"stage": dst}, device_id_type=MESH)

    def dn_copy(i, slot, dst):
        return pltpu.make_async_remote_copy(
            wdn.at[slot], wdn.at[slot], wsend.at[i], dnr.at[slot], device_id={"stage": dst}, device_id_type=MESH)

    first = [up_copy(0, me, right), dn_copy(1, me, left), dn_copy(2, me, right), up_copy(3, me, left),
             up_copy(4, me, sib), dn_copy(5, me, sib)]
    for copy in first:
        copy.start()

    load_tok.wait()
    load_lab.wait()
    tok_row = jnp.concatenate([joined_row(tok_ref, i, tok_n) for i in range(n_stage)], axis=0)
    pos = lax.broadcasted_iota(jnp.int32, (n_stage, tok_n), 0) * tok_n + lax.broadcasted_iota(jnp.int32, (n_stage, tok_n), 1)
    key_row = tok_row * total + pos
    lane = lax.broadcasted_iota(jnp.int32, (tok_n, tok_n), 1)
    key_cols = [column_of(key_row[j:j + 1, :], tok_n) for j in range(n_stage)]
    tok_cols = [column_of(tok_row[j:j + 1, :], tok_n) for j in range(n_stage)]
    rank_rows = []
    for i in range(n_stage):
        acc = jnp.zeros((tok_n, tok_n), jnp.int32)
        for j in range(n_stage):
            acc = acc + jnp.where(key_cols[j] < key_row[i:i + 1, :], 1, 0)
        rank_rows.append(jnp.sum(acc, axis=0, keepdims=True))
    rank_cols = [column_of(r, tok_n) for r in rank_rows]
    for c in range(n_stage):
        acc = jnp.zeros((tok_n, tok_n), jnp.int32)
        for j in range(n_stage):
            acc = acc + jnp.where(rank_cols[j] == lane + c * tok_n, tok_cols[j], 0)
        ids_out[c] = jnp.broadcast_to(jnp.sum(acc, axis=0, keepdims=True), (8, tok_n))
    ids_out[n_stage] = jnp.full((8, tok_n), -1, jnp.int32)
    acc = jnp.zeros((tok_n, tok_n), jnp.int32)
    for j in range(n_stage):
        acc = acc + jnp.where(tok_cols[j] < lane * EMB_BLOCK, 1, 0)
    starts_out[...] = jnp.sum(acc, axis=0, keepdims=True)
    for i in range(n_stage):
        rank_out[i:i + 1, :] = rank_rows[i]

    load_emb.wait()
    pick = jnp.concatenate(
        [column_of(joined_row(tok_ref, me, tok_n), tok_n), column_of(joined_row(lab_ref, me, tok_n), tok_n)], axis=0)
    lane2 = lax.broadcasted_iota(jnp.int32, (2 * tok_n, tok_n), 1)

    head_full = vocab // HEAD_BLOCK

    def blocks(body, lo=0, hi=head_full):
        def step(i, carry):
            body(pl.multiple_of(i * HEAD_BLOCK, HEAD_BLOCK), HEAD_BLOCK)
            return carry

        lax.fori_loop(lo, hi, step, 0)
        if hi == head_full and vocab % HEAD_BLOCK:
            body(head_full * HEAD_BLOCK, vocab % HEAD_BLOCK)

    gat[...] = jnp.zeros_like(gat)
    zero = jnp.minimum(joined_row(tok_ref, 0, tok_n), 0).astype(F32)
    one = zero + 1.0

    def gather_block(v0, size):
        hot = jnp.concatenate(
            [jnp.where(pick == lane2 + (v0 + j * tok_n), one, zero).astype(BF16) for j in range(size // tok_n)], axis=1)
        gat[...] += dot_nn(hot, emb[pl.ds(v0, size), :])

    blocks(gather_block, 0, head_full // 2)

    up_copy(0, left, sib).wait_recv()
    second = [up_copy(6, left, right), up_copy(7, left, sib)]
    second[0].start()
    second[1].start()
    dn_copy(0, right, sib).wait_recv()
    second += [dn_copy(8, right, left), dn_copy(9, right, sib)]
    second[2].start()
    second[3].start()

    blocks(gather_block, head_full // 2, head_full)
    x0 = gat[0:tok_n, :].astype(BF16)
    lab_rows = gat[tok_n:2 * tok_n, :]
    lab_bf = lab_rows.astype(BF16)

    dn_copy(0, left, sib).wait_recv()
    second.append(dn_copy(10, left, sib))
    second[4].start()
    up_copy(0, right, sib).wait_recv()
    second.append(up_copy(11, right, sib))
    second[5].start()
    up_copy(0, far, sib).wait_recv()
    second.append(up_copy(12, far, sib))
    second[6].start()
    dn_copy(0, far, sib).wait_recv()
    second.append(dn_copy(13, far, sib))
    second[7].start()

    def x_copy(layer):
        return pltpu.make_async_remote_copy(
            xs.at[layer], xs_out.at[me], xsend.at[layer], xrecv.at[me], device_id={"stage": layer}, device_id_type=MESH)

    def g_copy(layer):
        return pltpu.make_async_remote_copy(
            gs.at[layer + 1], gs_out.at[me], gsend.at[layer], grecv.at[me], device_id={"stage": layer}, device_id_type=MESH)


    xs[0] = x0

    def forward(layer, carry):
        @pl.when(lax.rem(layer, 2) != core)
        def _():
            up_copy(0, layer, sib).wait_recv()
            dn_copy(0, layer, sib).wait_recv()

        x = xs[layer]
        a = dot_nn(x, wup[layer]).astype(BF16)
        pre[layer] = a
        h = gelu_value(a.astype(F32)).astype(BF16)
        xs[layer + 1] = (x.astype(F32) + dot_nn(h, wdn[layer])).astype(BF16)

        @pl.when(layer != me)
        def _():
            x_copy(layer).start()

        @pl.when(layer == me)
        def _():
            xs_out[me] = x

        return carry

    lax.fori_loop(0, n_stage, forward, 0)

    x_last = xs[n_stage].astype(F32)
    inv = lax.rsqrt(jnp.mean(x_last * x_last, axis=-1, keepdims=True) + 1e-6)
    n_val = (x_last * inv).astype(BF16)
    n_all[me] = n_val

    def spread(src, dst, send, recv):
        return [pltpu.make_async_remote_copy(src, dst.at[me], send.at[d], recv.at[me], device_id={"stage": peer},
                                             device_id_type=MESH) for d, peer in enumerate(peers)]

    def stat_block(v0, size):
        z = (dot_nt(n_all[me], emb[pl.ds(v0, size), :]) * scale).astype(BF16)
        z_buf[:, pl.ds(v0, size)] = z
        parts = [z[:, j * tok_n:(j + 1) * tok_n].astype(F32) for j in range(size // tok_n)]
        m_old = gat[0:tok_n, :]
        m_new = functools.reduce(jnp.maximum, parts, m_old)
        s_new = gat[tok_n:2 * tok_n, :] * jnp.exp2((m_old - m_new) * LOG2E)
        for part in parts:
            s_new = s_new + jnp.exp2((part - m_new) * LOG2E)
        gat[0:tok_n, :] = m_new
        gat[tok_n:2 * tok_n, :] = s_new

    gat[0:tok_n, :] = jnp.full((tok_n, dim), -1e30, F32)
    gat[tok_n:2 * tok_n, :] = jnp.zeros((tok_n, dim), F32)
    send_n = spread(n_all.at[me], n_all, nsend, nrecv)
    for copy in send_n:
        copy.start()
    blocks(stat_block)
    m_lane = gat[0:tok_n, :]
    m_tok = jnp.max(m_lane, axis=-1, keepdims=True)
    s_tok = jnp.sum(gat[tok_n:2 * tok_n, :] * jnp.exp2((m_lane - m_tok) * LOG2E), axis=-1, keepdims=True)
    lse = m_tok + jnp.log(s_tok)
    level = lse * LOG2E + math.log2(total)
    z_pair = (dot_nt(n_val, lab_bf) * scale).astype(BF16).astype(F32)
    eye = lax.broadcasted_iota(jnp.int32, (tok_n, tok_n), 0) == lane
    z_lab = jnp.sum(jnp.where(eye, z_pair, 0.0), axis=-1, keepdims=True)
    p_lab = jnp.exp2(z_lab * LOG2E - level)
    d_lab = (p_lab - 1.0 / total).astype(BF16).astype(F32)
    p_lab = p_lab.astype(BF16).astype(F32)
    st_all[me] = jnp.concatenate(
        [row_of(level, tok_n), row_of(d_lab, tok_n), row_of(lse - z_lab, tok_n), jnp.zeros((5, tok_n), F32)], axis=0)
    level_full = jnp.broadcast_to(level, (tok_n, tok_n))

    gat[0:tok_n, :] = (d_lab - p_lab) * lab_rows
    send_s = spread(st_all.at[me], st_all, ssend, srecv)
    for copy in send_s:
        copy.start()

    def grad_block(v0, size):
        parts = []
        for j in range(size // tok_n):
            z = z_buf[:, pl.ds(v0 + j * tok_n, tok_n)].astype(F32)
            parts.append(jnp.exp2(z * LOG2E - level_full).astype(BF16))
        gat[0:tok_n, :] += dot_nn(jnp.concatenate(parts, axis=1), emb[pl.ds(v0, size), :])

    blocks(grad_block)
    dn = (gat[0:tok_n, :] * scale).astype(BF16).astype(F32)
    corr = jnp.mean(dn * x_last, axis=-1, keepdims=True)
    gs[n_stage] = (inv * dn - x_last * (inv * inv * inv * corr)).astype(BF16)

    def backward(layer):
        g = gs[layer + 1]
        dh = dot_nt(g, wdn[layer]).astype(BF16).astype(F32)
        da = (dh * gelu_slope(pre[layer].astype(F32))).astype(BF16)
        gs[layer] = (g.astype(F32) + dot_nt(da, wup[layer])).astype(BF16)

    def send_g(layer):
        @pl.when(layer != me)
        def _():
            g_copy(layer).start()

        @pl.when(layer == me)
        def _():
            gs_out[me] = gs[layer + 1]

    def back_step(i, carry):
        layer = n_stage - 1 - i
        backward(layer)
        send_g(layer)
        return carry

    lax.fori_loop(0, n_stage, back_step, 0)
    send_d = spread(gs.at[0], dx_out, dsend, drecv)
    for copy in send_d:
        copy.start()
    dx_out[me] = gs[0]

    for peer in peers:
        for buf, send, recv in ((n_all, nsend, nrecv), (st_all, ssend, srecv)):
            pltpu.make_async_remote_copy(buf.at[peer], buf.at[peer], send.at[0], recv.at[peer],
                                         device_id={"stage": peer}, device_id_type=MESH).wait_recv()
    for i in range(n_stage):
        cols = slice(i * tok_n, (i + 1) * tok_n)
        n_t[:, cols] = jnp.transpose(n_all[i])
        level_t[:, cols] = jnp.broadcast_to(st_all[i, 0:1, :], (8, tok_n))
        d_lab_t[:, cols] = jnp.broadcast_to(st_all[i, 1:2, :], (16, tok_n)).astype(BF16)
    half = vocab // 2
    wide = 2 * tok_n

    def table_copies(j, size):
        rows = pl.ds(pl.multiple_of(core * half + j * TABLE_BLOCK, 16), size)
        return (pltpu.make_async_remote_copy(table_out.at[rows], table_out.at[rows], tsend.at[j], trecv.at[j],
                                             device_id={"stage": sib}, device_id_type=MESH),)

    def table_start(j, size):
        for copy in table_copies(j, size):
            copy.start()

    def table_block(j, size):
        base = pl.multiple_of(core * half + j * TABLE_BLOCK, 16)
        for r in range(0, size, 608):
            table_rows(base, j * TABLE_BLOCK + r, r, min(608, size - r))

    def table_rows(base, at, r, size):
        e = emb[pl.ds(pl.multiple_of(base + r, 16), size), :]
        row16 = lax.broadcasted_iota(jnp.int16, (size, wide), 0)
        acc = jnp.zeros((size, dim), F32)
        for t in range(total // wide):
            cols = slice(t * wide, (t + 1) * wide)
            z = (dot_nn(e, n_t[:, cols]) * scale).astype(BF16).astype(F32)
            p = jnp.exp2(z * LOG2E - level_t[0:1, cols]).astype(BF16)
            lab = jnp.concatenate([joined_row(lab_ref, 2 * t, tok_n), joined_row(lab_ref, 2 * t + 1, tok_n)], axis=1) - (base + r)
            lab = jnp.broadcast_to(lab, (16, wide)).astype(jnp.int16)
            dz = jnp.where(row16 == lab[0:1, :], d_lab_t[0:1, cols], p)
            acc = acc + dot_nn(dz, jnp.concatenate([n_all[2 * t], n_all[2 * t + 1]], axis=0))
        table_out[pl.ds(pl.multiple_of(base + r, 16), size), :] = acc * scale

    full, tail = half // TABLE_BLOCK, half % TABLE_BLOCK
    grad_tok = 2 * tok_n

    def table_step(j, carry):
        @pl.when(j > 0)
        def _():
            table_start(j - 1, TABLE_BLOCK)

        table_block(j, TABLE_BLOCK)
        return carry

    lax.fori_loop(0, full, table_step, 0)
    table_start(full - 1, TABLE_BLOCK)
    if tail:
        table_block(full, tail)
        table_start(full, tail)

    for peer in peers:
        pltpu.make_async_remote_copy(xs.at[peer], xs_out.at[peer], xsend.at[peer], xrecv.at[peer],
                                     device_id={"stage": peer}, device_id_type=MESH).wait()
        pltpu.make_async_remote_copy(gs.at[peer + 1], gs_out.at[peer], gsend.at[peer], grecv.at[peer],
                                     device_id={"stage": peer}, device_id_type=MESH).wait()
        pltpu.make_async_remote_copy(gs.at[0], dx_out.at[peer], dsend.at[0], drecv.at[peer],
                                     device_id={"stage": peer}, device_id_type=MESH).wait_recv()

    def weight_part(i):
        x = jnp.concatenate([xs_out[2 * i], xs_out[2 * i + 1]], axis=0)
        g = jnp.concatenate([gs_out[2 * i], gs_out[2 * i + 1]], axis=0)
        a = dot_nn(x, wup[me]).astype(BF16).astype(F32)
        sq = a * a
        t = jnp.tanh(GELU_C * (a + 0.044715 * (sq * a)))
        cdf = 0.5 * (1.0 + t)
        rows = slice(i * grad_tok, (i + 1) * grad_tok)
        hid[rows, :] = (a * cdf).astype(BF16)
        slope = cdf + (0.5 * a) * (1.0 - t * t) * (GELU_C * (1.0 + (3.0 * 0.044715) * sq))
        dh = dot_nt(g, wdn[me]).astype(BF16).astype(F32)
        da_buf[rows, :] = (dh * slope).astype(BF16)

    for i in range(n_stage // 2):
        weight_part(i)
    gup_out[...] = dot_tn(xs_out[...].reshape(total, dim), da_buf[...])
    gdn_out[...] = jnp.transpose(dot_tn(gs_out[...].reshape(total, dim), hid[...]))
    row_id = lax.broadcasted_iota(jnp.int32, (tok_n, tok_n), 0)
    for c in range(n_stage):
        acc = jnp.zeros((tok_n, dim), F32)
        for i in range(n_stage):
            hot = jnp.where(rank_out[i:i + 1, :] == row_id + c * tok_n, one, zero).astype(BF16)
            acc = acc + dot_nn(hot, dx_out[i])
        dxs[c] = acc.astype(BF16)
    dxs[n_stage] = jnp.zeros((tok_n, dim), BF16)

    for copy in first + second + send_n + send_s:
        copy.wait_send()
    for copy in send_d:
        copy.wait_send()

    def table_wait(j, size):
        table_copies(j, size)[0].wait_send()
        rows = pl.ds(pl.multiple_of((1 - core) * half + j * TABLE_BLOCK, 16), size)
        pltpu.make_async_remote_copy(table_out.at[rows], table_out.at[rows],
                                     tsend.at[j], trecv.at[j], device_id={"stage": sib}, device_id_type=MESH).wait_recv()

    def wait_step(j, carry):
        table_wait(j, TABLE_BLOCK)
        return carry

    lax.fori_loop(0, full, wait_step, 0)
    if tail:
        table_wait(full, tail)


def finish_kernel(
    starts_ref, part_ref, st_ref, ids_ref, dxs, gup_ref, gdn_ref,
    out_hbm, gup_hbm, gdn_hbm, loss_ref,
    starts_sm, buf, write_sem, grad_sem,
):
    n_chunk, tok_n, _ = dxs.shape
    n_chunk = n_chunk - 1
    vocab = buf.shape[0]
    full, tail = vocab // EMB_BLOCK, vocab % EMB_BLOCK

    def span(j, size):
        return pl.ds(pl.multiple_of(j * EMB_BLOCK, 16), size)

    def write(j, size):
        part = size // WRITE_PARTS
        return [pltpu.make_async_copy(
            buf.at[pl.ds(pl.multiple_of(j * EMB_BLOCK + k * part, 8), part)],
            out_hbm.at[pl.ds(pl.multiple_of(j * EMB_BLOCK + k * part, 8), part)], write_sem.at[j, k]) for k in range(WRITE_PARTS)]

    def write_start(j, size):
        for k, copy in enumerate(write(j, size)):
            copy.start(priority=k % 2)

    def write_wait(j, size):
        for copy in write(j, size):
            copy.wait()

    def each(fn):
        def step(j, carry):
            fn(j, EMB_BLOCK)
            return carry

        lax.fori_loop(0, full, step, 0)
        if tail:
            fn(full, tail)

    load_starts = pltpu.make_async_copy(starts_ref, starts_sm, grad_sem.at[2])
    load_starts.start()

    grads = [pltpu.make_async_copy(gup_ref, gup_hbm, grad_sem.at[0]), pltpu.make_async_copy(gdn_ref, gdn_hbm, grad_sem.at[1])]
    for copy in grads:
        copy.start()
    loss_ref[0] = jnp.sum(st_ref[:, 2, :]) * (1.0 / (n_chunk * tok_n))

    mark = jnp.broadcast_to(ids_ref[n_chunk, 0:1, :].astype(F32), (16, tok_n))
    one, zero = (-mark).astype(BF16)[0:1, :], (mark + 1.0).astype(BF16)[0:1, :]

    def add_tokens(j, size):
        rows = span(j, size)
        row16 = lax.broadcasted_iota(jnp.int16, (size, tok_n), 0)

        def hot_rows(c):
            ids = jnp.broadcast_to(ids_ref[c, 0:1, :] - j * EMB_BLOCK, (16, tok_n)).astype(jnp.int16)
            return jnp.where(row16 == ids[0:1, :], one, zero)

        first = jnp.minimum(starts_sm[0, j] // tok_n, n_chunk - 1)
        last = (starts_sm[0, j + 1] + tok_n - 1) // tok_n
        buf[rows, :] = part_ref[rows, :] + dot_nn(jnp.concatenate([hot_rows(first), hot_rows(first + 1)], axis=1),
                               jnp.concatenate([dxs[first], dxs[first + 1]], axis=0))

        def more(c, carry):
            buf[rows, :] += dot_nn(hot_rows(c), dxs[c])
            return carry

        lax.fori_loop(first + 2, last, more, 0)
        write_start(j, size)

    load_starts.wait()
    each(add_tokens)
    each(write_wait)
    for copy in grads:
        copy.wait()


def solution(mesh):
    n_stage = mesh.shape["stage"]

    def device_fn(tokens, labels, emb_table, w_up, w_down):
        vocab, dim = emb_table.shape
        ffn = w_up.shape[2]
        total = tokens.shape[0] * tokens.shape[1]
        tok_n = total // n_stage
        w_up, w_down = w_up[0], w_down[0]
        hbm = pl.BlockSpec(memory_space=pl.ANY)
        vmem = pl.BlockSpec(memory_space=pltpu.VMEM)
        dma = pltpu.SemaphoreType.DMA
        act = pltpu.VMEM((n_stage, tok_n, dim), BF16)
        st_all, part, ids, starts, dxs, gup, gdn = pl.pallas_call(
            functools.partial(token_kernel, n_stage),
            out_shape=[pltpu.VMEM((n_stage, 8, tok_n), F32), pltpu.VMEM((vocab, dim), F32),
                       pltpu.VMEM((n_stage + 1, 8, tok_n), jnp.int32), pltpu.VMEM((1, tok_n), jnp.int32),
                       pltpu.VMEM((n_stage + 1, tok_n, dim), BF16), pltpu.VMEM((dim, ffn), F32), pltpu.VMEM((ffn, dim), F32)],
            in_specs=[hbm] * 5,
            out_specs=[vmem] * 7,
            scratch_shapes=[
                pltpu.VMEM(tokens.shape, jnp.int32), pltpu.VMEM(labels.shape, jnp.int32), pltpu.VMEM((n_stage, tok_n), jnp.int32),
                act, act, act, pltpu.VMEM((total, ffn), BF16), pltpu.VMEM((total, ffn), BF16),
                pltpu.VMEM((n_stage, dim, ffn), BF16), pltpu.VMEM((n_stage, ffn, dim), BF16),
                pltpu.VMEM((vocab, dim), BF16), pltpu.VMEM((tok_n, vocab), BF16),
                pltpu.VMEM((n_stage + 1, tok_n, dim), BF16), pltpu.VMEM((n_stage + 1, tok_n, dim), BF16),
                pltpu.VMEM((n_stage, tok_n, ffn), BF16), pltpu.VMEM((n_stage, tok_n, dim), BF16),
                pltpu.VMEM((2 * tok_n, dim), F32),
                pltpu.VMEM((dim, total), BF16), pltpu.VMEM((8, total), F32), pltpu.VMEM((16, total), BF16),
                dma((5,)), dma((14,))] + [dma((n_stage,))] * 12 + [dma((pl.cdiv(vocab // 2, TABLE_BLOCK),))] * 2,
            compiler_params=pltpu.CompilerParams(collective_id=0, has_side_effects=True, vmem_limit_bytes=TOKEN_VMEM),
            name="token_pass",
        )(tokens, labels, emb_table, w_up, w_down)

        smem = pl.BlockSpec(memory_space=pltpu.SMEM)
        n_blk = pl.cdiv(vocab, EMB_BLOCK)
        grad_emb, grad_up, grad_down, loss = pl.pallas_call(
            finish_kernel,
            out_shape=[jax.ShapeDtypeStruct((vocab, dim), F32), jax.ShapeDtypeStruct((dim, ffn), F32),
                       jax.ShapeDtypeStruct((ffn, dim), F32), jax.ShapeDtypeStruct((1,), F32)],
            in_specs=[vmem] * 7, out_specs=[hbm, hbm, hbm, smem],
            scratch_shapes=[
                pltpu.SMEM((1, tok_n), jnp.int32), pltpu.VMEM((vocab, dim), F32), dma((n_blk, WRITE_PARTS)), dma((3,))],
            compiler_params=pltpu.CompilerParams(vmem_limit_bytes=FINISH_VMEM),
            name="finish",
        )(starts, part, st_all, ids, dxs, gup, gdn)
        return loss, grad_up[None], grad_down[None], grad_emb

    return jax.shard_map(
        device_fn, mesh=mesh,
        in_specs=(P("dp", None), P("dp", None), P(None, None), P("stage", None, None), P("stage", None, None)),
        out_specs=(P("dp"), P(("dp", "stage"), None, None), P(("dp", "stage"), None, None), P("dp", None)),
        check_vma=False)
```
